32 devices in a mesh: dp: 4 (over z), rows: 8 (over y, x, core).
Axes of the slice: x: 2, y: 2, z: 4, core: 2. Of those that a mesh axis runs over, the one named last changes fastest.
Arguments:
- latent: bfloat16 [8, 8, 64, 640], P('dp', 'rows'), may hold values from -16.25 to 16.25
- hidden: bfloat16 [8, 8, 64, 640], P('dp', 'rows'), may hold values from -16.25 to 16.25
- cotangent: bfloat16 [8, 8, 64, 640], P('dp', 'rows'), may hold values from -6 to 6
- filter_one: bfloat16 [9, 640, 640], P(None, 'dp', 'rows'), may hold values from -0.078125 to 0.078125
- filter_two: bfloat16 [9, 640, 640], P(None, 'dp', 'rows'), may hold values from -0.078125 to 0.078125
- gain_one: float32 [640], replicated, may hold values from 0.1 to 1.9
- shift_one: float32 [640], replicated, may hold values from -2.5 to 2.5
- gain_two: float32 [640], replicated, may hold values from 0.1 to 1.9
- shift_two: float32 [640], replicated, may hold values from -2.5 to 2.5
Outputs:
- latent_grad: bfloat16 [8, 8, 64, 640], P('dp', 'rows')
The draws below stay inside these ranges and needn't reach their ends.
All inputs are finite; a program needn't handle non-finite values.
Results may differ from the reference program's by a relative error of at most 0.0027.
Values may be sent and summed in bfloat16 or wider, within the bound.
A program may use at most 128 MiB of HBM per device.

```python
import jax
import jax.numpy as jnp
from jax import lax

GROUPS = 16
GSIZE = 40
WIDTH = 64
CH = 640
IMAGES = 8
HEIGHT = 8


def draw_field(key, salt):
    key = jax.random.fold_in(key, salt)
    key_noise, key_channel = jax.random.split(key, 2)
    height_pos = jnp.arange(HEIGHT, dtype=jnp.float32) / max(HEIGHT - 1, 1)
    row_scale = jnp.exp(jnp.log(3.0) * height_pos)[None, :, None, None]
    channel_scale = jnp.exp(jax.random.uniform(key_channel, (CH,), jnp.float32, jnp.log(0.1), 0.0))
    noise = jnp.clip(jax.random.normal(key_noise, (IMAGES, HEIGHT, WIDTH, CH), jnp.float32), -5.0, 5.0)
    field = noise * row_scale * channel_scale
    return field.astype(jnp.bfloat16)


def draw_latent(key, part):
    return draw_field(key, 11)


def draw_hidden(key, part):
    return draw_field(key, 23)


def draw_cotangent(key, part):
    key = jax.random.fold_in(key, 37)
    key_noise, key_offset = jax.random.split(key, 2)
    noise = jax.random.normal(key_noise, (IMAGES, HEIGHT, WIDTH, CH), jnp.float32)
    offset = jax.random.normal(key_offset, (IMAGES, 1, 1, CH), jnp.float32)
    field = jnp.clip(noise + offset, -6.0, 6.0)
    return field.astype(jnp.bfloat16)


def levels(key, dims, cuts, low, top_value):
    factor_of, own = 1.0, jax.random.fold_in(key, 6)
    for axis_at, blocks in cuts:
        draws = jnp.exp(jax.random.uniform(jax.random.fold_in(own, axis_at), (blocks,), jnp.float32, low / len(cuts), top_value / len(cuts)))
        factor_of = factor_of * jnp.repeat(draws, dims[axis_at] // blocks).reshape([-1 if axis == axis_at else 1 for axis in range(len(dims))])
    return factor_of


def centred(stream_key, extent, scale, most, cuts=(), held_as=jnp.bfloat16):
    level = levels(stream_key, extent, cuts, -0.22, 0.18) if cuts else 1.0
    values = jax.random.normal(stream_key, extent, jnp.float32) * scale * level
    return jnp.minimum(jnp.maximum(values, -most), most).astype(held_as)


def setup_inputs(seed: int = 0) -> dict:
    seeds = jax.random.split(jax.random.key(seed), 10)
    return {
        "latent": draw_latent(jax.random.fold_in(seeds[9], 71), 0),
        "hidden": draw_hidden(jax.random.fold_in(seeds[9], 71), 0),
        "cotangent": draw_cotangent(jax.random.fold_in(seeds[9], 71), 0),
        "filter_one": centred(seeds[3], (9, CH, CH), (9 * CH) ** -0.5, 0.078125, ((1, 4), (2, 8))),
        "filter_two": centred(seeds[4], (9, CH, CH), (9 * CH) ** -0.5, 0.078125, ((1, 4), (2, 8))),
        "gain_one": jnp.clip(1.0 + 0.18 * jax.random.normal(seeds[5], (CH,), jnp.float32), 0.1, 1.9),
        "shift_one": centred(seeds[6], (CH,), 0.5, 2.5, (), jnp.float32),
        "gain_two": jnp.clip(1.0 + 0.18 * jax.random.normal(seeds[7], (CH,), jnp.float32), 0.1, 1.9),
        "shift_two": centred(seeds[8], (CH,), 0.5, 2.5, (), jnp.float32),
    }


def group_sums(values):
    per_channel = lax.optimization_barrier(jnp.sum(values, axis=(1, 2)))
    return lax.optimization_barrier(jnp.sum(per_channel.reshape(per_channel.shape[0], GROUPS, -1), axis=2))

def expand_groups(moment):
    return jnp.repeat(moment, GSIZE, axis=1)[:, None, None, :]

def finish_stats(sum_plain, sum_square, number):
    average = sum_plain / number
    variance = sum_square / number - average * average
    return (average, lax.rsqrt(variance + 1e-05))

def norm_backward(field, stats, gain, shift, incoming, number):
    average, inverse = stats
    values = field.astype(jnp.float32)
    normed = (values - expand_groups(average)) * expand_groups(inverse)
    linear = normed * gain + shift
    logistic = jax.nn.sigmoid(linear)
    scaled = incoming * logistic * (1.0 + linear * (1.0 - logistic)) * gain
    first = group_sums(scaled) / number
    second = group_sums(scaled * normed) / number
    return expand_groups(inverse) * (scaled - expand_groups(first) - normed * expand_groups(second))

def conv_backward(gradient, weights):
    images, height, breadth, channels = gradient.shape
    padded = jnp.pad(gradient, ((0, 0), (1, 1), (1, 1), (0, 0)))
    result = jnp.zeros((images * height * breadth, channels), jnp.float32)
    for tap_index in range(9):
        down_step = tap_index // 3 - 1
        side_step = tap_index % 3 - 1
        window = padded[:, 1 - down_step:1 - down_step + height, 1 - side_step:1 - side_step + breadth, :]
        window = window.reshape(images * height * breadth, channels)
        result = result + jnp.dot(window, weights[tap_index].T, preferred_element_type=jnp.float32)
    return result.reshape(images, height, breadth, channels)

def reference(latent, hidden, cotangent, filter_one, filter_two, gain_one, shift_one, gain_two, shift_two):
    number = HEIGHT * WIDTH * GSIZE
    latent_values = latent.astype(jnp.float32)
    hidden_values = hidden.astype(jnp.float32)
    stats_one = finish_stats(group_sums(latent_values), group_sums(latent_values * latent_values), number)
    stats_two = finish_stats(group_sums(hidden_values), group_sums(hidden_values * hidden_values), number)
    back_two = conv_backward(cotangent, filter_two)
    hidden_grad = norm_backward(hidden, stats_two, gain_two, shift_two, back_two, number).astype(jnp.bfloat16)
    back_one = conv_backward(hidden_grad, filter_one)
    latent_part = norm_backward(latent, stats_one, gain_one, shift_one, back_one, number)
    return (cotangent.astype(jnp.float32) + latent_part).astype(jnp.bfloat16)
```

```python
import functools

import jax
import jax.numpy as jnp
from jax import lax
from jax.experimental import pallas as pl
from jax.experimental.pallas import tpu as pltpu
from jax.sharding import PartitionSpec as P

GROUPS = 16
GSIZE = 40
TAPS = 9
MESH = pl.DeviceIdType.MESH


def extended(block, sides, width):
    for axis, dim in sides:
        count = lax.axis_size(axis)
        forward = [(i, i + 1) for i in range(count - 1)]
        backward = [(target, source) for source, target in forward]
        low = lax.ppermute(
            lax.slice_in_dim(block, block.shape[dim] - width, None, axis=dim), axis, forward
        )
        high = lax.ppermute(lax.slice_in_dim(block, 0, width, axis=dim), axis, backward)
        block = jnp.concatenate([low, block, high], axis=dim)
    return block


def group_sums(values):
    per_channel = jnp.sum(values, axis=(1, 2))
    return jnp.sum(per_channel.reshape(per_channel.shape[0], GROUPS, -1), axis=2)


def expand_groups(moment):
    return jnp.repeat(moment, GSIZE, axis=1)[:, None, None, :]


def finish_stats(sum_plain, sum_square, number):
    average = sum_plain / number
    variance = sum_square / number - average * average
    return (average, lax.rsqrt(variance + 1e-05))


def reduced_stats(field, number):
    values = field.astype(jnp.float32)
    sum_plain, sum_square = lax.psum((group_sums(values), group_sums(values * values)), "rows")
    return finish_stats(sum_plain, sum_square, number)


def norm_backward(field, stats, gain, shift, incoming, number):
    average, inverse = stats
    values = field.astype(jnp.float32)
    normed = (values - expand_groups(average)) * expand_groups(inverse)
    linear = normed * gain + shift
    logistic = jax.nn.sigmoid(linear)
    scaled = incoming * logistic * (1.0 + linear * (1.0 - logistic)) * gain
    sum_first, sum_second = lax.psum((group_sums(scaled), group_sums(scaled * normed)), "rows")
    first = sum_first / number
    second = sum_second / number
    return expand_groups(inverse) * (scaled - expand_groups(first) - normed * expand_groups(second))


def conv_backward(gradient, weights):
    images, rows_here, breadth, channels = gradient.shape
    padded = extended(gradient, (("rows", 1),), 1)
    padded = jnp.pad(padded, ((0, 0), (0, 0), (1, 1), (0, 0)))
    pixels = images * rows_here * breadth
    shifted = []
    for tap_index in range(9):
        down_step = tap_index // 3 - 1
        side_step = tap_index % 3 - 1
        window = padded[
            :, 1 - down_step : 1 - down_step + rows_here, 1 - side_step : 1 - side_step + breadth, :
        ]
        shifted.append(window.reshape(pixels, channels))
    stacked = jnp.stack(shifted, axis=1)
    gathered = lax.all_gather(weights, "dp", axis=1, tiled=True)
    section = lax.all_gather(gathered, "rows", axis=2, tiled=True)
    columns = section.shape[2]
    window = stacked.reshape(pixels, 9 * columns)
    flat = jnp.transpose(section, (0, 2, 1)).reshape(9 * columns, section.shape[1])
    result = jnp.dot(window, flat, preferred_element_type=jnp.float32)
    return result.reshape(images, rows_here, breadth, channels)


def plain_body(
    latent, hidden, cotangent, filter_one, filter_two, gain_one, shift_one, gain_two, shift_two
):
    number = latent.shape[1] * lax.axis_size("rows") * latent.shape[2] * GSIZE
    stats_two = reduced_stats(hidden, number)
    back_two = conv_backward(cotangent, filter_two)
    hidden_grad = norm_backward(hidden, stats_two, gain_two, shift_two, back_two, number).astype(
        jnp.bfloat16
    )
    stats_one = reduced_stats(latent, number)
    back_one = conv_backward(hidden_grad, filter_one)
    latent_part = norm_backward(latent, stats_one, gain_one, shift_one, back_one, number)
    return (cotangent.astype(jnp.float32) + latent_part).astype(jnp.bfloat16)


def kernel(
    depth, rows, breadth,
    lat_ref, hid_ref, cot_ref, raw1, raw2, gain1, shift1, gain2, shift2,
    out_ref,
    cot_t, x_cot, hid_s, hid_b, w1, w2, s1, s2, r1,
    xs1, xs2, y_ref, p1, q1, p2, q2, hg_s, hg_r,
    nrm1, act1, nrm2, act2, inv2_ref, st_s, st_b, par_ref,
    z_send, z_recv, f_send, f_recv, b_send, b_recv, c_send, c_recv, h_send, h_recv,
    p_send, p_recv, g_send, g_recv, o_send, o_recv, t_send, t_recv,
):
    d = lax.axis_index("dp")
    r = lax.axis_index("rows")
    chips = rows // 2
    c = r // 2
    k = lax.rem(r, 2)
    sibling = r + 1 - 2 * k
    channels, lanes = cot_t.shape
    block = channels // depth
    half = block // 2
    images = lanes // breadth
    wide = w1.shape[3]
    number = rows * breadth * GSIZE
    groups = channels // GSIZE
    bf16, f32 = jnp.bfloat16, jnp.float32

    def remote(src, dst, send, recv, **device):
        return pltpu.make_async_remote_copy(
            src_ref=src, dst_ref=dst, send_sem=send, recv_sem=recv,
            device_id=device, device_id_type=MESH,
        )

    barrier = pltpu.get_barrier_semaphore()

    @pl.when(d > 0)
    def _():
        pl.semaphore_signal(barrier, inc=1, device_id={"dp": d - 1}, device_id_type=MESH)

    @pl.when(d < depth - 1)
    def _():
        pl.semaphore_signal(barrier, inc=1, device_id={"dp": d + 1}, device_id_type=MESH)

    for off in range(1, rows):
        pl.semaphore_signal(barrier, inc=1, device_id={"rows": lax.rem(r + off, rows)}, device_id_type=MESH)

    pending = []

    def arrange(ready, raw, which):
        start = pl.multiple_of(which * half, 16)
        pad = wide - 3 * half
        ready[:, 3 * half :] = jnp.zeros((3 * half, pad), bf16)
        for tap in range(TAPS):
            down, side = tap // 3, tap % 3
            ready[down * half : (down + 1) * half, side * half : (side + 1) * half] = raw[
                tap, pl.ds(start, half), :
            ]

    arrange(w2.at[d, k], raw2, k)
    arrange(s2, raw2, 1 - k)

    beside = jnp.where((d > 0) & (d < depth - 1), 2, 1)
    pl.semaphore_wait(barrier, rows - 1 + beside)

    def hop(which, w, origin, part, way):
        return remote(
            w.at[origin, part], w.at[origin, part],
            z_send.at[which, way, origin, part], z_recv.at[which, origin, part], dp=d + 1 - 2 * way,
        )

    def can(way):
        return (d < depth - 1) if way == 0 else (d > 0)

    def start_hops(which, w, part, ways=(0, 1)):
        for way in ways:
            @pl.when(can(way))
            def _():
                hop(which, w, d, part, way).start()

    start_hops(0, w2, k)
    twin = remote(s2, w2.at[d, k], b_send.at[0], b_recv.at[0], rows=sibling)
    twin.start()
    pending.append(twin)

    cot_t[...] = cot_ref[...].T

    def piece_of(to):
        return cot_t.at[pl.ds(pl.multiple_of((to // 2) * block, block), block), :]

    for off in range(1, rows):
        to = lax.rem(r + off, rows)
        copy = remote(piece_of(to), x_cot.at[r], c_send.at[to], c_recv.at[r], rows=to)
        copy.start()
        pending.append(copy)
    x_cot[r] = piece_of(r)[...]

    remote(s2, w2.at[d, 1 - k], b_send.at[0], b_recv.at[0], rows=sibling).wait_recv()
    start_hops(0, w2, 1 - k)

    hid_full = hid_ref[...].astype(f32).T
    for to in range(rows):
        parts = [
            hid_full[block * b + GSIZE * (to // 2) : block * b + GSIZE * (to // 2 + 1)]
            for b in (to % 2, to % 2 + 2)
        ]
        hid_s[to] = jnp.concatenate(parts, axis=0).astype(bf16)
    for off in range(1, rows):
        to = lax.rem(r + off, rows)
        copy = remote(hid_s.at[to], hid_b.at[r], h_send.at[to], h_recv.at[r], rows=to)
        copy.start()
        pending.append(copy)
    hid_b[r] = hid_s[r]

    for part in range(2):
        for side_core in range(2):
            ready = s1.at[part, side_core]
            ready[:, 3 * GSIZE :] = jnp.zeros((3 * half, ready.shape[1] - 3 * GSIZE), bf16)
            for tap in range(TAPS):
                down, side = tap // 3, tap % 3
                ready[down * half : (down + 1) * half, side * GSIZE : (side + 1) * GSIZE] = raw1[
                    tap, side_core * half : (side_core + 1) * half, part * GSIZE : (part + 1) * GSIZE
                ]

    def each_shuffle(act):
        for part in range(2):
            for side_core in range(2):
                to = 2 * (2 * k + part) + side_core
                src = s1.at[part, side_core]

                @pl.when(to != r)
                def _():
                    act(remote(src, r1.at[c], f_send.at[part, side_core], f_recv.at[c], rows=to))

                yield to, src

    for to, src in each_shuffle(lambda copy: copy.start()):
        @pl.when(to == r)
        def _():
            r1[c] = src[...]

    lane = lax.broadcasted_iota(jnp.int32, (1, lanes), 1)
    column = lax.rem(lane, breadth)
    image_of = lax.div(lane, breadth)
    first_half = lax.rem(lane, breadth) < breadth // 2

    def image_totals(per_lane):
        total = jnp.zeros_like(per_lane)
        for image in range(images):
            mine = image_of == image
            part = jnp.sum(jnp.where(mine, per_lane, 0.0), axis=1, keepdims=True)
            total = jnp.where(mine, part, total)
        return total

    def pack_sums(one, two):
        return jnp.where(first_half, image_totals(one), image_totals(two))

    def send_sums(which, packed):
        st_s[which] = packed
        for off in range(1, rows):
            to = lax.rem(r + off, rows)
            copy = remote(st_s.at[which], st_b.at[which, r], t_send.at[which, to], t_recv.at[which, r], rows=to)
            copy.start()
            pending.append(copy)
        st_b[which, r] = packed

    def wait_sums(which):
        for off in range(1, rows):
            frm = lax.rem(r + off, rows)
            remote(
                st_s.at[which], st_b.at[which, frm], t_send.at[which, frm], t_recv.at[which, frm], rows=frm
            ).wait_recv()
        total = st_b[which, 0]
        for h in range(1, rows):
            total = total + st_b[which, h]
        total = total * (1.0 / number)
        quarter = breadth // 2
        ahead = pltpu.roll(total, lanes - quarter, 1)
        behind = pltpu.roll(total, quarter, 1)
        one = jnp.where(first_half, total, behind)
        two = jnp.where(first_half, ahead, total)
        return one, two

    def spread(moment):
        return jnp.broadcast_to(moment[:, None, :], (groups, GSIZE, lanes)).reshape(channels, lanes)

    def by_group(values):
        return jnp.sum(values.reshape(groups, GSIZE, lanes), axis=1)

    nrm1[...] = lat_ref[...].astype(f32).T
    send_sums(0, pack_sums(by_group(nrm1[...]), by_group(nrm1[...] * nrm1[...])))

    raw_params = [p[...].reshape(1, channels) for p in (gain1, shift1, gain2, shift2)]
    par_ref[...] = jnp.concatenate(raw_params + raw_params, axis=0).T

    def store_shifts(xs, part, h, values):
        left = jnp.where(column == breadth - 1, 0.0, pltpu.roll(values, lanes - 1, 1))
        right = jnp.where(column == 0, 0.0, pltpu.roll(values, 1, 1))
        xs[part, h, 0:half] = left.astype(bf16)
        xs[part, h, half : 2 * half] = values.astype(bf16)
        xs[part, h, 2 * half : 3 * half] = right.astype(bf16)

    for xs in (xs1, xs2):
        for part in range(2):
            for h in range(rows):
                xs[part, h, 3 * half :] = jnp.zeros((wide - 3 * half, lanes), bf16)

    def wait_exchange(src, dst, send, recv):
        for off in range(1, rows):
            frm = lax.rem(r + off, rows)
            remote(src, dst.at[frm], send.at[frm], recv.at[frm], rows=frm).wait_recv()

    wait_exchange(piece_of(r), x_cot, c_send, c_recv)
    for h in range(rows):
        values = x_cot[h].astype(f32)
        for part in range(2):
            store_shifts(xs2, part, h, values[part * half : (part + 1) * half])

    def conv(w, origin, xs):
        for h in range(0, rows, 2):
            total = None
            for part in range(2):
                pair = jnp.concatenate([xs[part, h], xs[part, h + 1]], axis=1)
                term = jnp.dot(w[origin, part], pair, preferred_element_type=f32)
                total = term if total is None else total + term
            y_ref[h] = total[:, :lanes]
            y_ref[h + 1] = total[:, lanes:]

    def row_of(h):
        total = y_ref[h, half : 2 * half]
        if h + 1 < rows:
            total = total + y_ref[h + 1, 0:half]
        if h > 0:
            total = total + y_ref[h - 1, 2 * half : 3 * half]
        return total

    def each_part(origin, act):
        for j in range(2):
            to = 2 * (2 * k + j) + lax.rem(origin, 2)
            slot = origin // 2

            @pl.when(to != r)
            def _():
                act(remote(
                    p1.at[origin, j], q1.at[slot, c], p_send.at[origin, j], p_recv.at[slot, c], rows=to
                ))

            yield j, to, slot

    def conv_two(origin):
        conv(w2, origin, xs2)
        for h in range(0, rows, 2):
            low, high = row_of(h), row_of(h + 1)
            for j in range(2):
                both = [low[j * GSIZE : (j + 1) * GSIZE], high[j * GSIZE : (j + 1) * GSIZE]]
                p1[origin, j, h // 2] = jnp.concatenate(both, axis=0).astype(bf16)
        for j, to, slot in each_part(origin, lambda copy: copy.start()):
            @pl.when(to == r)
            def _():
                q1[slot, c] = p1[origin, j]

    def conv_one(origin):
        conv(w1, origin, xs1)
        for h in range(rows):
            p2[origin, h] = row_of(h).astype(bf16)
        for off in range(1, rows):
            to = lax.rem(r + off, rows)
            remote(p2.at[origin, to], q2.at[origin, r], o_send.at[origin, to], o_recv.at[origin, r], rows=to).start()
        q2[origin, r] = p2[origin, r]

    near = jnp.minimum(d, depth - 1 - d)

    def nth(step):
        value = step - near if step == 1 else step
        return jnp.where(2 * d < depth, value, depth - 1 - value)

    def relay(which, w, step, last=None):
        origin = nth(step)
        for part in (k, 1 - k):
            for way in range(2):
                @pl.when((origin < d) if way == 0 else (origin > d))
                def _():
                    copy = hop(which, w, origin, part, way)
                    copy.wait_recv()

                    @pl.when(can(way))
                    def _():
                        copy.start()

        if last is not None:
            for way, end in ((0, 0), (1, depth - 1)):
                @pl.when(origin == end)
                def _():
                    for part in (k, 1 - k):
                        start_hops(1, w1, part, (way,))
        return origin

    conv_two(d)

    for frm in range(chips):
        source = 2 * frm + c // 2

        @pl.when(source != r)
        def _():
            remote(s1.at[0, 0], r1.at[frm], f_send.at[0, 0], f_recv.at[frm], rows=source).wait_recv()

    for part in range(2):
        w1[d, part, :, 3 * half :] = jnp.zeros((3 * half, wide - 3 * half), bf16)
        for j in range(2):
            for side in range(3):
                at = side * half + j * GSIZE
                w1[d, part, :, at : at + GSIZE] = r1[2 * j + part, :, side * GSIZE : (side + 1) * GSIZE]

    for way, end in ((0, 0), (1, depth - 1)):
        @pl.when(d == end)
        def _():
            for part in (k, 1 - k):
                start_hops(1, w1, part, (way,))

    conv_two(relay(0, w2, 1, True))

    def activation(normed, gain, shift):
        linear = normed * gain + shift
        logistic = 1.0 / (1.0 + jnp.exp(-linear))
        return logistic * (1.0 + linear * (1.0 - logistic)) * gain

    wait_exchange(hid_s.at[0], hid_b, h_send, h_recv)
    plain = jnp.zeros((2 * GSIZE, lanes), f32)
    square = jnp.zeros((2 * GSIZE, lanes), f32)
    for h in range(rows):
        values = hid_b[h].astype(f32)
        plain += values
        square += values * values

    def two_means(values):
        per_lane = jnp.sum(values.reshape(2, GSIZE, lanes), axis=1)
        return image_totals(per_lane) * (1.0 / number)

    average2 = two_means(plain)
    inverse2 = lax.rsqrt(two_means(square) - average2 * average2 + 1e-05)
    inv2_ref[...] = inverse2
    for slot in range(2):
        at = pl.multiple_of((k + 2 * slot) * block + GSIZE * c, GSIZE)
        gain = par_ref[pl.ds(at, GSIZE), 2:3]
        shift = par_ref[pl.ds(at, GSIZE), 3:4]
        for h in range(rows):
            values = hid_b[h].astype(f32)[slot * GSIZE : (slot + 1) * GSIZE]
            normed = (values - average2[slot : slot + 1]) * inverse2[slot : slot + 1]
            spot = (h % 2) * GSIZE
            nrm2[slot, h // 2, spot : spot + GSIZE] = normed
            act2[slot, h // 2, spot : spot + GSIZE] = activation(normed, gain, shift)

    conv_two(relay(0, w2, 2, True))

    average1, meansq1 = wait_sums(0)
    inverse1 = lax.rsqrt(meansq1 - average1 * average1 + 1e-05)
    for g in range(groups):
        rows_g = pl.ds(g * GSIZE, GSIZE)
        normed = (nrm1[rows_g, :] - average1[g : g + 1]) * inverse1[g : g + 1]
        nrm1[rows_g, :] = normed
        act1[rows_g, :] = activation(normed, par_ref[rows_g, 0:1], par_ref[rows_g, 1:2])

    for step in range(3, depth):
        conv_two(relay(0, w2, step, True))

    for slot in range(2):
        for frm in range(chips):
            source = 2 * frm + c // 2

            @pl.when(source != r)
            def _():
                remote(
                    p1.at[0, 0], q1.at[slot, frm], p_send.at[0, 0], p_recv.at[slot, frm], rows=source
                ).wait_recv()

    hg = []
    for slot in range(2):
        sum_first = jnp.zeros((2 * GSIZE, lanes), f32)
        sum_second = jnp.zeros((2 * GSIZE, lanes), f32)
        scaled = []
        for m in range(rows // 2):
            total = q1[slot, 0, m].astype(f32)
            for frm in range(1, chips):
                total = total + q1[slot, frm, m].astype(f32)
            value = total * act2[slot, m]
            scaled.append(value)
            sum_first += value
            sum_second += value * nrm2[slot, m]
        first = image_totals(jnp.sum(sum_first, axis=0, keepdims=True)) * (1.0 / number)
        second = image_totals(jnp.sum(sum_second, axis=0, keepdims=True)) * (1.0 / number)
        inverse = inv2_ref[slot : slot + 1]
        hg.append([inverse * (scaled[m] - first - nrm2[slot, m] * second) for m in range(rows // 2)])
    for h in range(rows):
        spot = (h % 2) * GSIZE
        hg_s[h] = jnp.concatenate([hg[slot][h // 2][spot : spot + GSIZE] for slot in range(2)], axis=0).astype(bf16)
    swap = remote(hg_s, hg_r, b_send.at[1], b_recv.at[1], rows=sibling)
    swap.start()
    pending.append(swap)
    for h in range(rows):
        store_shifts(xs1, k, h, hg_s[h].astype(f32))
    swap.wait_recv()
    for h in range(rows):
        store_shifts(xs1, 1 - k, h, hg_r[h].astype(f32))

    conv_one(d)
    for step in range(1, depth):
        conv_one(relay(1, w1, step))

    for origin in range(depth):
        for off in range(1, rows):
            frm = lax.rem(r + off, rows)
            remote(
                p2.at[origin, frm], q2.at[origin, frm], o_send.at[origin, frm], o_recv.at[origin, frm], rows=frm
            ).wait_recv()

    one, two = [], []
    for origin in range(depth):
        for part in range(2):
            total = q2[origin, part].astype(f32)
            for frm in range(1, chips):
                total = total + q2[origin, 2 * frm + part].astype(f32)
            at = pl.ds(origin * block + part * half, half)
            value = total * act1[at, :]
            act1[at, :] = value
            one.append(jnp.sum(value.reshape(2, GSIZE, lanes), axis=1))
            two.append(jnp.sum((value * nrm1[at, :]).reshape(2, GSIZE, lanes), axis=1))
    send_sums(1, pack_sums(jnp.concatenate(one, axis=0), jnp.concatenate(two, axis=0)))
    first1, second1 = wait_sums(1)
    value = spread(inverse1) * (act1[...] - spread(first1) - nrm1[...] * spread(second1))
    out_ref[...] = (cot_t[...].astype(f32) + value).astype(bf16).T

    for copy in pending:
        copy.wait_send()
    for _ in each_shuffle(lambda copy: copy.wait_send()):
        pass
    for origin in range(depth):
        for _ in each_part(origin, lambda copy: copy.wait_send()):
            pass
        for off in range(1, rows):
            to = lax.rem(r + off, rows)
            remote(
                p2.at[origin, to], q2.at[origin, r], o_send.at[origin, to], o_recv.at[origin, r], rows=to
            ).wait_send()
    for which, w in ((0, w2), (1, w1)):
        for origin in range(depth):
            for part in range(2):
                for way in range(2):
                    @pl.when(can(way) & ((origin <= d) if way == 0 else (origin >= d)))
                    def _():
                        hop(which, w, origin, part, way).wait_send()


def kernel_body(
    depth, rows,
    latent, hidden, cotangent, filter_one, filter_two, gain_one, shift_one, gain_two, shift_two,
):
    images, _, breadth, channels = latent.shape
    lanes = images * breadth
    block = channels // depth
    half = block // 2
    chips = rows // 2
    wide = -(-3 * half // 128) * 128
    narrow = -(-3 * GSIZE // 128) * 128
    groups = channels // GSIZE
    bf16, f32 = jnp.bfloat16, jnp.float32
    dma = pltpu.SemaphoreType.DMA
    out = pl.pallas_call(
        functools.partial(kernel, depth, rows, breadth),
        out_shape=jax.ShapeDtypeStruct((lanes, channels), bf16),
        in_specs=[pl.BlockSpec(memory_space=pltpu.VMEM)] * 9,
        out_specs=pl.BlockSpec(memory_space=pltpu.VMEM),
        scratch_shapes=[
            pltpu.VMEM((channels, lanes), bf16),
            pltpu.VMEM((rows, block, lanes), bf16),
            pltpu.VMEM((rows, 2 * GSIZE, lanes), bf16),
            pltpu.VMEM((rows, 2 * GSIZE, lanes), bf16),
            pltpu.VMEM((depth, 2, 3 * half, wide), bf16),
            pltpu.VMEM((depth, 2, 3 * half, wide), bf16),
            pltpu.VMEM((2, 2, 3 * half, narrow), bf16),
            pltpu.VMEM((3 * half, wide), bf16),
            pltpu.VMEM((chips, 3 * half, narrow), bf16),
            pltpu.VMEM((2, rows, wide, lanes), bf16),
            pltpu.VMEM((2, rows, wide, lanes), bf16),
            pltpu.VMEM((rows, 3 * half, lanes), f32),
            pltpu.VMEM((depth, 2, rows // 2, 2 * GSIZE, lanes), bf16),
            pltpu.VMEM((2, chips, rows // 2, 2 * GSIZE, lanes), bf16),
            pltpu.VMEM((depth, rows, half, lanes), bf16),
            pltpu.VMEM((depth, rows, half, lanes), bf16),
            pltpu.VMEM((rows, 2 * GSIZE, lanes), bf16),
            pltpu.VMEM((rows, 2 * GSIZE, lanes), bf16),
            pltpu.VMEM((channels, lanes), f32),
            pltpu.VMEM((channels, lanes), f32),
            pltpu.VMEM((2, rows // 2, 2 * GSIZE, lanes), f32),
            pltpu.VMEM((2, rows // 2, 2 * GSIZE, lanes), f32),
            pltpu.VMEM((2, lanes), f32),
            pltpu.VMEM((2, groups, lanes), f32),
            pltpu.VMEM((2, rows, groups, lanes), f32),
            pltpu.VMEM((channels, 8), f32),
            dma((2, 2, depth, 2)), dma((2, depth, 2)),
            dma((2, 2)), dma((chips,)),
            dma((2,)), dma((2,)),
            dma((rows,)), dma((rows,)),
            dma((rows,)), dma((rows,)),
            dma((depth, 2)), dma((2, chips)),
            dma((2,)), dma((2,)),
            dma((depth, rows)), dma((depth, rows)),
            dma((2, rows)), dma((2, rows)),
        ],
        compiler_params=pltpu.CompilerParams(collective_id=0, has_side_effects=True),
    )(
        latent.reshape(lanes, channels), hidden.reshape(lanes, channels),
        cotangent.reshape(lanes, channels), filter_one, filter_two,
        gain_one, shift_one, gain_two, shift_two,
    )
    return out.reshape(latent.shape)


def solution(mesh):
    depth, rows = mesh.shape["dp"], mesh.shape["rows"]
    in_specs = (
        P("dp", "rows", None, None),
        P("dp", "rows", None, None),
        P("dp", "rows", None, None),
        P(None, "dp", "rows"),
        P(None, "dp", "rows"),
        P(),
        P(),
        P(),
        P(),
    )

    def body(latent, *rest):
        images, rows_here, breadth, channels = latent.shape
        fits = (
            rows_here == 1
            and images * breadth == 128
            and breadth % 4 == 0
            and depth == 4
            and rows == 2 * depth
            and channels == GROUPS * GSIZE
            and channels == depth * (rows // 2) * GSIZE
        )
        if fits:
            return kernel_body(depth, rows, latent, *rest)
        return plain_body(latent, *rest)

    return jax.shard_map(
        body, mesh=mesh, in_specs=in_specs, out_specs=P("dp", "rows", None, None), check_vma=False
    )
```

```python
import functools

import jax
import jax.numpy as jnp
from jax import lax
from jax.experimental import pallas as pl
from jax.experimental.pallas import tpu as pltpu
from jax.sharding import PartitionSpec as P

GROUPS = 16
GSIZE = 40
TAPS = 9
MESH = pl.DeviceIdType.MESH


def extended(block, sides, width):
    for axis, dim in sides:
        count = lax.axis_size(axis)
        forward = [(i, i + 1) for i in range(count - 1)]
        backward = [(target, source) for source, target in forward]
        low = lax.ppermute(
            lax.slice_in_dim(block, block.shape[dim] - width, None, axis=dim), axis, forward
        )
        high = lax.ppermute(lax.slice_in_dim(block, 0, width, axis=dim), axis, backward)
        block = jnp.concatenate([low, block, high], axis=dim)
    return block


def group_sums(values):
    per_channel = jnp.sum(values, axis=(1, 2))
    return jnp.sum(per_channel.reshape(per_channel.shape[0], GROUPS, -1), axis=2)


def expand_groups(moment):
    return jnp.repeat(moment, GSIZE, axis=1)[:, None, None, :]


def finish_stats(sum_plain, sum_square, number):
    average = sum_plain / number
    variance = sum_square / number - average * average
    return (average, lax.rsqrt(variance + 1e-05))


def reduced_stats(field, number):
    values = field.astype(jnp.float32)
    sum_plain, sum_square = lax.psum((group_sums(values), group_sums(values * values)), "rows")
    return finish_stats(sum_plain, sum_square, number)


def norm_backward(field, stats, gain, shift, incoming, number):
    average, inverse = stats
    values = field.astype(jnp.float32)
    normed = (values - expand_groups(average)) * expand_groups(inverse)
    linear = normed * gain + shift
    logistic = jax.nn.sigmoid(linear)
    scaled = incoming * logistic * (1.0 + linear * (1.0 - logistic)) * gain
    sum_first, sum_second = lax.psum((group_sums(scaled), group_sums(scaled * normed)), "rows")
    first = sum_first / number
    second = sum_second / number
    return expand_groups(inverse) * (scaled - expand_groups(first) - normed * expand_groups(second))


def conv_backward(gradient, weights):
    images, rows_here, breadth, channels = gradient.shape
    padded = extended(gradient, (("rows", 1),), 1)
    padded = jnp.pad(padded, ((0, 0), (0, 0), (1, 1), (0, 0)))
    pixels = images * rows_here * breadth
    shifted = []
    for tap_index in range(9):
        down_step = tap_index // 3 - 1
        side_step = tap_index % 3 - 1
        window = padded[
            :, 1 - down_step : 1 - down_step + rows_here, 1 - side_step : 1 - side_step + breadth, :
        ]
        shifted.append(window.reshape(pixels, channels))
    stacked = jnp.stack(shifted, axis=1)
    gathered = lax.all_gather(weights, "dp", axis=1, tiled=True)
    section = lax.all_gather(gathered, "rows", axis=2, tiled=True)
    columns = section.shape[2]
    window = stacked.reshape(pixels, 9 * columns)
    flat = jnp.transpose(section, (0, 2, 1)).reshape(9 * columns, section.shape[1])
    result = jnp.dot(window, flat, preferred_element_type=jnp.float32)
    return result.reshape(images, rows_here, breadth, channels)


def plain_body(
    latent, hidden, cotangent, filter_one, filter_two, gain_one, shift_one, gain_two, shift_two
):
    number = latent.shape[1] * lax.axis_size("rows") * latent.shape[2] * GSIZE
    stats_two = reduced_stats(hidden, number)
    back_two = conv_backward(cotangent, filter_two)
    hidden_grad = norm_backward(hidden, stats_two, gain_two, shift_two, back_two, number).astype(
        jnp.bfloat16
    )
    stats_one = reduced_stats(latent, number)
    back_one = conv_backward(hidden_grad, filter_one)
    latent_part = norm_backward(latent, stats_one, gain_one, shift_one, back_one, number)
    return (cotangent.astype(jnp.float32) + latent_part).astype(jnp.bfloat16)


def kernel(
    depth, rows, breadth,
    lat_hbm, hid_hbm, cot_hbm, raw1_hbm, raw2_hbm, gain1_hbm, shift1_hbm, gain2_hbm, shift2_hbm,
    out_ref,
    lat_ref, hid_ref, cot_ref, raw1, raw2, gain1, shift1, gain2, shift2, in_sem,
    cot_t, x_cot, hid_s, hid_b, w1, w2, s1, s2, r1,
    xs1, xs2, y_ref, p1, q1, p2, q2, hg_s, hg_r,
    nrm1, act1, nrm2, act2, inv2_ref, st_s, st_b, par_ref,
    z_send, z_recv, f_send, f_recv, b_send, b_recv, c_send, c_recv, h_send, h_recv,
    p_send, p_recv, o_send, o_recv, t_send, t_recv,
):
    d = lax.axis_index("dp")
    r = lax.axis_index("rows")
    chips = rows // 2
    c = r // 2
    k = lax.rem(r, 2)
    sibling = r + 1 - 2 * k
    channels, lanes = cot_t.shape
    block = channels // depth
    half = block // 2
    images = lanes // breadth
    wide = w1.shape[3]
    number = rows * breadth * GSIZE
    groups = channels // GSIZE
    bf16, f32 = jnp.bfloat16, jnp.float32

    def remote(src, dst, send, recv, **device):
        return pltpu.make_async_remote_copy(
            src_ref=src, dst_ref=dst, send_sem=send, recv_sem=recv,
            device_id=device, device_id_type=MESH,
        )

    barrier = pltpu.get_barrier_semaphore()

    @pl.when(d > 0)
    def _():
        pl.semaphore_signal(barrier, inc=1, device_id={"dp": d - 1}, device_id_type=MESH)

    @pl.when(d < depth - 1)
    def _():
        pl.semaphore_signal(barrier, inc=1, device_id={"dp": d + 1}, device_id_type=MESH)

    for off in range(1, rows):
        pl.semaphore_signal(barrier, inc=1, device_id={"rows": lax.rem(r + off, rows)}, device_id_type=MESH)

    pending = []
    loads = {
        name: pltpu.make_async_copy(src, dst, in_sem.at[index])
        for index, (name, src, dst) in enumerate((
            ("raw2", raw2_hbm, raw2), ("cot", cot_hbm, cot_ref), ("hid", hid_hbm, hid_ref),
            ("raw1", raw1_hbm, raw1), ("lat", lat_hbm, lat_ref), ("gain1", gain1_hbm, gain1),
            ("shift1", shift1_hbm, shift1), ("gain2", gain2_hbm, gain2), ("shift2", shift2_hbm, shift2),
        ))
    }
    for load in loads.values():
        load.start()

    pad = wide - 3 * half
    own = k == c // 2
    w2[d, k, :, 3 * half :] = jnp.zeros((3 * half, pad), bf16)
    s2[:, 3 * half :] = jnp.zeros((3 * half, pad), bf16)
    for part in range(2):
        w1[d, part, :, 3 * half :] = jnp.zeros((3 * half, pad), bf16)
        for side_core in range(2):
            s1[part, side_core, :, 3 * GSIZE :] = jnp.zeros((3 * half, s1.shape[3] - 3 * GSIZE), bf16)
    for xs in (xs1, xs2):
        for part in range(2):
            for h in range(rows):
                xs[part, h, 3 * half :] = jnp.zeros((pad, lanes), bf16)
    loads["raw2"].wait()

    def arrange(ready, raw, which):
        start = pl.multiple_of(which * half, 16)
        for tap in range(TAPS):
            down, side = tap // 3, tap % 3
            ready[down * half : (down + 1) * half, side * half : (side + 1) * half] = raw[
                tap, pl.ds(start, half), :
            ]

    arrange(w2.at[d, k], raw2, k)
    arrange(s2, raw2, 1 - k)

    beside = jnp.where((d > 0) & (d < depth - 1), 2, 1)
    pl.semaphore_wait(barrier, rows - 1 + beside)

    segments = ((0, 128), (128, 3 * half))

    def hop(which, w, origin, part, seg, way):
        low, high = segments[seg]
        piece = w.at[origin, part, low:high]
        return remote(
            piece, piece, z_send.at[which, way], z_recv.at[which, origin, part, seg], dp=d + 1 - 2 * way
        )

    middle = (d > 0) & (d < depth - 1)
    near = jnp.minimum(d, depth - 1 - d)

    def nth(step):
        value = step - near if step == 1 else step
        return jnp.where(2 * d < depth, value, depth - 1 - value)

    def start_hops(which, w, part, ways=(0, 1)):
        for way in ways:
            @pl.when((d < depth - 1) if way == 0 else (d > 0))
            def _():
                for seg in range(2):
                    hop(which, w, d, part, seg, way).start()

    def forward(which, w, step, index):
        origin = nth(step)
        part, seg = (k, 1 - k)[index // 2], index % 2
        for way in range(2):
            @pl.when(middle & ((origin < d) if way == 0 else (origin > d)))
            def _():
                copy = hop(which, w, origin, part, seg, way)
                copy.wait_recv()
                copy.start()

    def take(which, w, step):
        origin = nth(step)

        @pl.when(jnp.logical_not(middle))
        def _():
            for part in (k, 1 - k):
                for seg in range(2):
                    hop(which, w, origin, part, seg, 0).wait_recv()

        return origin

    def wait_hops(which, w):
        for here in range(depth):
            for way, low, high in ((0, 0, here + 1), (1, here, depth)):
                if (way == 0 and here < depth - 1) or (way == 1 and here > 0):
                    @pl.when(d == here)
                    def _():
                        span = w.at[low:high]
                        remote(
                            span, span, z_send.at[which, way], z_recv.at[which, 0, 0, 0], dp=d + 1 - 2 * way
                        ).wait_send()

    start_hops(0, w2, k)
    twin = remote(s2, w2.at[d, k], b_send.at[0], b_recv.at[0], rows=sibling)
    twin.start()
    pending.append(twin)

    loads["cot"].wait()
    cot_t[...] = cot_ref[...].T

    def piece_of(to):
        return cot_t.at[pl.ds(pl.multiple_of((to // 2) * block, block), block), :]

    for off in range(1, rows):
        to = lax.rem(r + off, rows)
        remote(piece_of(to), x_cot.at[r], c_send.at[0], c_recv.at[0], rows=to).start()
    x_cot[r] = piece_of(r)[...]

    loads["hid"].wait()
    hid_full = hid_ref[...].astype(f32).T
    for to in range(rows):
        parts = [
            hid_full[block * b + GSIZE * (to // 2) : block * b + GSIZE * (to // 2 + 1)]
            for b in (to % 2, to % 2 + 2)
        ]
        hid_s[to] = jnp.concatenate(parts, axis=0).astype(bf16)
    for off in range(1, rows):
        to = lax.rem(r + off, rows)
        remote(hid_s.at[to], hid_b.at[r], h_send.at[0], h_recv.at[0], rows=to).start()
    hid_b[r] = hid_s[r]

    remote(s2, w2.at[d, 1 - k], b_send.at[0], b_recv.at[0], rows=sibling).wait_recv()
    start_hops(0, w2, 1 - k)

    loads["raw1"].wait()
    for part in range(2):
        for side_core in range(2):
            ready = s1.at[part, side_core]
            for tap in range(TAPS):
                down, side = tap // 3, tap % 3
                ready[down * half : (down + 1) * half, side * GSIZE : (side + 1) * GSIZE] = raw1[
                    tap, side_core * half : (side_core + 1) * half, part * GSIZE : (part + 1) * GSIZE
                ]

    for part in range(2):
        for side_core in range(2):
            to = 2 * (2 * k + part) + side_core

            @pl.when(to != r)
            def _():
                remote(s1.at[part, side_core], r1.at[c], f_send.at[0], f_recv.at[0], rows=to).start()

            @pl.when(to == r)
            def _():
                r1[c] = s1[part, side_core]

    forward(0, w2, 1, 0)
    forward(0, w2, 2, 0)
    loads["lat"].wait()
    lane = lax.broadcasted_iota(jnp.int32, (1, lanes), 1)
    column = lax.rem(lane, breadth)
    image_of = lax.div(lane, breadth)
    quarter = lax.rem(lane, breadth) // (breadth // 4)

    def image_totals(per_lane):
        total = jnp.zeros_like(per_lane)
        for image in range(images):
            mine = image_of == image
            part = jnp.sum(jnp.where(mine, per_lane, 0.0), axis=1, keepdims=True)
            total = jnp.where(mine, part, total)
        return total

    def pack_sums(one, two):
        one, two = image_totals(one), image_totals(two)
        top, low = slice(0, groups // 2), slice(groups // 2, groups)
        return jnp.where(
            quarter == 0, one[top], jnp.where(quarter == 1, two[top], jnp.where(quarter == 2, one[low], two[low]))
        )

    def send_sums(which, packed):
        st_s[which] = packed
        for off in range(1, rows):
            to = lax.rem(r + off, rows)
            remote(st_s.at[which], st_b.at[which, r], t_send.at[which], t_recv.at[which], rows=to).start()
        st_b[which, r] = packed

    def wait_sums(which):
        span = st_b.at[which, 0 : rows - 1]
        remote(span, span, t_send.at[which], t_recv.at[which], rows=sibling).wait_recv()
        total = st_b[which, 0]
        for h in range(1, rows):
            total = total + st_b[which, h]
        total = total * (1.0 / number)
        full = []
        for at in range(4):
            mine = jnp.where(quarter == at, total, 0.0)
            pair = mine + pltpu.roll(mine, ((1 if at % 2 == 0 else -1) * breadth // 4) % lanes, 1)
            full.append(pair + pltpu.roll(pair, ((1 if at < 2 else -1) * breadth // 2) % lanes, 1))
        return jnp.concatenate([full[0], full[2]], axis=0), jnp.concatenate([full[1], full[3]], axis=0)

    def spread(moment):
        return jnp.broadcast_to(moment[:, None, :], (groups, GSIZE, lanes)).reshape(channels, lanes)

    def by_group(values):
        return jnp.sum(values.reshape(groups, GSIZE, lanes), axis=1)

    nrm1[...] = lat_ref[...].astype(f32).T
    send_sums(0, pack_sums(by_group(nrm1[...]), by_group(nrm1[...] * nrm1[...])))

    for name in ("gain1", "shift1", "gain2", "shift2"):
        loads[name].wait()
    raw_params = [p[...].reshape(1, channels) for p in (gain1, shift1, gain2, shift2)]
    par_ref[...] = jnp.concatenate(raw_params + raw_params, axis=0).T

    def store_shifts(xs, part, h, values):
        left = jnp.where(column == breadth - 1, 0.0, pltpu.roll(values, lanes - 1, 1))
        right = jnp.where(column == 0, 0.0, pltpu.roll(values, 1, 1))
        xs[part, h, 0:half] = left.astype(bf16)
        xs[part, h, half : 2 * half] = values.astype(bf16)
        xs[part, h, 2 * half : 3 * half] = right.astype(bf16)

    def wait_group(src, dst, send, recv):
        remote(src, dst, send, recv, rows=sibling).wait_recv()

    forward(0, w2, 1, 1)
    forward(0, w2, 2, 1)
    everyone = x_cot.at[0 : rows - 1]
    wait_group(everyone, everyone, c_send.at[0], c_recv.at[0])
    for h in range(rows):
        values = x_cot[h].astype(f32)
        for part in range(2):
            store_shifts(xs2, part, h, values[part * half : (part + 1) * half])

    def conv(w, origin, xs):
        for h in range(0, rows, 2):
            total = None
            for part in range(2):
                pair = jnp.concatenate([xs[part, h], xs[part, h + 1]], axis=1)
                term = jnp.dot(w[origin, part], pair, preferred_element_type=f32)
                total = term if total is None else total + term
            y_ref[h] = total[:, :lanes]
            y_ref[h + 1] = total[:, lanes:]

    def row_of(h):
        total = y_ref[h, half : 2 * half]
        if h + 1 < rows:
            total = total + y_ref[h + 1, 0:half]
        if h > 0:
            total = total + y_ref[h - 1, 2 * half : 3 * half]
        return total

    def conv_two(origin):
        conv(w2, origin, xs2)
        for h in range(0, rows, 2):
            low, high = row_of(h), row_of(h + 1)
            for j in range(2):
                both = [low[j * GSIZE : (j + 1) * GSIZE], high[j * GSIZE : (j + 1) * GSIZE]]
                p1[origin, j, h // 2] = jnp.concatenate(both, axis=0).astype(bf16)
        slot = origin // 2
        for j in range(2):
            to = 2 * (2 * k + j) + lax.rem(origin, 2)

            @pl.when(to != r)
            def _():
                remote(p1.at[origin, j], q1.at[slot, c], p_send.at[0], p_recv.at[slot], rows=to).start()

            @pl.when(to == r)
            def _():
                q1[slot, c] = p1[origin, j]

    def conv_one(origin):
        conv(w1, origin, xs1)
        for h in range(rows):
            p2[origin, h] = row_of(h).astype(bf16)
        for off in range(1, rows):
            to = lax.rem(r + off, rows)
            remote(p2.at[origin, to], q2.at[origin, r], o_send.at[0], o_recv.at[origin], rows=to).start()
        q2[origin, r] = p2[origin, r]

    forward(0, w2, 1, 2)
    forward(0, w2, 2, 2)
    conv_two(d)
    forward(0, w2, 1, 3)
    forward(0, w2, 2, 3)
    take(0, w2, 1)
    conv_two(nth(1))

    def activation(normed, gain, shift):
        linear = normed * gain + shift
        logistic = 1.0 / (1.0 + jnp.exp(-linear))
        return logistic * (1.0 + linear * (1.0 - logistic)) * gain

    everyone = hid_b.at[0 : rows - 1]
    wait_group(everyone, everyone, h_send.at[0], h_recv.at[0])
    plain = jnp.zeros((2 * GSIZE, lanes), f32)
    square = jnp.zeros((2 * GSIZE, lanes), f32)
    for h in range(rows):
        values = hid_b[h].astype(f32)
        plain += values
        square += values * values

    def two_means(values):
        per_lane = jnp.sum(values.reshape(2, GSIZE, lanes), axis=1)
        return image_totals(per_lane) * (1.0 / number)

    average2 = two_means(plain)
    inverse2 = lax.rsqrt(two_means(square) - average2 * average2 + 1e-05)
    inv2_ref[...] = inverse2
    for slot in range(2):
        at = pl.multiple_of((k + 2 * slot) * block + GSIZE * c, GSIZE)
        gain = par_ref[pl.ds(at, GSIZE), 2:3]
        shift = par_ref[pl.ds(at, GSIZE), 3:4]
        for h in range(rows):
            values = hid_b[h].astype(f32)[slot * GSIZE : (slot + 1) * GSIZE]
            normed = (values - average2[slot : slot + 1]) * inverse2[slot : slot + 1]
            spot = (h % 2) * GSIZE
            nrm2[slot, h // 2, spot : spot + GSIZE] = normed
            act2[slot, h // 2, spot : spot + GSIZE] = activation(normed, gain, shift)

    forward(0, w2, 3, 0)
    for count, here in ((chips - 1, own), (chips, jnp.logical_not(own))):
        @pl.when(here)
        def _():
            span = r1.at[0:count]
            wait_group(span, span, f_send.at[0], f_recv.at[0])

    for part in range(2):
        for j in range(2):
            for side in range(3):
                at = side * half + j * GSIZE
                w1[d, part, :, at : at + GSIZE] = r1[2 * j + part, :, side * GSIZE : (side + 1) * GSIZE]

    for way, here in ((0, 2 * d < depth), (1, 2 * d >= depth)):
        @pl.when(here)
        def _():
            for part in (k, 1 - k):
                start_hops(1, w1, part, (way,))

    forward(0, w2, 3, 1)
    take(0, w2, 2)
    conv_two(nth(2))
    forward(0, w2, 3, 2)
    forward(0, w2, 3, 3)
    for way, here in ((0, 2 * d >= depth), (1, 2 * d < depth)):
        @pl.when(here)
        def _():
            for part in (k, 1 - k):
                start_hops(1, w1, part, (way,))

    take(0, w2, 3)
    conv_two(nth(3))

    average1, meansq1 = wait_sums(0)
    inverse1 = lax.rsqrt(meansq1 - average1 * average1 + 1e-05)
    for g in range(groups):
        rows_g = pl.ds(g * GSIZE, GSIZE)
        normed = (nrm1[rows_g, :] - average1[g : g + 1]) * inverse1[g : g + 1]
        nrm1[rows_g, :] = normed
        act1[rows_g, :] = activation(normed, par_ref[rows_g, 0:1], par_ref[rows_g, 1:2])

    for index in range(4):
        forward(1, w1, 1, index)
        forward(1, w1, 2, index)

    for count, here in ((chips - 1, own), (chips, jnp.logical_not(own))):
        @pl.when(here)
        def _():
            for slot in range(2):
                span = q1.at[slot, 0:count]
                wait_group(span, span, p_send.at[0], p_recv.at[slot])

    hg = []
    for slot in range(2):
        sum_first = jnp.zeros((2 * GSIZE, lanes), f32)
        sum_second = jnp.zeros((2 * GSIZE, lanes), f32)
        scaled = []
        for m in range(rows // 2):
            total = q1[slot, 0, m].astype(f32)
            for frm in range(1, chips):
                total = total + q1[slot, frm, m].astype(f32)
            value = total * act2[slot, m]
            scaled.append(value)
            sum_first += value
            sum_second += value * nrm2[slot, m]
        first = image_totals(jnp.sum(sum_first, axis=0, keepdims=True)) * (1.0 / number)
        second = image_totals(jnp.sum(sum_second, axis=0, keepdims=True)) * (1.0 / number)
        inverse = inv2_ref[slot : slot + 1]
        hg.append([inverse * (scaled[m] - first - nrm2[slot, m] * second) for m in range(rows // 2)])
    for h in range(rows):
        spot = (h % 2) * GSIZE
        hg_s[h] = jnp.concatenate([hg[slot][h // 2][spot : spot + GSIZE] for slot in range(2)], axis=0).astype(bf16)
    swap = remote(hg_s, hg_r, b_send.at[1], b_recv.at[1], rows=sibling)
    swap.start()
    pending.append(swap)
    for h in range(rows):
        store_shifts(xs1, k, h, hg_s[h].astype(f32))
    swap.wait_recv()
    for h in range(rows):
        store_shifts(xs1, 1 - k, h, hg_r[h].astype(f32))

    forward(1, w1, 3, 0)
    conv_one(d)
    forward(1, w1, 3, 1)
    take(1, w1, 1)
    conv_one(nth(1))
    forward(1, w1, 3, 2)
    take(1, w1, 2)
    conv_one(nth(2))
    forward(1, w1, 3, 3)
    take(1, w1, 3)
    conv_one(nth(3))
    for origin in range(depth):
        span = q2.at[origin, 0 : rows - 1]
        wait_group(span, span, o_send.at[0], o_recv.at[origin])

    one, two = [], []
    for origin in range(depth):
        for part in range(2):
            total = q2[origin, part].astype(f32)
            for frm in range(1, chips):
                total = total + q2[origin, 2 * frm + part].astype(f32)
            at = pl.ds(origin * block + part * half, half)
            value = total * act1[at, :]
            act1[at, :] = value
            one.append(jnp.sum(value.reshape(2, GSIZE, lanes), axis=1))
            two.append(jnp.sum((value * nrm1[at, :]).reshape(2, GSIZE, lanes), axis=1))
    send_sums(1, pack_sums(jnp.concatenate(one, axis=0), jnp.concatenate(two, axis=0)))
    first1, second1 = wait_sums(1)
    value = spread(inverse1) * (act1[...] - spread(first1) - nrm1[...] * spread(second1))
    out_ref[...] = (cot_t[...].astype(f32) + value).astype(bf16).T

    for copy in pending:
        copy.wait_send()
    def sent(span, send, recv):
        remote(span, span, send, recv, rows=sibling).wait_send()

    sent(x_cot.at[0 : rows - 1], c_send.at[0], c_recv.at[0])
    sent(hid_b.at[0 : rows - 1], h_send.at[0], h_recv.at[0])
    for which in range(2):
        sent(st_b.at[which, 0 : rows - 1], t_send.at[which], t_recv.at[which])
    sent(p2.at[:, 0 : rows - 1], o_send.at[0], o_recv.at[0])
    for count, here in ((chips - 1, own), (chips, jnp.logical_not(own))):
        @pl.when(here)
        def _():
            sent(r1.at[0:count], f_send.at[0], f_recv.at[0])
            sent(q1.at[:, 0:count], p_send.at[0], p_recv.at[0])

    wait_hops(0, w2)
    wait_hops(1, w1)


def kernel_body(
    depth, rows,
    latent, hidden, cotangent, filter_one, filter_two, gain_one, shift_one, gain_two, shift_two,
):
    images, _, breadth, channels = latent.shape
    lanes = images * breadth
    block = channels // depth
    half = block // 2
    chips = rows // 2
    wide = -(-3 * half // 128) * 128
    narrow = -(-3 * GSIZE // 128) * 128
    groups = channels // GSIZE
    bf16, f32 = jnp.bfloat16, jnp.float32
    dma = pltpu.SemaphoreType.DMA
    out = pl.pallas_call(
        functools.partial(kernel, depth, rows, breadth),
        out_shape=jax.ShapeDtypeStruct((lanes, channels), bf16),
        in_specs=[pl.BlockSpec(memory_space=pltpu.HBM)] * 9,
        out_specs=pl.BlockSpec(memory_space=pltpu.VMEM),
        scratch_shapes=[
            pltpu.VMEM((lanes, channels), bf16),
            pltpu.VMEM((lanes, channels), bf16),
            pltpu.VMEM((lanes, channels), bf16),
            pltpu.VMEM(filter_one.shape, bf16),
            pltpu.VMEM(filter_two.shape, bf16),
            pltpu.VMEM((channels,), f32),
            pltpu.VMEM((channels,), f32),
            pltpu.VMEM((channels,), f32),
            pltpu.VMEM((channels,), f32),
            dma((9,)),
            pltpu.VMEM((channels, lanes), bf16),
            pltpu.VMEM((rows, block, lanes), bf16),
            pltpu.VMEM((rows, 2 * GSIZE, lanes), bf16),
            pltpu.VMEM((rows, 2 * GSIZE, lanes), bf16),
            pltpu.VMEM((depth, 2, 3 * half, wide), bf16),
            pltpu.VMEM((depth, 2, 3 * half, wide), bf16),
            pltpu.VMEM((2, 2, 3 * half, narrow), bf16),
            pltpu.VMEM((3 * half, wide), bf16),
            pltpu.VMEM((chips, 3 * half, narrow), bf16),
            pltpu.VMEM((2, rows, wide, lanes), bf16),
            pltpu.VMEM((2, rows, wide, lanes), bf16),
            pltpu.VMEM((rows, 3 * half, lanes), f32),
            pltpu.VMEM((depth, 2, rows // 2, 2 * GSIZE, lanes), bf16),
            pltpu.VMEM((2, chips, rows // 2, 2 * GSIZE, lanes), bf16),
            pltpu.VMEM((depth, rows, half, lanes), bf16),
            pltpu.VMEM((depth, rows, half, lanes), bf16),
            pltpu.VMEM((rows, 2 * GSIZE, lanes), bf16),
            pltpu.VMEM((rows, 2 * GSIZE, lanes), bf16),
            pltpu.VMEM((channels, lanes), f32),
            pltpu.VMEM((channels, lanes), f32),
            pltpu.VMEM((2, rows // 2, 2 * GSIZE, lanes), f32),
            pltpu.VMEM((2, rows // 2, 2 * GSIZE, lanes), f32),
            pltpu.VMEM((2, lanes), f32),
            pltpu.VMEM((2, groups // 2, lanes), f32),
            pltpu.VMEM((2, rows, groups // 2, lanes), f32),
            pltpu.VMEM((channels, 8), f32),
            dma((2, 2)), dma((2, depth, 2, 2)),
            dma((1,)), dma((1,)),
            dma((2,)), dma((2,)),
            dma((1,)), dma((1,)),
            dma((1,)), dma((1,)),
            dma((1,)), dma((2,)),
            dma((1,)), dma((depth,)),
            dma((2,)), dma((2,)),
        ],
        compiler_params=pltpu.CompilerParams(
            collective_id=0, has_side_effects=True
        ),
    )(
        latent.reshape(lanes, channels), hidden.reshape(lanes, channels),
        cotangent.reshape(lanes, channels), filter_one, filter_two,
        gain_one, shift_one, gain_two, shift_two,
    )
    return out.reshape(latent.shape)


def solution(mesh):
    depth, rows = mesh.shape["dp"], mesh.shape["rows"]
    in_specs = (
        P("dp", "rows", None, None),
        P("dp", "rows", None, None),
        P("dp", "rows", None, None),
        P(None, "dp", "rows"),
        P(None, "dp", "rows"),
        P(),
        P(),
        P(),
        P(),
    )

    def body(latent, *rest):
        images, rows_here, breadth, channels = latent.shape
        fits = (
            rows_here == 1
            and images * breadth == 128
            and breadth % 4 == 0
            and depth == 4
            and rows == 2 * depth
            and channels == GROUPS * GSIZE
            and channels == depth * (rows // 2) * GSIZE
        )
        if fits:
            return kernel_body(depth, rows, latent, *rest)
        return plain_body(latent, *rest)

    return jax.shard_map(
        body, mesh=mesh, in_specs=in_specs, out_specs=P("dp", "rows", None, None), check_vma=False
    )
```

```python
import functools

import jax
import jax.numpy as jnp
from jax import lax
from jax.experimental import pallas as pl
from jax.experimental.pallas import tpu as pltpu
from jax.sharding import PartitionSpec as P

GROUPS = 16
GSIZE = 40
TAPS = 9
MESH = pl.DeviceIdType.MESH


def extended(block, sides, width):
    for axis, dim in sides:
        count = lax.axis_size(axis)
        forward = [(i, i + 1) for i in range(count - 1)]
        backward = [(target, source) for source, target in forward]
        low = lax.ppermute(
            lax.slice_in_dim(block, block.shape[dim] - width, None, axis=dim), axis, forward
        )
        high = lax.ppermute(lax.slice_in_dim(block, 0, width, axis=dim), axis, backward)
        block = jnp.concatenate([low, block, high], axis=dim)
    return block


def group_sums(values):
    per_channel = jnp.sum(values, axis=(1, 2))
    return jnp.sum(per_channel.reshape(per_channel.shape[0], GROUPS, -1), axis=2)


def expand_groups(moment):
    return jnp.repeat(moment, GSIZE, axis=1)[:, None, None, :]


def finish_stats(sum_plain, sum_square, number):
    average = sum_plain / number
    variance = sum_square / number - average * average
    return (average, lax.rsqrt(variance + 1e-05))


def reduced_stats(field, number):
    values = field.astype(jnp.float32)
    sum_plain, sum_square = lax.psum((group_sums(values), group_sums(values * values)), "rows")
    return finish_stats(sum_plain, sum_square, number)


def norm_backward(field, stats, gain, shift, incoming, number):
    average, inverse = stats
    values = field.astype(jnp.float32)
    normed = (values - expand_groups(average)) * expand_groups(inverse)
    linear = normed * gain + shift
    logistic = jax.nn.sigmoid(linear)
    scaled = incoming * logistic * (1.0 + linear * (1.0 - logistic)) * gain
    sum_first, sum_second = lax.psum((group_sums(scaled), group_sums(scaled * normed)), "rows")
    first = sum_first / number
    second = sum_second / number
    return expand_groups(inverse) * (scaled - expand_groups(first) - normed * expand_groups(second))


def conv_backward(gradient, weights):
    images, rows_here, breadth, channels = gradient.shape
    padded = extended(gradient, (("rows", 1),), 1)
    padded = jnp.pad(padded, ((0, 0), (0, 0), (1, 1), (0, 0)))
    pixels = images * rows_here * breadth
    shifted = []
    for tap_index in range(9):
        down_step = tap_index // 3 - 1
        side_step = tap_index % 3 - 1
        window = padded[
            :, 1 - down_step : 1 - down_step + rows_here, 1 - side_step : 1 - side_step + breadth, :
        ]
        shifted.append(window.reshape(pixels, channels))
    stacked = jnp.stack(shifted, axis=1)
    gathered = lax.all_gather(weights, "dp", axis=1, tiled=True)
    section = lax.all_gather(gathered, "rows", axis=2, tiled=True)
    columns = section.shape[2]
    window = stacked.reshape(pixels, 9 * columns)
    flat = jnp.transpose(section, (0, 2, 1)).reshape(9 * columns, section.shape[1])
    result = jnp.dot(window, flat, preferred_element_type=jnp.float32)
    return result.reshape(images, rows_here, breadth, channels)


def plain_body(
    latent, hidden, cotangent, filter_one, filter_two, gain_one, shift_one, gain_two, shift_two
):
    number = latent.shape[1] * lax.axis_size("rows") * latent.shape[2] * GSIZE
    stats_two = reduced_stats(hidden, number)
    back_two = conv_backward(cotangent, filter_two)
    hidden_grad = norm_backward(hidden, stats_two, gain_two, shift_two, back_two, number).astype(
        jnp.bfloat16
    )
    stats_one = reduced_stats(latent, number)
    back_one = conv_backward(hidden_grad, filter_one)
    latent_part = norm_backward(latent, stats_one, gain_one, shift_one, back_one, number)
    return (cotangent.astype(jnp.float32) + latent_part).astype(jnp.bfloat16)


def kernel(
    depth, rows, breadth,
    lat_hbm, hid_hbm, cot_hbm, raw1_hbm, raw2_hbm, gain1_hbm, shift1_hbm, gain2_hbm, shift2_hbm,
    out_ref,
    lat_ref, hid_ref, cot_ref, raw1, raw2, gain1, shift1, gain2, shift2, in_sem,
    cot_t, x_cot, hid_b, w1, w2, s1, s2, r1,
    xs1, xs2, y_ref, p1, q1, p2, q2, hg_s, hg_r,
    nrm1, act1, nrm2, act2, inv2_ref, st_s, st_b, par_ref,
    x_far, hid_two, hid_far, xs_far, p_far, q_far, nrm_far, act_far, hg_far, hg_two,
    z_send, z_recv, f_send, f_recv, b_send, b_recv, c_send, c_recv, h_send, h_recv,
    p_send, p_recv, o_send, o_recv, t_send, t_recv, d_send, d_recv, e_send, e_recv,
):
    d = lax.axis_index("dp")
    r = lax.axis_index("rows")
    chips = rows // 2
    c = r // 2
    k = lax.rem(r, 2)
    sibling = r + 1 - 2 * k
    channels, lanes = cot_t.shape
    block = channels // depth
    half = block // 2
    images = lanes // breadth
    wide = w1.shape[3]
    number = rows * breadth * GSIZE
    groups = channels // GSIZE
    bf16, f32 = jnp.bfloat16, jnp.float32

    def remote(src, dst, send, recv, **device):
        return pltpu.make_async_remote_copy(
            src_ref=src, dst_ref=dst, send_sem=send, recv_sem=recv,
            device_id=device, device_id_type=MESH,
        )

    barrier = pltpu.get_barrier_semaphore()

    middle = (d > 0) & (d < depth - 1)
    partner = d + 1 - 2 * lax.rem(d, 2)
    lent = jnp.where(2 * d < depth, 1, 0)

    @pl.when(middle)
    def _():
        pl.semaphore_signal(barrier, inc=1, device_id={"dp": depth - 1 - d}, device_id_type=MESH)

    for to in range(rows):
        pl.semaphore_signal(barrier, inc=1, device_id={"dp": partner, "rows": to}, device_id_type=MESH)

    for off in range(1, rows):
        pl.semaphore_signal(barrier, inc=1, device_id={"rows": lax.rem(r + off, rows)}, device_id_type=MESH)

    pending = []
    loads = {
        name: pltpu.make_async_copy(src, dst, in_sem.at[index])
        for index, (name, src, dst) in enumerate((
            ("raw2", raw2_hbm, raw2), ("cot", cot_hbm, cot_ref), ("hid", hid_hbm, hid_ref),
            ("raw1", raw1_hbm, raw1), ("lat", lat_hbm, lat_ref), ("gain1", gain1_hbm, gain1),
            ("shift1", shift1_hbm, shift1), ("gain2", gain2_hbm, gain2), ("shift2", shift2_hbm, shift2),
        ))
    }
    for load in loads.values():
        load.start()

    pad = wide - 3 * half
    own = k == c // 2
    w2[d, k, :, 3 * half :] = jnp.zeros((3 * half, pad), bf16)
    s2[:, 3 * half :] = jnp.zeros((3 * half, pad), bf16)
    for part in range(2):
        w1[d, part, :, 3 * half :] = jnp.zeros((3 * half, pad), bf16)
        for side_core in range(2):
            s1[part, side_core, :, 3 * GSIZE :] = jnp.zeros((3 * half, s1.shape[3] - 3 * GSIZE), bf16)
    for xs in (xs1, xs2, xs_far):
        for part in range(2):
            for h in range(rows):
                xs[part, h, 3 * half :] = jnp.zeros((pad, lanes), bf16)
    loads["raw2"].wait()

    def arrange(ready, raw, which):
        start = pl.multiple_of(which * half, 16)
        for tap in range(TAPS):
            down, side = tap // 3, tap % 3
            ready[down * half : (down + 1) * half, side * half : (side + 1) * half] = raw[
                tap, pl.ds(start, half), :
            ]

    arrange(w2.at[d, k], raw2, k)
    arrange(s2, raw2, 1 - k)

    pl.semaphore_wait(barrier, 2 * rows - 1 + jnp.where(middle, 1, 0))

    segments = ((0, 128), (128, 3 * half))

    def hop(which, w, origin, part, seg, way):
        low, high = segments[seg]
        piece = w.at[origin, part, low:high]
        return remote(
            piece, piece, z_send.at[which, way], z_recv.at[which, origin, part, seg], dp=d + 1 - 2 * way
        )

    near = jnp.minimum(d, depth - 1 - d)

    def nth(step):
        value = step - near if step == 1 else step
        return jnp.where(2 * d < depth, value, depth - 1 - value)

    def start_hops(which, w, part, ways=(0, 1)):
        for way in ways:
            @pl.when((d < depth - 1) if way == 0 else (d > 0))
            def _():
                for seg in range(2):
                    hop(which, w, d, part, seg, way).start()

    def forward(which, w, step, index):
        origin = nth(step)
        part, seg = (k, 1 - k)[index // 2], index % 2
        for way in range(2):
            @pl.when(middle & ((origin < d) if way == 0 else (origin > d)))
            def _():
                copy = hop(which, w, origin, part, seg, way)
                copy.wait_recv()
                copy.start()

    def take(which, w, step):
        for part in (k, 1 - k):
            for seg in range(2):
                hop(which, w, nth(step), part, seg, 0).wait_recv()

    def take_end(which, w, step):
        @pl.when(jnp.logical_not(middle))
        def _():
            take(which, w, step)

    def wait_hops(which, w, spans):
        for here, way, low, high in spans:
            @pl.when(d == here)
            def _():
                span = w.at[low:high]
                remote(
                    span, span, z_send.at[which, way], z_recv.at[which, 0, 0, 0], dp=d + 1 - 2 * way
                ).wait_send()

    start_hops(0, w2, k)
    twin = remote(s2, w2.at[d, k], b_send.at[0], b_recv.at[0], rows=sibling)
    twin.start()
    pending.append(twin)

    loads["cot"].wait()
    cot_t[...] = cot_ref[...].T

    def piece_of(to):
        return cot_t.at[pl.ds(pl.multiple_of((to // 2) * block, block), block), :]

    for off in range(1, chips):
        to = 2 * lax.rem(c + off, chips) + k
        remote(piece_of(to), x_cot.at[k, c], c_send.at[0], c_recv.at[0], rows=to).start()
    x_cot[k, c] = piece_of(r)[...]

    loads["raw1"].wait()
    for part in range(2):
        for side_core in range(2):
            ready = s1.at[part, side_core]
            for tap in range(TAPS):
                down, side = tap // 3, tap % 3
                ready[down * half : (down + 1) * half, side * GSIZE : (side + 1) * GSIZE] = raw1[
                    tap, side_core * half : (side_core + 1) * half, part * GSIZE : (part + 1) * GSIZE
                ]

    for part in range(2):
        for side_core in range(2):
            to = 2 * (2 * k + part) + side_core

            @pl.when(to != r)
            def _():
                remote(s1.at[part, side_core], r1.at[c], f_send.at[0], f_recv.at[0], rows=to).start()

            @pl.when(to == r)
            def _():
                r1[c] = s1[part, side_core]

    loads["hid"].wait()
    hid_full = hid_ref[...].astype(f32).T
    for to in range(rows):
        parts = [
            hid_full[block * b + GSIZE * (to // 2) : block * b + GSIZE * (to // 2 + 1)]
            for b in (to % 2, to % 2 + 2)
        ]
        for slot in range(2):
            hid_two[to, slot] = parts[slot].astype(bf16)
    for off in range(1, rows):
        to = lax.rem(r + off, rows)
        remote(hid_two.at[to], hid_b.at[:, r], h_send.at[0], h_recv.at[0], rows=to).start()
    hid_b[:, r] = hid_two[r]

    remote(s2, w2.at[d, 1 - k], b_send.at[0], b_recv.at[0], rows=sibling).wait_recv()
    start_hops(0, w2, 1 - k)

    forward(0, w2, 1, 0)
    loads["lat"].wait()
    lane = lax.broadcasted_iota(jnp.int32, (1, lanes), 1)
    column = lax.rem(lane, breadth)
    image_of = lax.div(lane, breadth)
    quarter = lax.rem(lane, breadth) // (breadth // 4)

    def image_totals(per_lane):
        total = jnp.zeros_like(per_lane)
        for image in range(images):
            mine = image_of == image
            part = jnp.sum(jnp.where(mine, per_lane, 0.0), axis=1, keepdims=True)
            total = jnp.where(mine, part, total)
        return total

    def pack_sums(one, two):
        one, two = image_totals(one), image_totals(two)
        top, low = slice(0, groups // 2), slice(groups // 2, groups)
        return jnp.where(
            quarter == 0, one[top], jnp.where(quarter == 1, two[top], jnp.where(quarter == 2, one[low], two[low]))
        )

    def send_sums(which, packed):
        st_s[which] = packed
        for off in range(1, rows):
            to = lax.rem(r + off, rows)
            remote(st_s.at[which], st_b.at[which, r], t_send.at[which], t_recv.at[which], rows=to).start()
        st_b[which, r] = packed

    def wait_sums(which):
        span = st_b.at[which, 0 : rows - 1]
        remote(span, span, t_send.at[which], t_recv.at[which], rows=sibling).wait_recv()
        total = st_b[which, 0]
        for h in range(1, rows):
            total = total + st_b[which, h]
        total = total * (1.0 / number)
        full = []
        for at in range(4):
            mine = jnp.where(quarter == at, total, 0.0)
            pair = mine + pltpu.roll(mine, ((1 if at % 2 == 0 else -1) * breadth // 4) % lanes, 1)
            full.append(pair + pltpu.roll(pair, ((1 if at < 2 else -1) * breadth // 2) % lanes, 1))
        return jnp.concatenate([full[0], full[2]], axis=0), jnp.concatenate([full[1], full[3]], axis=0)

    def spread(moment):
        return jnp.broadcast_to(moment[:, None, :], (groups, GSIZE, lanes)).reshape(channels, lanes)

    def by_group(values):
        return jnp.sum(values.reshape(groups, GSIZE, lanes), axis=1)

    nrm1[...] = lat_ref[...].astype(f32).T
    send_sums(0, pack_sums(by_group(nrm1[...]), by_group(nrm1[...] * nrm1[...])))

    for name in ("gain1", "shift1", "gain2", "shift2"):
        loads[name].wait()
    raw_params = [p[...].reshape(1, channels) for p in (gain1, shift1, gain2, shift2)]
    par_ref[...] = jnp.concatenate(raw_params + raw_params, axis=0).T

    def store_shifts(xs, part, h, values):
        left = jnp.where(column == breadth - 1, 0.0, pltpu.roll(values, lanes - 1, 1))
        right = jnp.where(column == 0, 0.0, pltpu.roll(values, 1, 1))
        xs[part, h, 0:half] = left.astype(bf16)
        xs[part, h, half : 2 * half] = values.astype(bf16)
        xs[part, h, 2 * half : 3 * half] = right.astype(bf16)

    def wait_group(src, dst, send, recv):
        remote(src, dst, send, recv, rows=sibling).wait_recv()

    forward(0, w2, 1, 1)
    everyone = x_cot.at[0, 0 : chips - 1]
    wait_group(everyone, everyone, c_send.at[0], c_recv.at[0])

    def share(x, at):
        return remote(x.at[k], x.at[k], d_send.at[at], d_recv.at[at], rows=sibling)

    def shift_rows(x, xs):
        for h in range(rows):
            values = x[h % 2, h // 2].astype(f32)
            for part in range(2):
                store_shifts(xs, part, h, values[part * half : (part + 1) * half])

    share(x_cot, 0).start()
    lend_cot = remote(x_cot.at[k], x_far.at[k], c_send.at[1], c_recv.at[1], dp=partner)
    lend_hid = remote(hid_b.at[lent], hid_far, h_send.at[1], h_recv.at[1], dp=partner)

    @pl.when(jnp.logical_not(middle))
    def _():
        lend_cot.start()

    forward(0, w2, 1, 2)
    share(x_cot, 0).wait_recv()
    shift_rows(x_cot, xs2)

    def conv(w, origin, xs):
        for h in range(0, rows, 2):
            total = None
            for part in range(2):
                pair = jnp.concatenate([xs[part, h], xs[part, h + 1]], axis=1)
                term = jnp.dot(w[origin, part], pair, preferred_element_type=f32)
                total = term if total is None else total + term
            y_ref[h] = total[:, :lanes]
            y_ref[h + 1] = total[:, lanes:]

    def row_of(h):
        total = y_ref[h, half : 2 * half]
        if h + 1 < rows:
            total = total + y_ref[h + 1, 0:half]
        if h > 0:
            total = total + y_ref[h - 1, 2 * half : 3 * half]
        return total

    def conv_two(origin, xs, p, q, send, recv):
        conv(w2, origin, xs)
        for h in range(0, rows, 2):
            low, high = row_of(h), row_of(h + 1)
            for j in range(2):
                both = [low[j * GSIZE : (j + 1) * GSIZE], high[j * GSIZE : (j + 1) * GSIZE]]
                p[j, h // 2] = jnp.concatenate(both, axis=0).astype(bf16)
        for j in range(2):
            to = 2 * (2 * k + j) + lax.rem(origin, 2)

            @pl.when(to != r)
            def _():
                remote(p.at[j], q.at[c], send, recv, rows=to).start()

            @pl.when(to == r)
            def _():
                q[c] = p[j]

    def conv_own(origin):
        slot = origin // 2
        conv_two(origin, xs2, p1.at[origin], q1.at[slot], p_send.at[0], p_recv.at[slot])

    def conv_far(step):
        conv_two(nth(step), xs_far, p_far.at[step - 2], q_far, p_send.at[1], p_recv.at[2])

    def conv_one(origin):
        conv(w1, origin, xs1)
        for h in range(rows):
            p2[origin, h] = row_of(h).astype(bf16)
        for off in range(1, rows):
            to = lax.rem(r + off, rows)
            remote(p2.at[origin, to], q2.at[origin, r], o_send.at[0], o_recv.at[origin], rows=to).start()
        q2[origin, r] = p2[origin, r]

    conv_own(d)
    forward(0, w2, 1, 3)
    for count, here in ((chips - 1, own), (chips, jnp.logical_not(own))):
        @pl.when(here)
        def _():
            span = r1.at[0:count]
            wait_group(span, span, f_send.at[0], f_recv.at[0])

    for part in range(2):
        for j in range(2):
            for side in range(3):
                at = side * half + j * GSIZE
                w1[d, part, :, at : at + GSIZE] = r1[2 * j + part, :, side * GSIZE : (side + 1) * GSIZE]

    def start_inner(toward):
        for here, way in ((1, toward), (2, 1 - toward)):
            @pl.when(d == here)
            def _():
                start_hops(1, w1, k, (way,))
                start_hops(1, w1, 1 - k, (way,))

    start_inner(1)

    take_end(0, w2, 1)
    conv_own(nth(1))
    @pl.when(middle)
    def _():
        take(0, w2, 2)
        conv_own(nth(2))

    def activation(normed, gain, shift):
        linear = normed * gain + shift
        logistic = 1.0 / (1.0 + jnp.exp(-linear))
        return logistic * (1.0 + linear * (1.0 - logistic)) * gain

    everyone = hid_two.at[0 : rows - 1]
    wait_group(everyone, everyone, h_send.at[0], h_recv.at[0])

    @pl.when(jnp.logical_not(middle))
    def _():
        lend_hid.start()
        start_hops(1, w1, k)
        start_hops(1, w1, 1 - k)

    def field_stats(field, slot, nrm, act, inverse_at):
        plain = jnp.zeros((GSIZE, lanes), f32)
        square = jnp.zeros((GSIZE, lanes), f32)
        for h in range(rows):
            values = field[h].astype(f32)
            plain += values
            square += values * values
        average = image_totals(jnp.sum(plain, axis=0, keepdims=True)) * (1.0 / number)
        meansq = image_totals(jnp.sum(square, axis=0, keepdims=True)) * (1.0 / number)
        inverse = lax.rsqrt(meansq - average * average + 1e-05)
        inv2_ref[inverse_at : inverse_at + 1] = inverse
        at = pl.multiple_of((k + 2 * slot) * block + GSIZE * c, GSIZE)
        gain = par_ref[pl.ds(at, GSIZE), 2:3]
        shift = par_ref[pl.ds(at, GSIZE), 3:4]
        for h in range(rows):
            normed = (field[h].astype(f32) - average) * inverse
            spot = (h % 2) * GSIZE
            nrm[h // 2, spot : spot + GSIZE] = normed
            act[h // 2, spot : spot + GSIZE] = activation(normed, gain, shift)

    for slot in range(2):
        field_stats(hid_b.at[slot], slot, nrm2.at[slot], act2.at[slot], slot)

    @pl.when(middle)
    def _():
        lend_cot.wait_recv()
        share(x_far, 1).start()
        start_inner(0)
        share(x_far, 1).wait_recv()
        shift_rows(x_far, xs_far)
        conv_far(2)
        take(0, w2, 3)
        conv_far(3)
        conv_own(nth(3))

    forward(1, w1, 2, 0)
    forward(1, w1, 1, 0)
    @pl.when(middle)
    def _():
        lend_hid.wait_recv()
        field_stats(hid_far, lent, nrm_far, act_far, 2)

    forward(1, w1, 2, 1)
    forward(1, w1, 1, 1)

    average1, meansq1 = wait_sums(0)
    inverse1 = lax.rsqrt(meansq1 - average1 * average1 + 1e-05)
    for g in range(groups):
        rows_g = pl.ds(g * GSIZE, GSIZE)
        normed = (nrm1[rows_g, :] - average1[g : g + 1]) * inverse1[g : g + 1]
        nrm1[rows_g, :] = normed
        act1[rows_g, :] = activation(normed, par_ref[rows_g, 0:1], par_ref[rows_g, 1:2])

    forward(1, w1, 2, 2)
    forward(1, w1, 1, 2)
    def norm_two(slot, recv, q, nrm, act, inverse, dst):
        for count, here in ((chips - 1, own), (chips, jnp.logical_not(own))):
            @pl.when(here)
            def _():
                span = q.at[0:count]
                wait_group(span, span, p_send.at[0], recv)

        sum_first = jnp.zeros((2 * GSIZE, lanes), f32)
        sum_second = jnp.zeros((2 * GSIZE, lanes), f32)
        scaled = []
        for m in range(rows // 2):
            total = q[0, m].astype(f32)
            for frm in range(1, chips):
                total = total + q[frm, m].astype(f32)
            value = total * act[m]
            scaled.append(value)
            sum_first += value
            sum_second += value * nrm[m]
        first = image_totals(jnp.sum(sum_first, axis=0, keepdims=True)) * (1.0 / number)
        second = image_totals(jnp.sum(sum_second, axis=0, keepdims=True)) * (1.0 / number)
        for m in range(rows // 2):
            dst[m] = (inverse * (scaled[m] - first - nrm[m] * second)).astype(bf16)

    def norm_own(slot):
        norm_two(
            slot, p_recv.at[slot], q1.at[slot], nrm2.at[slot], act2.at[slot],
            inv2_ref[pl.ds(slot, 1), :], hg_two.at[slot],
        )

    lend = remote(hg_far, hg_two.at[lent], e_send.at[0], e_recv.at[0], dp=partner)

    @pl.when(middle)
    def _():
        norm_two(lent, p_recv.at[2], q_far, nrm_far, act_far, inv2_ref[2:3, :], hg_far)
        lend.start()

    forward(1, w1, 2, 3)
    forward(1, w1, 1, 3)
    forward(1, w1, 3, 0)
    forward(1, w1, 3, 1)
    @pl.when(middle)
    def _():
        norm_own(0)
        norm_own(1)

    @pl.when(jnp.logical_not(middle))
    def _():
        norm_own(1 - lent)
        lend.wait_recv()

    for h in range(rows):
        spot = (h % 2) * GSIZE
        both = [hg_two[slot, h // 2].astype(f32)[spot : spot + GSIZE] for slot in range(2)]
        hg_s[h] = jnp.concatenate(both, axis=0).astype(bf16)
    swap = remote(hg_s, hg_r, b_send.at[1], b_recv.at[1], rows=sibling)
    swap.start()
    pending.append(swap)
    for h in range(rows):
        store_shifts(xs1, k, h, hg_s[h].astype(f32))
    swap.wait_recv()
    for h in range(rows):
        store_shifts(xs1, 1 - k, h, hg_r[h].astype(f32))

    forward(1, w1, 3, 2)
    conv_one(d)
    take_end(1, w1, 1)
    conv_one(nth(1))
    forward(1, w1, 3, 3)
    take_end(1, w1, 2)
    conv_one(nth(2))
    take_end(1, w1, 3)
    conv_one(nth(3))
    for origin in range(depth):
        span = q2.at[origin, 0 : rows - 1]
        wait_group(span, span, o_send.at[0], o_recv.at[origin])

    one, two = [], []
    for origin in range(depth):
        for part in range(2):
            total = q2[origin, part].astype(f32)
            for frm in range(1, chips):
                total = total + q2[origin, 2 * frm + part].astype(f32)
            at = pl.ds(origin * block + part * half, half)
            value = total * act1[at, :]
            act1[at, :] = value
            one.append(jnp.sum(value.reshape(2, GSIZE, lanes), axis=1))
            two.append(jnp.sum((value * nrm1[at, :]).reshape(2, GSIZE, lanes), axis=1))
    send_sums(1, pack_sums(jnp.concatenate(one, axis=0), jnp.concatenate(two, axis=0)))
    first1, second1 = wait_sums(1)
    value = spread(inverse1) * (act1[...] - spread(first1) - nrm1[...] * spread(second1))
    out_ref[...] = (cot_t[...].astype(f32) + value).astype(bf16).T

    for copy in pending:
        copy.wait_send()
    def sent(span, send, recv):
        remote(span, span, send, recv, rows=sibling).wait_send()

    sent(x_cot.at[0, 0 : chips - 1], c_send.at[0], c_recv.at[0])
    share(x_cot, 0).wait_send()
    sent(hid_two.at[0 : rows - 1], h_send.at[0], h_recv.at[0])
    for which in range(2):
        sent(st_b.at[which, 0 : rows - 1], t_send.at[which], t_recv.at[which])
    sent(p2.at[:, 0 : rows - 1], o_send.at[0], o_recv.at[0])
    for count, here in ((chips - 1, own), (chips, jnp.logical_not(own))):
        @pl.when(here)
        def _():
            sent(r1.at[0:count], f_send.at[0], f_recv.at[0])

            @pl.when(middle)
            def _():
                sent(q1.at[:, 0:count], p_send.at[0], p_recv.at[0])
                sent(q_far.at[0:count], p_send.at[1], p_recv.at[2])

            @pl.when(jnp.logical_not(middle))
            def _():
                sent(q1.at[0, 0:count], p_send.at[0], p_recv.at[0])

    @pl.when(middle)
    def _():
        share(x_far, 1).wait_send()
        lend.wait_send()

    @pl.when(jnp.logical_not(middle))
    def _():
        lend_cot.wait_send()
        lend_hid.wait_send()

    last = depth - 1
    wait_hops(0, w2, [(0, 0, 0, 1), (1, 0, 0, 2), (1, 1, 1, 2), (2, 0, 2, 3), (2, 1, 2, 4), (3, 1, 3, 4)])
    wait_hops(
        1, w1,
        [(here, 0, 0, here + 1) for here in range(last)] + [(here, 1, here, depth) for here in range(1, depth)],
    )


def kernel_body(
    depth, rows,
    latent, hidden, cotangent, filter_one, filter_two, gain_one, shift_one, gain_two, shift_two,
):
    images, _, breadth, channels = latent.shape
    lanes = images * breadth
    block = channels // depth
    half = block // 2
    chips = rows // 2
    wide = -(-3 * half // 128) * 128
    narrow = -(-3 * GSIZE // 128) * 128
    groups = channels // GSIZE
    bf16, f32 = jnp.bfloat16, jnp.float32
    dma = pltpu.SemaphoreType.DMA
    out = pl.pallas_call(
        functools.partial(kernel, depth, rows, breadth),
        out_shape=jax.ShapeDtypeStruct((lanes, channels), bf16),
        in_specs=[pl.BlockSpec(memory_space=pltpu.HBM)] * 9,
        out_specs=pl.BlockSpec(memory_space=pltpu.VMEM),
        scratch_shapes=[
            pltpu.VMEM((lanes, channels), bf16),
            pltpu.VMEM((lanes, channels), bf16),
            pltpu.VMEM((lanes, channels), bf16),
            pltpu.VMEM(filter_one.shape, bf16),
            pltpu.VMEM(filter_two.shape, bf16),
            pltpu.VMEM((channels,), f32),
            pltpu.VMEM((channels,), f32),
            pltpu.VMEM((channels,), f32),
            pltpu.VMEM((channels,), f32),
            dma((9,)),
            pltpu.VMEM((channels, lanes), bf16),
            pltpu.VMEM((2, chips, block, lanes), bf16),
            pltpu.VMEM((2, rows, GSIZE, lanes), bf16),
            pltpu.VMEM((depth, 2, 3 * half, wide), bf16),
            pltpu.VMEM((depth, 2, 3 * half, wide), bf16),
            pltpu.VMEM((2, 2, 3 * half, narrow), bf16),
            pltpu.VMEM((3 * half, wide), bf16),
            pltpu.VMEM((chips, 3 * half, narrow), bf16),
            pltpu.VMEM((2, rows, wide, lanes), bf16),
            pltpu.VMEM((2, rows, wide, lanes), bf16),
            pltpu.VMEM((rows, 3 * half, lanes), f32),
            pltpu.VMEM((depth, 2, rows // 2, 2 * GSIZE, lanes), bf16),
            pltpu.VMEM((2, chips, rows // 2, 2 * GSIZE, lanes), bf16),
            pltpu.VMEM((depth, rows, half, lanes), bf16),
            pltpu.VMEM((depth, rows, half, lanes), bf16),
            pltpu.VMEM((rows, 2 * GSIZE, lanes), bf16),
            pltpu.VMEM((rows, 2 * GSIZE, lanes), bf16),
            pltpu.VMEM((channels, lanes), f32),
            pltpu.VMEM((channels, lanes), f32),
            pltpu.VMEM((2, rows // 2, 2 * GSIZE, lanes), f32),
            pltpu.VMEM((2, rows // 2, 2 * GSIZE, lanes), f32),
            pltpu.VMEM((4, lanes), f32),
            pltpu.VMEM((2, groups // 2, lanes), f32),
            pltpu.VMEM((2, rows, groups // 2, lanes), f32),
            pltpu.VMEM((channels, 8), f32),
            pltpu.VMEM((2, chips, block, lanes), bf16),
            pltpu.VMEM((rows, 2, GSIZE, lanes), bf16),
            pltpu.VMEM((rows, GSIZE, lanes), bf16),
            pltpu.VMEM((2, rows, wide, lanes), bf16),
            pltpu.VMEM((2, 2, rows // 2, 2 * GSIZE, lanes), bf16),
            pltpu.VMEM((chips, rows // 2, 2 * GSIZE, lanes), bf16),
            pltpu.VMEM((rows // 2, 2 * GSIZE, lanes), f32),
            pltpu.VMEM((rows // 2, 2 * GSIZE, lanes), f32),
            pltpu.VMEM((rows // 2, 2 * GSIZE, lanes), bf16),
            pltpu.VMEM((2, rows // 2, 2 * GSIZE, lanes), bf16),
            dma((2, 2)), dma((2, depth, 2, 2)),
            dma((1,)), dma((1,)),
            dma((2,)), dma((2,)),
            dma((2,)), dma((2,)),
            dma((2,)), dma((2,)),
            dma((2,)), dma((3,)),
            dma((1,)), dma((depth,)),
            dma((2,)), dma((2,)),
            dma((2,)), dma((2,)),
            dma((1,)), dma((1,)),
        ],
        compiler_params=pltpu.CompilerParams(
            collective_id=0, has_side_effects=True, vmem_limit_bytes=48 * 1024 * 1024
        ),
    )(
        *[
            pltpu.with_memory_space_constraint(array, pltpu.HBM)
            for array in (
                latent.reshape(lanes, channels), hidden.reshape(lanes, channels),
                cotangent.reshape(lanes, channels), filter_one, filter_two,
                gain_one, shift_one, gain_two, shift_two,
            )
        ]
    )
    return out.reshape(latent.shape)


def solution(mesh):
    depth, rows = mesh.shape["dp"], mesh.shape["rows"]
    in_specs = (
        P("dp", "rows", None, None),
        P("dp", "rows", None, None),
        P("dp", "rows", None, None),
        P(None, "dp", "rows"),
        P(None, "dp", "rows"),
        P(),
        P(),
        P(),
        P(),
    )

    def body(latent, *rest):
        images, rows_here, breadth, channels = latent.shape
        fits = (
            rows_here == 1
            and images * breadth == 128
            and breadth % 4 == 0
            and depth == 4
            and rows == 2 * depth
            and channels == GROUPS * GSIZE
            and channels == depth * (rows // 2) * GSIZE
        )
        if fits:
            return kernel_body(depth, rows, latent, *rest)
        return plain_body(latent, *rest)

    return jax.shard_map(
        body, mesh=mesh, in_specs=in_specs, out_specs=P("dp", "rows", None, None), check_vma=False
    )
```

```python
import functools

import jax
import jax.numpy as jnp
from jax import lax
from jax.experimental import pallas as pl
from jax.experimental.pallas import tpu as pltpu
from jax.sharding import PartitionSpec as P

GROUPS = 16
GSIZE = 40
TAPS = 9
MESH = pl.DeviceIdType.MESH


def extended(block, sides, width):
    for axis, dim in sides:
        count = lax.axis_size(axis)
        forward = [(i, i + 1) for i in range(count - 1)]
        backward = [(target, source) for source, target in forward]
        low = lax.ppermute(
            lax.slice_in_dim(block, block.shape[dim] - width, None, axis=dim), axis, forward
        )
        high = lax.ppermute(lax.slice_in_dim(block, 0, width, axis=dim), axis, backward)
        block = jnp.concatenate([low, block, high], axis=dim)
    return block


def group_sums(values):
    per_channel = jnp.sum(values, axis=(1, 2))
    return jnp.sum(per_channel.reshape(per_channel.shape[0], GROUPS, -1), axis=2)


def expand_groups(moment):
    return jnp.repeat(moment, GSIZE, axis=1)[:, None, None, :]


def finish_stats(sum_plain, sum_square, number):
    average = sum_plain / number
    variance = sum_square / number - average * average
    return (average, lax.rsqrt(variance + 1e-05))


def reduced_stats(field, number):
    values = field.astype(jnp.float32)
    sum_plain, sum_square = lax.psum((group_sums(values), group_sums(values * values)), "rows")
    return finish_stats(sum_plain, sum_square, number)


def norm_backward(field, stats, gain, shift, incoming, number):
    average, inverse = stats
    values = field.astype(jnp.float32)
    normed = (values - expand_groups(average)) * expand_groups(inverse)
    linear = normed * gain + shift
    logistic = jax.nn.sigmoid(linear)
    scaled = incoming * logistic * (1.0 + linear * (1.0 - logistic)) * gain
    sum_first, sum_second = lax.psum((group_sums(scaled), group_sums(scaled * normed)), "rows")
    first = sum_first / number
    second = sum_second / number
    return expand_groups(inverse) * (scaled - expand_groups(first) - normed * expand_groups(second))


def conv_backward(gradient, weights):
    images, rows_here, breadth, channels = gradient.shape
    padded = extended(gradient, (("rows", 1),), 1)
    padded = jnp.pad(padded, ((0, 0), (0, 0), (1, 1), (0, 0)))
    pixels = images * rows_here * breadth
    shifted = []
    for tap_index in range(9):
        down_step = tap_index // 3 - 1
        side_step = tap_index % 3 - 1
        window = padded[
            :, 1 - down_step : 1 - down_step + rows_here, 1 - side_step : 1 - side_step + breadth, :
        ]
        shifted.append(window.reshape(pixels, channels))
    stacked = jnp.stack(shifted, axis=1)
    gathered = lax.all_gather(weights, "dp", axis=1, tiled=True)
    section = lax.all_gather(gathered, "rows", axis=2, tiled=True)
    columns = section.shape[2]
    window = stacked.reshape(pixels, 9 * columns)
    flat = jnp.transpose(section, (0, 2, 1)).reshape(9 * columns, section.shape[1])
    result = jnp.dot(window, flat, preferred_element_type=jnp.float32)
    return result.reshape(images, rows_here, breadth, channels)


def plain_body(
    latent, hidden, cotangent, filter_one, filter_two, gain_one, shift_one, gain_two, shift_two
):
    number = latent.shape[1] * lax.axis_size("rows") * latent.shape[2] * GSIZE
    stats_two = reduced_stats(hidden, number)
    back_two = conv_backward(cotangent, filter_two)
    hidden_grad = norm_backward(hidden, stats_two, gain_two, shift_two, back_two, number).astype(
        jnp.bfloat16
    )
    stats_one = reduced_stats(latent, number)
    back_one = conv_backward(hidden_grad, filter_one)
    latent_part = norm_backward(latent, stats_one, gain_one, shift_one, back_one, number)
    return (cotangent.astype(jnp.float32) + latent_part).astype(jnp.bfloat16)


def kernel(
    depth, rows, breadth,
    lat_hbm, hid_hbm, cot_hbm, raw1_hbm, raw2_hbm, gain1_hbm, shift1_hbm, gain2_hbm, shift2_hbm,
    out_ref,
    lat_ref, hid_ref, cot_ref, raw1, raw2, gain1, shift1, gain2, shift2, in_sem,
    cot_t, x_cot, hid_b, w1, w2, s1, s2, r1,
    xs1, xs2, y_ref, p1, q1, p2, q2, hg_s, hg_r,
    nrm1, act1, nrm2, act2, inv2_ref, st_s, st_b, par_ref,
    x_far, hid_two, hid_far, xs_far, p_far, q_far, nrm_far, act_far, hg_far, hg_two,
    z_send, z_recv, f_send, f_recv, b_send, b_recv, c_send, c_recv, h_send, h_recv,
    p_send, p_recv, o_send, o_recv, t_send, t_recv, d_send, d_recv, e_send, e_recv,
):
    d = lax.axis_index("dp")
    r = lax.axis_index("rows")
    chips = rows // 2
    c = r // 2
    k = lax.rem(r, 2)
    sibling = r + 1 - 2 * k
    channels, lanes = cot_t.shape
    block = channels // depth
    half = block // 2
    images = lanes // breadth
    wide = w1.shape[4]
    number = rows * breadth * GSIZE
    groups = channels // GSIZE
    bf16, f32 = jnp.bfloat16, jnp.float32

    def remote(src, dst, send, recv, **device):
        return pltpu.make_async_remote_copy(
            src_ref=src, dst_ref=dst, send_sem=send, recv_sem=recv,
            device_id=device, device_id_type=MESH,
        )

    pending = []
    loads = {
        name: pltpu.make_async_copy(src, dst, in_sem.at[index])
        for index, (name, src, dst) in enumerate((
            ("raw2", raw2_hbm, raw2), ("cot", cot_hbm, cot_ref), ("hid", hid_hbm, hid_ref),
            ("raw1", raw1_hbm, raw1), ("lat", lat_hbm, lat_ref), ("gain1", gain1_hbm, gain1),
            ("shift1", shift1_hbm, shift1), ("gain2", gain2_hbm, gain2), ("shift2", shift2_hbm, shift2),
        ))
    }
    loads["raw2"].start()

    barrier = pltpu.get_barrier_semaphore()

    middle = (d > 0) & (d < depth - 1)
    partner = d + 1 - 2 * lax.rem(d, 2)
    lent = jnp.where(2 * d < depth, 1, 0)

    @pl.when(d > 0)
    def _():
        pl.semaphore_signal(barrier, inc=1, device_id={"dp": d - 1}, device_id_type=MESH)

    @pl.when(d < depth - 1)
    def _():
        pl.semaphore_signal(barrier, inc=1, device_id={"dp": d + 1}, device_id_type=MESH)

    for off in range(1, rows):
        pl.semaphore_signal(barrier, inc=1, device_id={"rows": lax.rem(r + off, rows)}, device_id_type=MESH)

    for name, load in loads.items():
        if name != "raw2":
            load.start()

    pad = wide - 3 * half
    own = k == c // 2
    w2[d, k, :, :, 3 * half :] = jnp.zeros((3, half, pad), bf16)
    s2[:, :, 3 * half :] = jnp.zeros((3, half, pad), bf16)
    for part in range(2):
        w1[d, part, :, :, 3 * half :] = jnp.zeros((3, half, pad), bf16)
        for side_core in range(2):
            s1[part, side_core, :, :, 3 * GSIZE :] = jnp.zeros((3, half, s1.shape[4] - 3 * GSIZE), bf16)
    for xs in (xs1, xs2, xs_far):
        for part in range(2):
            for h in range(rows):
                xs[part, h, 3 * half :] = jnp.zeros((pad, lanes), bf16)
    loads["raw2"].wait()

    def arrange(ready, raw, which):
        start = pl.multiple_of(which * half, 16)
        for tap in range(TAPS):
            down, side = tap // 3, tap % 3
            ready[down, :, side * half : (side + 1) * half] = raw[
                tap, pl.ds(start, half), :
            ]

    arrange(w2.at[d, k], raw2, k)

    pl.semaphore_wait(barrier, rows + jnp.where(middle, 1, 0))

    split = half // 32 * 16 + 16
    segments = ((0, split), (split, half))

    def hop(which, w, origin, part, seg, way):
        low, high = segments[seg]
        piece = w.at[origin, part, :, low:high]
        return remote(
            piece, piece, z_send.at[which, way], z_recv.at[which, origin, part, seg], dp=d + 1 - 2 * way
        )

    near = jnp.minimum(d, depth - 1 - d)

    def nth(step):
        value = step - near if step == 1 else step
        return jnp.where(2 * d < depth, value, depth - 1 - value)

    def start_hops(which, w, part, ways=(0, 1), segs=(0, 1)):
        for way in ways:
            @pl.when((d < depth - 1) if way == 0 else (d > 0))
            def _():
                for seg in segs:
                    hop(which, w, d, part, seg, way).start()

    def start_one(ways):
        for seg in range(2):
            for part in (k, 1 - k):
                start_hops(1, w1, part, ways, (seg,))

    def forward(which, w, step, index):
        origin = nth(step)
        at, seg = (index // 2, index % 2) if which == 0 else (index % 2, index // 2)
        part = (k, 1 - k)[at]
        for way in range(2):
            @pl.when(middle & ((origin < d) if way == 0 else (origin > d)))
            def _():
                copy = hop(which, w, origin, part, seg, way)
                copy.wait_recv()
                copy.start()

    def take(which, w, step, segs=(0, 1)):
        for part in (k, 1 - k):
            for seg in segs:
                hop(which, w, nth(step), part, seg, 0).wait_recv()

    def take_end(which, w, step, segs=(0, 1)):
        @pl.when(jnp.logical_not(middle))
        def _():
            take(which, w, step, segs)

    def wait_hops(which, w, spans):
        for here, way, low, high in spans:
            @pl.when(d == here)
            def _():
                span = w.at[low:high]
                remote(
                    span, span, z_send.at[which, way], z_recv.at[which, 0, 0, 0], dp=d + 1 - 2 * way
                ).wait_send()

    start_hops(0, w2, k)
    arrange(s2, raw2, 1 - k)
    twin = remote(s2, w2.at[d, k], b_send.at[0], b_recv.at[0], rows=sibling)
    twin.start()
    pending.append(twin)

    loads["cot"].wait()
    cot_t[...] = cot_ref[...].T

    def piece_of(to):
        return cot_t.at[pl.ds(pl.multiple_of((to // 2) * block, block), block), :]

    for off in range(1, chips):
        to = 2 * lax.rem(c + off, chips) + k
        remote(piece_of(to), x_cot.at[k, c], c_send.at[0], c_recv.at[0], rows=to).start()
    x_cot[k, c] = piece_of(r)[...]

    loads["raw1"].wait()
    for part in range(2):
        for side_core in range(2):
            ready = s1.at[part, side_core]
            for tap in range(TAPS):
                down, side = tap // 3, tap % 3
                ready[down, :, side * GSIZE : (side + 1) * GSIZE] = raw1[
                    tap, side_core * half : (side_core + 1) * half, part * GSIZE : (part + 1) * GSIZE
                ]

    for part in range(2):
        for side_core in range(2):
            to = 2 * (2 * k + part) + side_core

            @pl.when(to != r)
            def _():
                remote(s1.at[part, side_core], r1.at[c], f_send.at[0], f_recv.at[0], rows=to).start()

            @pl.when(to == r)
            def _():
                r1[c] = s1[part, side_core]

    loads["hid"].wait()
    hid_full = hid_ref[...].astype(f32).T
    for to in range(rows):
        parts = [
            hid_full[block * b + GSIZE * (to // 2) : block * b + GSIZE * (to // 2 + 1)]
            for b in (to % 2, to % 2 + 2)
        ]
        for slot in range(2):
            hid_two[to, slot] = parts[slot].astype(bf16)
    for off in range(1, rows):
        to = lax.rem(r + off, rows)
        remote(hid_two.at[to], hid_b.at[:, r], h_send.at[0], h_recv.at[0], rows=to).start()
    hid_b[:, r] = hid_two[r]

    remote(s2, w2.at[d, 1 - k], b_send.at[0], b_recv.at[0], rows=sibling).wait_recv()
    start_hops(0, w2, 1 - k)

    forward(0, w2, 1, 0)
    loads["lat"].wait()
    lane = lax.broadcasted_iota(jnp.int32, (1, lanes), 1)
    column = lax.rem(lane, breadth)
    image_of = lax.div(lane, breadth)
    quarter = lax.rem(lane, breadth) // (breadth // 4)

    def image_totals(per_lane):
        total = jnp.zeros_like(per_lane)
        for image in range(images):
            mine = image_of == image
            part = jnp.sum(jnp.where(mine, per_lane, 0.0), axis=1, keepdims=True)
            total = jnp.where(mine, part, total)
        return total

    def pack_sums(one, two):
        one, two = image_totals(one), image_totals(two)
        top, low = slice(0, groups // 2), slice(groups // 2, groups)
        return jnp.where(
            quarter == 0, one[top], jnp.where(quarter == 1, two[top], jnp.where(quarter == 2, one[low], two[low]))
        )

    def send_sums(which, packed):
        st_s[which] = packed
        for off in range(1, rows):
            to = lax.rem(r + off, rows)
            remote(st_s.at[which], st_b.at[which, r], t_send.at[which], t_recv.at[which], rows=to).start()
        st_b[which, r] = packed

    def wait_sums(which):
        span = st_b.at[which, 0 : rows - 1]
        remote(span, span, t_send.at[which], t_recv.at[which], rows=sibling).wait_recv()
        total = st_b[which, 0]
        for h in range(1, rows):
            total = total + st_b[which, h]
        total = total * (1.0 / number)
        full = []
        for at in range(4):
            mine = jnp.where(quarter == at, total, 0.0)
            pair = mine + pltpu.roll(mine, ((1 if at % 2 == 0 else -1) * breadth // 4) % lanes, 1)
            full.append(pair + pltpu.roll(pair, ((1 if at < 2 else -1) * breadth // 2) % lanes, 1))
        return jnp.concatenate([full[0], full[2]], axis=0), jnp.concatenate([full[1], full[3]], axis=0)

    def spread(moment):
        return jnp.broadcast_to(moment[:, None, :], (groups, GSIZE, lanes)).reshape(channels, lanes)

    def by_group(values):
        return jnp.sum(values.reshape(groups, GSIZE, lanes), axis=1)

    nrm1[...] = lat_ref[...].astype(f32).T
    send_sums(0, pack_sums(by_group(nrm1[...]), by_group(nrm1[...] * nrm1[...])))

    for name in ("gain1", "shift1", "gain2", "shift2"):
        loads[name].wait()
    raw_params = [p[...].reshape(1, channels) for p in (gain1, shift1, gain2, shift2)]
    par_ref[...] = jnp.concatenate(raw_params + raw_params, axis=0).T

    def store_shifts(xs, part, h, values):
        left = jnp.where(column == breadth - 1, 0.0, pltpu.roll(values, lanes - 1, 1))
        right = jnp.where(column == 0, 0.0, pltpu.roll(values, 1, 1))
        xs[part, h, 0:half] = left.astype(bf16)
        xs[part, h, half : 2 * half] = values.astype(bf16)
        xs[part, h, 2 * half : 3 * half] = right.astype(bf16)

    def wait_group(src, dst, send, recv):
        remote(src, dst, send, recv, rows=sibling).wait_recv()

    forward(0, w2, 1, 1)
    everyone = x_cot.at[0, 0 : chips - 1]
    wait_group(everyone, everyone, c_send.at[0], c_recv.at[0])

    def share(x, at):
        return remote(x.at[k], x.at[k], d_send.at[at], d_recv.at[at], rows=sibling)

    def shift_rows(x, xs):
        for h in range(rows):
            values = x[h % 2, h // 2].astype(f32)
            for part in range(2):
                store_shifts(xs, part, h, values[part * half : (part + 1) * half])

    share(x_cot, 0).start()
    lend_cot = remote(x_cot.at[k], x_far.at[k], c_send.at[1], c_recv.at[1], dp=partner)
    lend_hid = remote(hid_b.at[lent], hid_far, h_send.at[1], h_recv.at[1], dp=partner)

    @pl.when(jnp.logical_not(middle))
    def _():
        lend_cot.start()

    forward(0, w2, 1, 2)
    share(x_cot, 0).wait_recv()
    shift_rows(x_cot, xs2)

    def conv(w, origin, xs, low, high):
        for h in range(0, rows, 2):
            total = None
            for part in range(2):
                pair = jnp.concatenate([xs[part, h], xs[part, h + 1]], axis=1)
                piece = w[origin, part, :, low:high].reshape(3 * (high - low), wide)
                term = jnp.dot(piece, pair, preferred_element_type=f32)
                total = term if total is None else total + term
            y_ref[h, 0 : 3 * (high - low)] = total[:, :lanes]
            y_ref[h + 1, 0 : 3 * (high - low)] = total[:, lanes:]

    def row_of(h, size):
        total = y_ref[h, size : 2 * size]
        if h + 1 < rows:
            total = total + y_ref[h + 1, 0:size]
        if h > 0:
            total = total + y_ref[h - 1, 2 * size : 3 * size]
        return total

    def conv_two(origin, xs, p, q, send, recv):
        conv(w2, origin, xs, 0, half)
        for h in range(0, rows, 2):
            low, high = row_of(h, half), row_of(h + 1, half)
            for j in range(2):
                both = [low[j * GSIZE : (j + 1) * GSIZE], high[j * GSIZE : (j + 1) * GSIZE]]
                p[j, h // 2] = jnp.concatenate(both, axis=0).astype(bf16)
        for j in range(2):
            to = 2 * (2 * k + j) + lax.rem(origin, 2)

            @pl.when(to != r)
            def _():
                remote(p.at[j], q.at[c], send, recv, rows=to).start()

            @pl.when(to == r)
            def _():
                q[c] = p[j]

    def conv_own(origin):
        slot = origin // 2
        conv_two(origin, xs2, p1.at[origin], q1.at[slot], p_send.at[0], p_recv.at[slot])

    def conv_far(step):
        conv_two(nth(step), xs_far, p_far.at[step - 2], q_far, p_send.at[1], p_recv.at[2])

    def conv_one(origin, low=0, high=half):
        conv(w1, origin, xs1, low, high)
        for h in range(rows):
            p2[origin, h, low:high] = row_of(h, high - low).astype(bf16)
        for off in range(1, rows):
            to = lax.rem(r + off, rows)
            remote(
                p2.at[origin, to, low:high], q2.at[origin, r, low:high], o_send.at[0], o_recv.at[origin], rows=to
            ).start()
        q2[origin, r, low:high] = p2[origin, r, low:high]

    conv_own(d)
    forward(0, w2, 1, 3)
    for count, here in ((chips - 1, own), (chips, jnp.logical_not(own))):
        @pl.when(here)
        def _():
            span = r1.at[0:count]
            wait_group(span, span, f_send.at[0], f_recv.at[0])

    for part in range(2):
        for j in range(2):
            for side in range(3):
                at = side * half + j * GSIZE
                w1[d, part, :, :, at : at + GSIZE] = r1[2 * j + part, :, :, side * GSIZE : (side + 1) * GSIZE]

    def start_inner(toward):
        for here, way in ((1, toward), (2, 1 - toward)):
            @pl.when(d == here)
            def _():
                start_one((way,))

    start_inner(1)

    take_end(0, w2, 1)
    conv_own(nth(1))
    @pl.when(middle)
    def _():
        take(0, w2, 2)
        conv_own(nth(2))

    def activation(normed, gain, shift):
        linear = normed * gain + shift
        logistic = 1.0 / (1.0 + jnp.exp(-linear))
        return logistic * (1.0 + linear * (1.0 - logistic)) * gain

    everyone = hid_two.at[0 : rows - 1]
    wait_group(everyone, everyone, h_send.at[0], h_recv.at[0])

    @pl.when(jnp.logical_not(middle))
    def _():
        lend_hid.start()
        start_one((0, 1))

    def field_stats(field, slot, nrm, act, inverse_at):
        plain = jnp.zeros((GSIZE, lanes), f32)
        square = jnp.zeros((GSIZE, lanes), f32)
        for h in range(rows):
            values = field[h].astype(f32)
            plain += values
            square += values * values
        average = image_totals(jnp.sum(plain, axis=0, keepdims=True)) * (1.0 / number)
        meansq = image_totals(jnp.sum(square, axis=0, keepdims=True)) * (1.0 / number)
        inverse = lax.rsqrt(meansq - average * average + 1e-05)
        inv2_ref[inverse_at : inverse_at + 1] = inverse
        at = pl.multiple_of((k + 2 * slot) * block + GSIZE * c, GSIZE)
        gain = par_ref[pl.ds(at, GSIZE), 2:3]
        shift = par_ref[pl.ds(at, GSIZE), 3:4]
        for h in range(rows):
            normed = (field[h].astype(f32) - average) * inverse
            spot = (h % 2) * GSIZE
            nrm[h // 2, spot : spot + GSIZE] = normed
            act[h // 2, spot : spot + GSIZE] = activation(normed, gain, shift)

    for slot in range(2):
        field_stats(hid_b.at[slot], slot, nrm2.at[slot], act2.at[slot], slot)

    @pl.when(middle)
    def _():
        lend_cot.wait_recv()
        share(x_far, 1).start()
        start_inner(0)
        share(x_far, 1).wait_recv()
        shift_rows(x_far, xs_far)
        conv_far(2)
        take(0, w2, 3)
        conv_far(3)
        conv_own(nth(3))

    forward(1, w1, 2, 0)
    forward(1, w1, 1, 0)
    @pl.when(middle)
    def _():
        lend_hid.wait_recv()
        field_stats(hid_far, lent, nrm_far, act_far, 2)

    forward(1, w1, 2, 1)
    forward(1, w1, 1, 1)

    average1, meansq1 = wait_sums(0)
    inverse1 = lax.rsqrt(meansq1 - average1 * average1 + 1e-05)
    for g in range(groups):
        rows_g = pl.ds(g * GSIZE, GSIZE)
        normed = (nrm1[rows_g, :] - average1[g : g + 1]) * inverse1[g : g + 1]
        nrm1[rows_g, :] = normed
        act1[rows_g, :] = activation(normed, par_ref[rows_g, 0:1], par_ref[rows_g, 1:2])

    def norm_two(slot, recv, q, nrm, act, inverse, dst):
        for count, here in ((chips - 1, own), (chips, jnp.logical_not(own))):
            @pl.when(here)
            def _():
                span = q.at[0:count]
                wait_group(span, span, p_send.at[0], recv)

        sum_first = jnp.zeros((2 * GSIZE, lanes), f32)
        sum_second = jnp.zeros((2 * GSIZE, lanes), f32)
        scaled = []
        for m in range(rows // 2):
            total = q[0, m].astype(f32)
            for frm in range(1, chips):
                total = total + q[frm, m].astype(f32)
            value = total * act[m]
            scaled.append(value)
            sum_first += value
            sum_second += value * nrm[m]
        first = image_totals(jnp.sum(sum_first, axis=0, keepdims=True)) * (1.0 / number)
        second = image_totals(jnp.sum(sum_second, axis=0, keepdims=True)) * (1.0 / number)
        for m in range(rows // 2):
            dst[m] = (inverse * (scaled[m] - first - nrm[m] * second)).astype(bf16)

    def norm_own(slot):
        norm_two(
            slot, p_recv.at[slot], q1.at[slot], nrm2.at[slot], act2.at[slot],
            inv2_ref[pl.ds(slot, 1), :], hg_two.at[slot],
        )

    lend = remote(hg_far, hg_two.at[lent], e_send.at[0], e_recv.at[0], dp=partner)

    @pl.when(middle)
    def _():
        norm_two(lent, p_recv.at[2], q_far, nrm_far, act_far, inv2_ref[2:3, :], hg_far)
        lend.start()

    forward(1, w1, 2, 2)
    forward(1, w1, 1, 2)
    forward(1, w1, 2, 3)
    forward(1, w1, 1, 3)
    forward(1, w1, 3, 0)
    forward(1, w1, 3, 1)
    @pl.when(middle)
    def _():
        norm_own(0)
        norm_own(1)

    @pl.when(jnp.logical_not(middle))
    def _():
        norm_own(1 - lent)
        lend.wait_recv()

    for h in range(rows):
        spot = (h % 2) * GSIZE
        both = [hg_two[slot, h // 2].astype(f32)[spot : spot + GSIZE] for slot in range(2)]
        hg_s[h] = jnp.concatenate(both, axis=0).astype(bf16)
    swap = remote(hg_s, hg_r, b_send.at[1], b_recv.at[1], rows=sibling)
    swap.start()
    pending.append(swap)
    for h in range(rows):
        store_shifts(xs1, k, h, hg_s[h].astype(f32))
    swap.wait_recv()
    for h in range(rows):
        store_shifts(xs1, 1 - k, h, hg_r[h].astype(f32))

    forward(1, w1, 3, 2)
    conv_one(d)
    take_end(1, w1, 1)
    conv_one(nth(1))
    forward(1, w1, 3, 3)
    take_end(1, w1, 2)
    conv_one(nth(2))
    take_end(1, w1, 3)
    conv_one(nth(3))
    for origin in range(depth):
        span = q2.at[origin, 0 : rows - 1]
        wait_group(span, span, o_send.at[0], o_recv.at[origin])

    one, two = [], []
    for origin in range(depth):
        for part in range(2):
            total = q2[origin, part].astype(f32)
            for frm in range(1, chips):
                total = total + q2[origin, 2 * frm + part].astype(f32)
            at = pl.ds(origin * block + part * half, half)
            value = total * act1[at, :]
            act1[at, :] = value
            one.append(jnp.sum(value.reshape(2, GSIZE, lanes), axis=1))
            two.append(jnp.sum((value * nrm1[at, :]).reshape(2, GSIZE, lanes), axis=1))
    send_sums(1, pack_sums(jnp.concatenate(one, axis=0), jnp.concatenate(two, axis=0)))
    first1, second1 = wait_sums(1)
    value = spread(inverse1) * (act1[...] - spread(first1) - nrm1[...] * spread(second1))
    out_ref[...] = (cot_t[...].astype(f32) + value).astype(bf16).T

    for copy in pending:
        copy.wait_send()
    def sent(span, send, recv):
        remote(span, span, send, recv, rows=sibling).wait_send()

    sent(x_cot.at[0, 0 : chips - 1], c_send.at[0], c_recv.at[0])
    share(x_cot, 0).wait_send()
    sent(hid_two.at[0 : rows - 1], h_send.at[0], h_recv.at[0])
    for which in range(2):
        sent(st_b.at[which, 0 : rows - 1], t_send.at[which], t_recv.at[which])
    sent(p2.at[:, 0 : rows - 1], o_send.at[0], o_recv.at[0])
    for count, here in ((chips - 1, own), (chips, jnp.logical_not(own))):
        @pl.when(here)
        def _():
            sent(r1.at[0:count], f_send.at[0], f_recv.at[0])

            @pl.when(middle)
            def _():
                sent(q1.at[:, 0:count], p_send.at[0], p_recv.at[0])
                sent(q_far.at[0:count], p_send.at[1], p_recv.at[2])

            @pl.when(jnp.logical_not(middle))
            def _():
                sent(q1.at[0, 0:count], p_send.at[0], p_recv.at[0])

    @pl.when(middle)
    def _():
        share(x_far, 1).wait_send()
        lend.wait_send()

    @pl.when(jnp.logical_not(middle))
    def _():
        lend_cot.wait_send()
        lend_hid.wait_send()

    last = depth - 1
    wait_hops(0, w2, [(0, 0, 0, 1), (1, 0, 0, 2), (1, 1, 1, 2), (2, 0, 2, 3), (2, 1, 2, 4), (3, 1, 3, 4)])
    wait_hops(
        1, w1,
        [(here, 0, 0, here + 1) for here in range(last)] + [(here, 1, here, depth) for here in range(1, depth)],
    )


def kernel_body(
    depth, rows,
    latent, hidden, cotangent, filter_one, filter_two, gain_one, shift_one, gain_two, shift_two,
):
    images, _, breadth, channels = latent.shape
    lanes = images * breadth
    block = channels // depth
    half = block // 2
    chips = rows // 2
    wide = -(-3 * half // 128) * 128
    narrow = -(-3 * GSIZE // 128) * 128
    groups = channels // GSIZE
    bf16, f32 = jnp.bfloat16, jnp.float32
    dma = pltpu.SemaphoreType.DMA
    out = pl.pallas_call(
        functools.partial(kernel, depth, rows, breadth),
        out_shape=jax.ShapeDtypeStruct((lanes, channels), bf16),
        in_specs=[pl.BlockSpec(memory_space=pltpu.HBM)] * 9,
        out_specs=pl.BlockSpec(memory_space=pltpu.VMEM),
        scratch_shapes=[
            pltpu.VMEM((lanes, channels), bf16),
            pltpu.VMEM((lanes, channels), bf16),
            pltpu.VMEM((lanes, channels), bf16),
            pltpu.VMEM(filter_one.shape, bf16),
            pltpu.VMEM(filter_two.shape, bf16),
            pltpu.VMEM((channels,), f32),
            pltpu.VMEM((channels,), f32),
            pltpu.VMEM((channels,), f32),
            pltpu.VMEM((channels,), f32),
            dma((9,)),
            pltpu.VMEM((channels, lanes), bf16),
            pltpu.VMEM((2, chips, block, lanes), bf16),
            pltpu.VMEM((2, rows, GSIZE, lanes), bf16),
            pltpu.VMEM((depth, 2, 3, half, wide), bf16),
            pltpu.VMEM((depth, 2, 3, half, wide), bf16),
            pltpu.VMEM((2, 2, 3, half, narrow), bf16),
            pltpu.VMEM((3, half, wide), bf16),
            pltpu.VMEM((chips, 3, half, narrow), bf16),
            pltpu.VMEM((2, rows, wide, lanes), bf16),
            pltpu.VMEM((2, rows, wide, lanes), bf16),
            pltpu.VMEM((rows, 3 * half, lanes), f32),
            pltpu.VMEM((depth, 2, rows // 2, 2 * GSIZE, lanes), bf16),
            pltpu.VMEM((2, chips, rows // 2, 2 * GSIZE, lanes), bf16),
            pltpu.VMEM((depth, rows, half, lanes), bf16),
            pltpu.VMEM((depth, rows, half, lanes), bf16),
            pltpu.VMEM((rows, 2 * GSIZE, lanes), bf16),
            pltpu.VMEM((rows, 2 * GSIZE, lanes), bf16),
            pltpu.VMEM((channels, lanes), f32),
            pltpu.VMEM((channels, lanes), f32),
            pltpu.VMEM((2, rows // 2, 2 * GSIZE, lanes), f32),
            pltpu.VMEM((2, rows // 2, 2 * GSIZE, lanes), f32),
            pltpu.VMEM((4, lanes), f32),
            pltpu.VMEM((2, groups // 2, lanes), f32),
            pltpu.VMEM((2, rows, groups // 2, lanes), f32),
            pltpu.VMEM((channels, 8), f32),
            pltpu.VMEM((2, chips, block, lanes), bf16),
            pltpu.VMEM((rows, 2, GSIZE, lanes), bf16),
            pltpu.VMEM((rows, GSIZE, lanes), bf16),
            pltpu.VMEM((2, rows, wide, lanes), bf16),
            pltpu.VMEM((2, 2, rows // 2, 2 * GSIZE, lanes), bf16),
            pltpu.VMEM((chips, rows // 2, 2 * GSIZE, lanes), bf16),
            pltpu.VMEM((rows // 2, 2 * GSIZE, lanes), f32),
            pltpu.VMEM((rows // 2, 2 * GSIZE, lanes), f32),
            pltpu.VMEM((rows // 2, 2 * GSIZE, lanes), bf16),
            pltpu.VMEM((2, rows // 2, 2 * GSIZE, lanes), bf16),
            dma((2, 2)), dma((2, depth, 2, 2)),
            dma((1,)), dma((1,)),
            dma((2,)), dma((2,)),
            dma((2,)), dma((2,)),
            dma((2,)), dma((2,)),
            dma((2,)), dma((3,)),
            dma((1,)), dma((depth,)),
            dma((2,)), dma((2,)),
            dma((2,)), dma((2,)),
            dma((1,)), dma((1,)),
        ],
        compiler_params=pltpu.CompilerParams(
            collective_id=0, has_side_effects=True, vmem_limit_bytes=48 * 1024 * 1024
        ),
    )(
        *[
            pltpu.with_memory_space_constraint(array, pltpu.HBM)
            for array in (
                latent.reshape(lanes, channels), hidden.reshape(lanes, channels),
                cotangent.reshape(lanes, channels), filter_one, filter_two,
                gain_one, shift_one, gain_two, shift_two,
            )
        ]
    )
    return out.reshape(latent.shape)


def solution(mesh):
    depth, rows = mesh.shape["dp"], mesh.shape["rows"]
    in_specs = (
        P("dp", "rows", None, None),
        P("dp", "rows", None, None),
        P("dp", "rows", None, None),
        P(None, "dp", "rows"),
        P(None, "dp", "rows"),
        P(),
        P(),
        P(),
        P(),
    )

    def body(latent, *rest):
        images, rows_here, breadth, channels = latent.shape
        fits = (
            rows_here == 1
            and images * breadth == 128
            and breadth % 4 == 0
            and depth == 4
            and rows == 2 * depth
            and channels == GROUPS * GSIZE
            and channels == depth * (rows // 2) * GSIZE
        )
        if fits:
            return kernel_body(depth, rows, latent, *rest)
        return plain_body(latent, *rest)

    return jax.shard_map(
        body, mesh=mesh, in_specs=in_specs, out_specs=P("dp", "rows", None, None), check_vma=False
    )
```

```python
import functools

import jax
import jax.numpy as jnp
from jax import lax
from jax.experimental import pallas as pl
from jax.experimental.pallas import tpu as pltpu
from jax.sharding import PartitionSpec as P

GROUPS = 16
GSIZE = 40
TAPS = 9
MESH = pl.DeviceIdType.MESH


def extended(block, sides, width):
    for axis, dim in sides:
        count = lax.axis_size(axis)
        forward = [(i, i + 1) for i in range(count - 1)]
        backward = [(target, source) for source, target in forward]
        low = lax.ppermute(
            lax.slice_in_dim(block, block.shape[dim] - width, None, axis=dim), axis, forward
        )
        high = lax.ppermute(lax.slice_in_dim(block, 0, width, axis=dim), axis, backward)
        block = jnp.concatenate([low, block, high], axis=dim)
    return block


def group_sums(values):
    per_channel = jnp.sum(values, axis=(1, 2))
    return jnp.sum(per_channel.reshape(per_channel.shape[0], GROUPS, -1), axis=2)


def expand_groups(moment):
    return jnp.repeat(moment, GSIZE, axis=1)[:, None, None, :]


def finish_stats(sum_plain, sum_square, number):
    average = sum_plain / number
    variance = sum_square / number - average * average
    return (average, lax.rsqrt(variance + 1e-05))


def reduced_stats(field, number):
    values = field.astype(jnp.float32)
    sum_plain, sum_square = lax.psum((group_sums(values), group_sums(values * values)), "rows")
    return finish_stats(sum_plain, sum_square, number)


def norm_backward(field, stats, gain, shift, incoming, number):
    average, inverse = stats
    values = field.astype(jnp.float32)
    normed = (values - expand_groups(average)) * expand_groups(inverse)
    linear = normed * gain + shift
    logistic = jax.nn.sigmoid(linear)
    scaled = incoming * logistic * (1.0 + linear * (1.0 - logistic)) * gain
    sum_first, sum_second = lax.psum((group_sums(scaled), group_sums(scaled * normed)), "rows")
    first = sum_first / number
    second = sum_second / number
    return expand_groups(inverse) * (scaled - expand_groups(first) - normed * expand_groups(second))


def conv_backward(gradient, weights):
    images, rows_here, breadth, channels = gradient.shape
    padded = extended(gradient, (("rows", 1),), 1)
    padded = jnp.pad(padded, ((0, 0), (0, 0), (1, 1), (0, 0)))
    pixels = images * rows_here * breadth
    shifted = []
    for tap_index in range(9):
        down_step = tap_index // 3 - 1
        side_step = tap_index % 3 - 1
        window = padded[
            :, 1 - down_step : 1 - down_step + rows_here, 1 - side_step : 1 - side_step + breadth, :
        ]
        shifted.append(window.reshape(pixels, channels))
    stacked = jnp.stack(shifted, axis=1)
    gathered = lax.all_gather(weights, "dp", axis=1, tiled=True)
    section = lax.all_gather(gathered, "rows", axis=2, tiled=True)
    columns = section.shape[2]
    window = stacked.reshape(pixels, 9 * columns)
    flat = jnp.transpose(section, (0, 2, 1)).reshape(9 * columns, section.shape[1])
    result = jnp.dot(window, flat, preferred_element_type=jnp.float32)
    return result.reshape(images, rows_here, breadth, channels)


def plain_body(
    latent, hidden, cotangent, filter_one, filter_two, gain_one, shift_one, gain_two, shift_two
):
    number = latent.shape[1] * lax.axis_size("rows") * latent.shape[2] * GSIZE
    stats_two = reduced_stats(hidden, number)
    back_two = conv_backward(cotangent, filter_two)
    hidden_grad = norm_backward(hidden, stats_two, gain_two, shift_two, back_two, number).astype(
        jnp.bfloat16
    )
    stats_one = reduced_stats(latent, number)
    back_one = conv_backward(hidden_grad, filter_one)
    latent_part = norm_backward(latent, stats_one, gain_one, shift_one, back_one, number)
    return (cotangent.astype(jnp.float32) + latent_part).astype(jnp.bfloat16)


def kernel(
    depth, rows, breadth,
    lat_hbm, hid_hbm, cot_hbm, raw1_hbm, raw2_hbm, gain1_hbm, shift1_hbm, gain2_hbm, shift2_hbm,
    out_ref,
    lat_ref, hid_ref, cot_ref, raw1, raw2, gain1, shift1, gain2, shift2, in_sem,
    cot_t, x_cot, hid_b, w1, w2, s1, s2, r1,
    xs1, xs2, y_ref, p1, q1, p2, q2, hg_s, hg_r,
    nrm1, act1, nrm2, act2, inv2_ref, st_s, st_b, par_ref,
    x_far, hid_two, hid_far, xs_far, p_far, q_far, nrm_far, act_far, hg_far, hg_two,
    z_send, z_recv, f_send, f_recv, b_send, b_recv, c_send, c_recv, h_send, h_recv,
    p_send, p_recv, o_send, o_recv, t_send, t_recv, d_send, d_recv, e_send, e_recv,
):
    d = lax.axis_index("dp")
    r = lax.axis_index("rows")
    chips = rows // 2
    c = r // 2
    k = lax.rem(r, 2)
    sibling = r + 1 - 2 * k
    channels, lanes = cot_t.shape
    block = channels // depth
    half = block // 2
    images = lanes // breadth
    wide = w1.shape[3]
    number = rows * breadth * GSIZE
    groups = channels // GSIZE
    bf16, f32 = jnp.bfloat16, jnp.float32

    def remote(src, dst, send, recv, **device):
        return pltpu.make_async_remote_copy(
            src_ref=src, dst_ref=dst, send_sem=send, recv_sem=recv,
            device_id=device, device_id_type=MESH,
        )

    pending = []
    loads = {
        name: pltpu.make_async_copy(src, dst, in_sem.at[index])
        for index, (name, src, dst) in enumerate((
            ("raw2", raw2_hbm, raw2), ("cot", cot_hbm, cot_ref), ("hid", hid_hbm, hid_ref),
            ("raw1", raw1_hbm, raw1), ("lat", lat_hbm, lat_ref), ("gain1", gain1_hbm, gain1),
            ("shift1", shift1_hbm, shift1), ("gain2", gain2_hbm, gain2), ("shift2", shift2_hbm, shift2),
        ))
    }
    loads["raw2"].start()

    barrier = pltpu.get_barrier_semaphore()

    middle = (d > 0) & (d < depth - 1)
    partner = d + 1 - 2 * lax.rem(d, 2)
    lent = jnp.where(2 * d < depth, 1, 0)

    @pl.when(d > 0)
    def _():
        pl.semaphore_signal(barrier, inc=1, device_id={"dp": d - 1}, device_id_type=MESH)

    @pl.when(d < depth - 1)
    def _():
        pl.semaphore_signal(barrier, inc=1, device_id={"dp": d + 1}, device_id_type=MESH)

    for off in range(1, rows):
        pl.semaphore_signal(barrier, inc=1, device_id={"rows": lax.rem(r + off, rows)}, device_id_type=MESH)

    for name, load in loads.items():
        if name != "raw2":
            load.start()

    pad = wide - 3 * half
    own = k == c // 2
    tall = 3 * half
    w2[d, k, :, tall:] = jnp.zeros((tall, pad), bf16)
    s2[:, tall:] = jnp.zeros((tall, pad), bf16)
    for part in range(2):
        w1[d, part, :, tall:] = jnp.zeros((tall, pad), bf16)
        for side_core in range(2):
            s1[part, side_core, :, :, 3 * GSIZE :] = jnp.zeros((3, half, s1.shape[4] - 3 * GSIZE), bf16)
    for xs in (xs1, xs2, xs_far):
        for part in range(2):
            for h in range(rows):
                xs[part, h, 3 * half :] = jnp.zeros((pad, lanes), bf16)
    loads["raw2"].wait()

    def arrange(ready, raw, which):
        start = pl.multiple_of(which * half, 16)
        for tap in range(TAPS):
            down, side = tap // 3, tap % 3
            ready[down * half : (down + 1) * half, side * half : (side + 1) * half] = raw[
                tap, pl.ds(start, half), :
            ]

    def pack(ready):
        for at in range((tall - 128) // pad):
            ready[pad * at : pad * (at + 1), tall:] = ready[tall - pad :, 128 + pad * at : 128 + pad * (at + 1)]

    def unpack(w, origin):
        for part in range(2):
            pieces = [w[origin, part, pad * at : pad * (at + 1), tall:] for at in range((tall - 128) // pad)]
            full = jnp.concatenate(pieces + [jnp.zeros((pad, pad), bf16)], axis=1)
            w[origin, part, tall - pad :, 128:] = full

    arrange(w2.at[d, k], raw2, k)

    pl.semaphore_wait(barrier, rows + jnp.where(middle, 1, 0))

    segments = ((tall, 0, 128), (tall - pad, 128, wide))

    def hop(which, w, origin, part, seg, way):
        deep, low, high = segments[seg]
        piece = w.at[origin, part, 0:deep, low:high]
        return remote(
            piece, piece, z_send.at[which, way, seg], z_recv.at[which, origin, part, seg], dp=d + 1 - 2 * way
        )

    near = jnp.minimum(d, depth - 1 - d)

    def nth(step):
        value = step - near if step == 1 else step
        return jnp.where(2 * d < depth, value, depth - 1 - value)

    def start_hops(which, w, part, ways=(0, 1), segs=(0, 1)):
        for way in ways:
            @pl.when((d < depth - 1) if way == 0 else (d > 0))
            def _():
                for seg in segs:
                    hop(which, w, d, part, seg, way).start()

    def start_one(ways):
        for part in (k, 1 - k):
            start_hops(1, w1, part, ways)

    def forward(which, w, step, index):
        origin = nth(step)
        part, seg = (k, 1 - k)[index // 2], index % 2
        for way in range(2):
            @pl.when(middle & ((origin < d) if way == 0 else (origin > d)))
            def _():
                copy = hop(which, w, origin, part, seg, way)
                copy.wait_recv()
                copy.start()

    def take(which, w, step, segs=(0, 1)):
        for part in (k, 1 - k):
            for seg in segs:
                hop(which, w, nth(step), part, seg, 0).wait_recv()

    def take_end(which, w, step, segs=(0, 1)):
        @pl.when(jnp.logical_not(middle))
        def _():
            take(which, w, step, segs)

    def wait_hops(which, w, spans):
        for here, way, low, high in spans:
            @pl.when(d == here)
            def _():
                for seg, (deep, left, right) in enumerate(segments):
                    span = w.at[low:high, :, 0:deep, left:right]
                    remote(
                        span, span, z_send.at[which, way, seg], z_recv.at[which, 0, 0, 0], dp=d + 1 - 2 * way
                    ).wait_send()

    start_hops(0, w2, k, segs=(0,))
    pack(w2.at[d, k])
    start_hops(0, w2, k, segs=(1,))
    arrange(s2, raw2, 1 - k)
    pack(s2)
    twin = remote(s2, w2.at[d, k], b_send.at[0], b_recv.at[0], rows=sibling)
    twin.start()
    pending.append(twin)

    loads["cot"].wait()
    cot_t[...] = cot_ref[...].T

    def piece_of(to):
        return cot_t.at[pl.ds(pl.multiple_of((to // 2) * block, block), block), :]

    for off in range(1, chips):
        to = 2 * lax.rem(c + off, chips) + k
        remote(piece_of(to), x_cot.at[k, c], c_send.at[0], c_recv.at[0], rows=to).start()
    x_cot[k, c] = piece_of(r)[...]

    loads["raw1"].wait()
    for part in range(2):
        for side_core in range(2):
            ready = s1.at[part, side_core]
            for tap in range(TAPS):
                down, side = tap // 3, tap % 3
                ready[down, :, side * GSIZE : (side + 1) * GSIZE] = raw1[
                    tap, side_core * half : (side_core + 1) * half, part * GSIZE : (part + 1) * GSIZE
                ]

    for part in range(2):
        for side_core in range(2):
            to = 2 * (2 * k + part) + side_core

            @pl.when(to != r)
            def _():
                remote(s1.at[part, side_core], r1.at[c], f_send.at[0], f_recv.at[0], rows=to).start()

            @pl.when(to == r)
            def _():
                r1[c] = s1[part, side_core]

    loads["hid"].wait()
    hid_full = hid_ref[...].astype(f32).T
    for to in range(rows):
        parts = [
            hid_full[block * b + GSIZE * (to // 2) : block * b + GSIZE * (to // 2 + 1)]
            for b in (to % 2, to % 2 + 2)
        ]
        for slot in range(2):
            hid_two[to, slot] = parts[slot].astype(bf16)
    for off in range(1, rows):
        to = lax.rem(r + off, rows)
        remote(hid_two.at[to], hid_b.at[:, r], h_send.at[0], h_recv.at[0], rows=to).start()
    hid_b[:, r] = hid_two[r]

    remote(s2, w2.at[d, 1 - k], b_send.at[0], b_recv.at[0], rows=sibling).wait_recv()
    start_hops(0, w2, 1 - k)

    forward(0, w2, 1, 0)
    loads["lat"].wait()
    lane = lax.broadcasted_iota(jnp.int32, (1, lanes), 1)
    column = lax.rem(lane, breadth)
    image_of = lax.div(lane, breadth)
    quarter = lax.rem(lane, breadth) // (breadth // 4)

    def image_totals(per_lane):
        total = jnp.zeros_like(per_lane)
        for image in range(images):
            mine = image_of == image
            part = jnp.sum(jnp.where(mine, per_lane, 0.0), axis=1, keepdims=True)
            total = jnp.where(mine, part, total)
        return total

    def pack_sums(one, two):
        one, two = image_totals(one), image_totals(two)
        top, low = slice(0, groups // 2), slice(groups // 2, groups)
        return jnp.where(
            quarter == 0, one[top], jnp.where(quarter == 1, two[top], jnp.where(quarter == 2, one[low], two[low]))
        )

    def send_sums(which, packed):
        st_s[which] = packed
        for off in range(1, rows):
            to = lax.rem(r + off, rows)
            remote(st_s.at[which], st_b.at[which, r], t_send.at[which], t_recv.at[which], rows=to).start()
        st_b[which, r] = packed

    def wait_sums(which):
        span = st_b.at[which, 0 : rows - 1]
        remote(span, span, t_send.at[which], t_recv.at[which], rows=sibling).wait_recv()
        total = st_b[which, 0]
        for h in range(1, rows):
            total = total + st_b[which, h]
        total = total * (1.0 / number)
        full = []
        for at in range(4):
            mine = jnp.where(quarter == at, total, 0.0)
            pair = mine + pltpu.roll(mine, ((1 if at % 2 == 0 else -1) * breadth // 4) % lanes, 1)
            full.append(pair + pltpu.roll(pair, ((1 if at < 2 else -1) * breadth // 2) % lanes, 1))
        return jnp.concatenate([full[0], full[2]], axis=0), jnp.concatenate([full[1], full[3]], axis=0)

    def spread(moment):
        return jnp.broadcast_to(moment[:, None, :], (groups, GSIZE, lanes)).reshape(channels, lanes)

    def by_group(values):
        return jnp.sum(values.reshape(groups, GSIZE, lanes), axis=1)

    nrm1[...] = lat_ref[...].astype(f32).T
    send_sums(0, pack_sums(by_group(nrm1[...]), by_group(nrm1[...] * nrm1[...])))

    for name in ("gain1", "shift1", "gain2", "shift2"):
        loads[name].wait()
    raw_params = [p[...].reshape(1, channels) for p in (gain1, shift1, gain2, shift2)]
    par_ref[...] = jnp.concatenate(raw_params + raw_params, axis=0).T

    def store_shifts(xs, part, h, values):
        left = jnp.where(column == breadth - 1, 0.0, pltpu.roll(values, lanes - 1, 1))
        right = jnp.where(column == 0, 0.0, pltpu.roll(values, 1, 1))
        xs[part, h, 0:half] = left.astype(bf16)
        xs[part, h, half : 2 * half] = values.astype(bf16)
        xs[part, h, 2 * half : 3 * half] = right.astype(bf16)

    def wait_group(src, dst, send, recv):
        remote(src, dst, send, recv, rows=sibling).wait_recv()

    forward(0, w2, 1, 1)
    everyone = x_cot.at[0, 0 : chips - 1]
    wait_group(everyone, everyone, c_send.at[0], c_recv.at[0])

    def share(x, at):
        return remote(x.at[k], x.at[k], d_send.at[at], d_recv.at[at], rows=sibling)

    def shift_rows(x, xs):
        for h in range(rows):
            values = x[h % 2, h // 2].astype(f32)
            for part in range(2):
                store_shifts(xs, part, h, values[part * half : (part + 1) * half])

    share(x_cot, 0).start()
    lend_cot = remote(x_cot.at[k], x_far.at[k], c_send.at[1], c_recv.at[1], dp=partner)
    lend_hid = remote(hid_b.at[lent], hid_far, h_send.at[1], h_recv.at[1], dp=partner)

    @pl.when(jnp.logical_not(middle))
    def _():
        lend_cot.start()

    forward(0, w2, 1, 2)
    share(x_cot, 0).wait_recv()
    shift_rows(x_cot, xs2)

    def conv(w, origin, xs):
        for h in range(0, rows, 2):
            total = None
            for part in range(2):
                pair = jnp.concatenate([xs[part, h], xs[part, h + 1]], axis=1)
                term = jnp.dot(w[origin, part], pair, preferred_element_type=f32)
                total = term if total is None else total + term
            y_ref[h] = total[:, :lanes]
            y_ref[h + 1] = total[:, lanes:]

    def row_of(h):
        total = y_ref[h, half : 2 * half]
        if h + 1 < rows:
            total = total + y_ref[h + 1, 0:half]
        if h > 0:
            total = total + y_ref[h - 1, 2 * half : 3 * half]
        return total

    def conv_two(origin, xs, p, q, send, recv):
        conv(w2, origin, xs)
        for h in range(0, rows, 2):
            low, high = row_of(h), row_of(h + 1)
            for j in range(2):
                both = [low[j * GSIZE : (j + 1) * GSIZE], high[j * GSIZE : (j + 1) * GSIZE]]
                p[j, h // 2] = jnp.concatenate(both, axis=0).astype(bf16)
        for j in range(2):
            to = 2 * (2 * k + j) + lax.rem(origin, 2)

            @pl.when(to != r)
            def _():
                remote(p.at[j], q.at[c], send, recv, rows=to).start()

            @pl.when(to == r)
            def _():
                q[c] = p[j]

    def conv_own(origin):
        slot = origin // 2
        conv_two(origin, xs2, p1.at[origin], q1.at[slot], p_send.at[0], p_recv.at[slot])

    def conv_far(step):
        conv_two(nth(step), xs_far, p_far.at[step - 2], q_far, p_send.at[1], p_recv.at[2])

    def conv_one(origin):
        conv(w1, origin, xs1)
        for h in range(rows):
            p2[origin, h] = row_of(h).astype(bf16)
        for off in range(1, rows):
            to = lax.rem(r + off, rows)
            remote(p2.at[origin, to], q2.at[origin, r], o_send.at[0], o_recv.at[origin], rows=to).start()
        q2[origin, r] = p2[origin, r]

    conv_own(d)
    forward(0, w2, 1, 3)
    for count, here in ((chips - 1, own), (chips, jnp.logical_not(own))):
        @pl.when(here)
        def _():
            span = r1.at[0:count]
            wait_group(span, span, f_send.at[0], f_recv.at[0])

    for part in range(2):
        for j in range(2):
            for side in range(3):
                at = side * half + j * GSIZE
                piece = r1[2 * j + part, :, :, side * GSIZE : (side + 1) * GSIZE]
                w1[d, part, :, at : at + GSIZE] = piece.reshape(tall, GSIZE)
        pack(w1.at[d, part])

    def start_inner(toward):
        for here, way in ((1, toward), (2, 1 - toward)):
            @pl.when(d == here)
            def _():
                start_one((way,))

    start_inner(1)

    take_end(0, w2, 1)
    unpack(w2, nth(1))
    conv_own(nth(1))
    @pl.when(middle)
    def _():
        take(0, w2, 2)
        unpack(w2, nth(2))
        conv_own(nth(2))

    def activation(normed, gain, shift):
        linear = normed * gain + shift
        logistic = 1.0 / (1.0 + jnp.exp(-linear))
        return logistic * (1.0 + linear * (1.0 - logistic)) * gain

    everyone = hid_two.at[0 : rows - 1]
    wait_group(everyone, everyone, h_send.at[0], h_recv.at[0])

    @pl.when(jnp.logical_not(middle))
    def _():
        lend_hid.start()
        start_one((0, 1))

    def field_stats(field, slot, nrm, act, inverse_at):
        plain = jnp.zeros((GSIZE, lanes), f32)
        square = jnp.zeros((GSIZE, lanes), f32)
        for h in range(rows):
            values = field[h].astype(f32)
            plain += values
            square += values * values
        average = image_totals(jnp.sum(plain, axis=0, keepdims=True)) * (1.0 / number)
        meansq = image_totals(jnp.sum(square, axis=0, keepdims=True)) * (1.0 / number)
        inverse = lax.rsqrt(meansq - average * average + 1e-05)
        inv2_ref[inverse_at : inverse_at + 1] = inverse
        at = pl.multiple_of((k + 2 * slot) * block + GSIZE * c, GSIZE)
        gain = par_ref[pl.ds(at, GSIZE), 2:3]
        shift = par_ref[pl.ds(at, GSIZE), 3:4]
        for h in range(rows):
            normed = (field[h].astype(f32) - average) * inverse
            spot = (h % 2) * GSIZE
            nrm[h // 2, spot : spot + GSIZE] = normed
            act[h // 2, spot : spot + GSIZE] = activation(normed, gain, shift)

    for slot in range(2):
        field_stats(hid_b.at[slot], slot, nrm2.at[slot], act2.at[slot], slot)

    @pl.when(middle)
    def _():
        start_inner(0)
        lend_cot.wait_recv()
        share(x_far, 1).start()
        share(x_far, 1).wait_recv()
        shift_rows(x_far, xs_far)
        conv_far(2)
        take(0, w2, 3)
        unpack(w2, nth(3))
        conv_far(3)
        conv_own(nth(3))

    forward(1, w1, 2, 0)
    forward(1, w1, 1, 0)
    @pl.when(middle)
    def _():
        lend_hid.wait_recv()
        field_stats(hid_far, lent, nrm_far, act_far, 2)

    forward(1, w1, 2, 1)
    forward(1, w1, 1, 1)

    average1, meansq1 = wait_sums(0)
    inverse1 = lax.rsqrt(meansq1 - average1 * average1 + 1e-05)
    for g in range(groups):
        rows_g = pl.ds(g * GSIZE, GSIZE)
        normed = (nrm1[rows_g, :] - average1[g : g + 1]) * inverse1[g : g + 1]
        nrm1[rows_g, :] = normed
        act1[rows_g, :] = activation(normed, par_ref[rows_g, 0:1], par_ref[rows_g, 1:2])

    def norm_two(slot, recv, q, nrm, act, inverse, dst):
        for count, here in ((chips - 1, own), (chips, jnp.logical_not(own))):
            @pl.when(here)
            def _():
                span = q.at[0:count]
                wait_group(span, span, p_send.at[0], recv)

        sum_first = jnp.zeros((2 * GSIZE, lanes), f32)
        sum_second = jnp.zeros((2 * GSIZE, lanes), f32)
        scaled = []
        for m in range(rows // 2):
            total = q[0, m].astype(f32)
            for frm in range(1, chips):
                total = total + q[frm, m].astype(f32)
            value = total * act[m]
            scaled.append(value)
            sum_first += value
            sum_second += value * nrm[m]
        first = image_totals(jnp.sum(sum_first, axis=0, keepdims=True)) * (1.0 / number)
        second = image_totals(jnp.sum(sum_second, axis=0, keepdims=True)) * (1.0 / number)
        for m in range(rows // 2):
            dst[m] = (inverse * (scaled[m] - first - nrm[m] * second)).astype(bf16)

    def norm_own(slot):
        norm_two(
            slot, p_recv.at[slot], q1.at[slot], nrm2.at[slot], act2.at[slot],
            inv2_ref[pl.ds(slot, 1), :], hg_two.at[slot],
        )

    lend = remote(hg_far, hg_two.at[lent], e_send.at[0], e_recv.at[0], dp=partner)

    @pl.when(middle)
    def _():
        norm_two(lent, p_recv.at[2], q_far, nrm_far, act_far, inv2_ref[2:3, :], hg_far)
        lend.start()

    forward(1, w1, 2, 2)
    forward(1, w1, 1, 2)
    forward(1, w1, 2, 3)
    forward(1, w1, 1, 3)
    forward(1, w1, 3, 0)
    forward(1, w1, 3, 1)
    @pl.when(middle)
    def _():
        norm_own(0)
        norm_own(1)

    @pl.when(jnp.logical_not(middle))
    def _():
        norm_own(1 - lent)
        lend.wait_recv()

    for h in range(rows):
        spot = (h % 2) * GSIZE
        both = [hg_two[slot, h // 2].astype(f32)[spot : spot + GSIZE] for slot in range(2)]
        hg_s[h] = jnp.concatenate(both, axis=0).astype(bf16)
    swap = remote(hg_s, hg_r, b_send.at[1], b_recv.at[1], rows=sibling)
    swap.start()
    pending.append(swap)
    for h in range(rows):
        store_shifts(xs1, k, h, hg_s[h].astype(f32))
    swap.wait_recv()
    for h in range(rows):
        store_shifts(xs1, 1 - k, h, hg_r[h].astype(f32))

    forward(1, w1, 3, 2)
    conv_one(d)
    take_end(1, w1, 1)
    unpack(w1, nth(1))
    conv_one(nth(1))
    forward(1, w1, 3, 3)
    take_end(1, w1, 2)
    unpack(w1, nth(2))
    conv_one(nth(2))
    take_end(1, w1, 3)
    unpack(w1, nth(3))
    conv_one(nth(3))
    for origin in range(depth):
        span = q2.at[origin, 0 : rows - 1]
        wait_group(span, span, o_send.at[0], o_recv.at[origin])

    one, two = [], []
    for origin in range(depth):
        for part in range(2):
            total = q2[origin, part].astype(f32)
            for frm in range(1, chips):
                total = total + q2[origin, 2 * frm + part].astype(f32)
            at = pl.ds(origin * block + part * half, half)
            value = total * act1[at, :]
            act1[at, :] = value
            one.append(jnp.sum(value.reshape(2, GSIZE, lanes), axis=1))
            two.append(jnp.sum((value * nrm1[at, :]).reshape(2, GSIZE, lanes), axis=1))
    send_sums(1, pack_sums(jnp.concatenate(one, axis=0), jnp.concatenate(two, axis=0)))
    first1, second1 = wait_sums(1)
    value = spread(inverse1) * (act1[...] - spread(first1) - nrm1[...] * spread(second1))
    out_ref[...] = (cot_t[...].astype(f32) + value).astype(bf16).T

    for copy in pending:
        copy.wait_send()
    def sent(span, send, recv):
        remote(span, span, send, recv, rows=sibling).wait_send()

    sent(x_cot.at[0, 0 : chips - 1], c_send.at[0], c_recv.at[0])
    share(x_cot, 0).wait_send()
    sent(hid_two.at[0 : rows - 1], h_send.at[0], h_recv.at[0])
    for which in range(2):
        sent(st_b.at[which, 0 : rows - 1], t_send.at[which], t_recv.at[which])
    sent(p2.at[:, 0 : rows - 1], o_send.at[0], o_recv.at[0])
    for count, here in ((chips - 1, own), (chips, jnp.logical_not(own))):
        @pl.when(here)
        def _():
            sent(r1.at[0:count], f_send.at[0], f_recv.at[0])

            @pl.when(middle)
            def _():
                sent(q1.at[:, 0:count], p_send.at[0], p_recv.at[0])
                sent(q_far.at[0:count], p_send.at[1], p_recv.at[2])

            @pl.when(jnp.logical_not(middle))
            def _():
                sent(q1.at[0, 0:count], p_send.at[0], p_recv.at[0])

    @pl.when(middle)
    def _():
        share(x_far, 1).wait_send()
        lend.wait_send()

    @pl.when(jnp.logical_not(middle))
    def _():
        lend_cot.wait_send()
        lend_hid.wait_send()

    last = depth - 1
    wait_hops(0, w2, [(0, 0, 0, 1), (1, 0, 0, 2), (1, 1, 1, 2), (2, 0, 2, 3), (2, 1, 2, 4), (3, 1, 3, 4)])
    wait_hops(
        1, w1,
        [(here, 0, 0, here + 1) for here in range(last)] + [(here, 1, here, depth) for here in range(1, depth)],
    )


def kernel_body(
    depth, rows,
    latent, hidden, cotangent, filter_one, filter_two, gain_one, shift_one, gain_two, shift_two,
):
    images, _, breadth, channels = latent.shape
    lanes = images * breadth
    block = channels // depth
    half = block // 2
    chips = rows // 2
    wide = -(-3 * half // 128) * 128
    narrow = -(-3 * GSIZE // 128) * 128
    groups = channels // GSIZE
    bf16, f32 = jnp.bfloat16, jnp.float32
    dma = pltpu.SemaphoreType.DMA
    out = pl.pallas_call(
        functools.partial(kernel, depth, rows, breadth),
        out_shape=jax.ShapeDtypeStruct((lanes, channels), bf16),
        in_specs=[pl.BlockSpec(memory_space=pltpu.HBM)] * 9,
        out_specs=pl.BlockSpec(memory_space=pltpu.VMEM),
        scratch_shapes=[
            pltpu.VMEM((lanes, channels), bf16),
            pltpu.VMEM((lanes, channels), bf16),
            pltpu.VMEM((lanes, channels), bf16),
            pltpu.VMEM(filter_one.shape, bf16),
            pltpu.VMEM(filter_two.shape, bf16),
            pltpu.VMEM((channels,), f32),
            pltpu.VMEM((channels,), f32),
            pltpu.VMEM((channels,), f32),
            pltpu.VMEM((channels,), f32),
            dma((9,)),
            pltpu.VMEM((channels, lanes), bf16),
            pltpu.VMEM((2, chips, block, lanes), bf16),
            pltpu.VMEM((2, rows, GSIZE, lanes), bf16),
            pltpu.VMEM((depth, 2, 3 * half, wide), bf16),
            pltpu.VMEM((depth, 2, 3 * half, wide), bf16),
            pltpu.VMEM((2, 2, 3, half, narrow), bf16),
            pltpu.VMEM((3 * half, wide), bf16),
            pltpu.VMEM((chips, 3, half, narrow), bf16),
            pltpu.VMEM((2, rows, wide, lanes), bf16),
            pltpu.VMEM((2, rows, wide, lanes), bf16),
            pltpu.VMEM((rows, 3 * half, lanes), f32),
            pltpu.VMEM((depth, 2, rows // 2, 2 * GSIZE, lanes), bf16),
            pltpu.VMEM((2, chips, rows // 2, 2 * GSIZE, lanes), bf16),
            pltpu.VMEM((depth, rows, half, lanes), bf16),
            pltpu.VMEM((depth, rows, half, lanes), bf16),
            pltpu.VMEM((rows, 2 * GSIZE, lanes), bf16),
            pltpu.VMEM((rows, 2 * GSIZE, lanes), bf16),
            pltpu.VMEM((channels, lanes), f32),
            pltpu.VMEM((channels, lanes), f32),
            pltpu.VMEM((2, rows // 2, 2 * GSIZE, lanes), f32),
            pltpu.VMEM((2, rows // 2, 2 * GSIZE, lanes), f32),
            pltpu.VMEM((4, lanes), f32),
            pltpu.VMEM((2, groups // 2, lanes), f32),
            pltpu.VMEM((2, rows, groups // 2, lanes), f32),
            pltpu.VMEM((channels, 8), f32),
            pltpu.VMEM((2, chips, block, lanes), bf16),
            pltpu.VMEM((rows, 2, GSIZE, lanes), bf16),
            pltpu.VMEM((rows, GSIZE, lanes), bf16),
            pltpu.VMEM((2, rows, wide, lanes), bf16),
            pltpu.VMEM((2, 2, rows // 2, 2 * GSIZE, lanes), bf16),
            pltpu.VMEM((chips, rows // 2, 2 * GSIZE, lanes), bf16),
            pltpu.VMEM((rows // 2, 2 * GSIZE, lanes), f32),
            pltpu.VMEM((rows // 2, 2 * GSIZE, lanes), f32),
            pltpu.VMEM((rows // 2, 2 * GSIZE, lanes), bf16),
            pltpu.VMEM((2, rows // 2, 2 * GSIZE, lanes), bf16),
            dma((2, 2, 2)), dma((2, depth, 2, 2)),
            dma((1,)), dma((1,)),
            dma((2,)), dma((2,)),
            dma((2,)), dma((2,)),
            dma((2,)), dma((2,)),
            dma((2,)), dma((3,)),
            dma((1,)), dma((depth,)),
            dma((2,)), dma((2,)),
            dma((2,)), dma((2,)),
            dma((1,)), dma((1,)),
        ],
        compiler_params=pltpu.CompilerParams(
            collective_id=0, has_side_effects=True, vmem_limit_bytes=48 * 1024 * 1024
        ),
    )(
        *[
            pltpu.with_memory_space_constraint(array, pltpu.HBM)
            for array in (
                latent.reshape(lanes, channels), hidden.reshape(lanes, channels),
                cotangent.reshape(lanes, channels), filter_one, filter_two,
                gain_one, shift_one, gain_two, shift_two,
            )
        ]
    )
    return out.reshape(latent.shape)


def solution(mesh):
    depth, rows = mesh.shape["dp"], mesh.shape["rows"]
    in_specs = (
        P("dp", "rows", None, None),
        P("dp", "rows", None, None),
        P("dp", "rows", None, None),
        P(None, "dp", "rows"),
        P(None, "dp", "rows"),
        P(),
        P(),
        P(),
        P(),
    )

    def body(latent, *rest):
        images, rows_here, breadth, channels = latent.shape
        fits = (
            rows_here == 1
            and images * breadth == 128
            and breadth % 4 == 0
            and depth == 4
            and rows == 2 * depth
            and channels == GROUPS * GSIZE
            and channels == depth * (rows // 2) * GSIZE
        )
        if fits:
            return kernel_body(depth, rows, latent, *rest)
        return plain_body(latent, *rest)

    return jax.shard_map(
        body, mesh=mesh, in_specs=in_specs, out_specs=P("dp", "rows", None, None), check_vma=False
    )
```

```python
import functools

import jax
import jax.numpy as jnp
from jax import lax
from jax.experimental import pallas as pl
from jax.experimental.pallas import tpu as pltpu
from jax.sharding import PartitionSpec as P

GROUPS = 16
GSIZE = 40
TAPS = 9
MESH = pl.DeviceIdType.MESH


def extended(block, sides, width):
    for axis, dim in sides:
        count = lax.axis_size(axis)
        forward = [(i, i + 1) for i in range(count - 1)]
        backward = [(target, source) for source, target in forward]
        low = lax.ppermute(
            lax.slice_in_dim(block, block.shape[dim] - width, None, axis=dim), axis, forward
        )
        high = lax.ppermute(lax.slice_in_dim(block, 0, width, axis=dim), axis, backward)
        block = jnp.concatenate([low, block, high], axis=dim)
    return block


def group_sums(values):
    per_channel = jnp.sum(values, axis=(1, 2))
    return jnp.sum(per_channel.reshape(per_channel.shape[0], GROUPS, -1), axis=2)


def expand_groups(moment):
    return jnp.repeat(moment, GSIZE, axis=1)[:, None, None, :]


def finish_stats(sum_plain, sum_square, number):
    average = sum_plain / number
    variance = sum_square / number - average * average
    return (average, lax.rsqrt(variance + 1e-05))


def reduced_stats(field, number):
    values = field.astype(jnp.float32)
    sum_plain, sum_square = lax.psum((group_sums(values), group_sums(values * values)), "rows")
    return finish_stats(sum_plain, sum_square, number)


def norm_backward(field, stats, gain, shift, incoming, number):
    average, inverse = stats
    values = field.astype(jnp.float32)
    normed = (values - expand_groups(average)) * expand_groups(inverse)
    linear = normed * gain + shift
    logistic = jax.nn.sigmoid(linear)
    scaled = incoming * logistic * (1.0 + linear * (1.0 - logistic)) * gain
    sum_first, sum_second = lax.psum((group_sums(scaled), group_sums(scaled * normed)), "rows")
    first = sum_first / number
    second = sum_second / number
    return expand_groups(inverse) * (scaled - expand_groups(first) - normed * expand_groups(second))


def conv_backward(gradient, weights):
    images, rows_here, breadth, channels = gradient.shape
    padded = extended(gradient, (("rows", 1),), 1)
    padded = jnp.pad(padded, ((0, 0), (0, 0), (1, 1), (0, 0)))
    pixels = images * rows_here * breadth
    shifted = []
    for tap_index in range(9):
        down_step = tap_index // 3 - 1
        side_step = tap_index % 3 - 1
        window = padded[
            :, 1 - down_step : 1 - down_step + rows_here, 1 - side_step : 1 - side_step + breadth, :
        ]
        shifted.append(window.reshape(pixels, channels))
    stacked = jnp.stack(shifted, axis=1)
    gathered = lax.all_gather(weights, "dp", axis=1, tiled=True)
    section = lax.all_gather(gathered, "rows", axis=2, tiled=True)
    columns = section.shape[2]
    window = stacked.reshape(pixels, 9 * columns)
    flat = jnp.transpose(section, (0, 2, 1)).reshape(9 * columns, section.shape[1])
    result = jnp.dot(window, flat, preferred_element_type=jnp.float32)
    return result.reshape(images, rows_here, breadth, channels)


def plain_body(
    latent, hidden, cotangent, filter_one, filter_two, gain_one, shift_one, gain_two, shift_two
):
    number = latent.shape[1] * lax.axis_size("rows") * latent.shape[2] * GSIZE
    stats_two = reduced_stats(hidden, number)
    back_two = conv_backward(cotangent, filter_two)
    hidden_grad = norm_backward(hidden, stats_two, gain_two, shift_two, back_two, number).astype(
        jnp.bfloat16
    )
    stats_one = reduced_stats(latent, number)
    back_one = conv_backward(hidden_grad, filter_one)
    latent_part = norm_backward(latent, stats_one, gain_one, shift_one, back_one, number)
    return (cotangent.astype(jnp.float32) + latent_part).astype(jnp.bfloat16)


def kernel(
    depth, rows, breadth,
    lat_hbm, hid_hbm, cot_hbm, raw1_hbm, raw2_hbm, gain1_hbm, shift1_hbm, gain2_hbm, shift2_hbm,
    out_ref,
    lat_ref, hid_ref, cot_ref, raw1, raw2, gain1, shift1, gain2, shift2, in_sem,
    cot_t, x_cot, hid_b, w1, w2, s1, s2, r1,
    xs1, xs2, y_ref, p1, q1, p2, q2, hg_s, hg_r,
    nrm1, act1, nrm2, act2, inv2_ref, st_s, st_b, par_ref,
    sums_ref, x_far, hid_two, hid_far, xs_far, p_far, q_far, nrm_far, act_far, hg_far, hg_two,
    z_send, z_recv, f_send, f_recv, b_send, b_recv, c_send, c_recv, h_send, h_recv,
    p_send, p_recv, o_send, o_recv, t_send, t_recv, d_send, d_recv, e_send, e_recv,
):
    d = lax.axis_index("dp")
    r = lax.axis_index("rows")
    chips = rows // 2
    c = r // 2
    k = lax.rem(r, 2)
    sibling = r + 1 - 2 * k
    channels, lanes = cot_t.shape
    block = channels // depth
    half = block // 2
    images = lanes // breadth
    wide = w1.shape[3]
    number = rows * breadth * GSIZE
    groups = channels // GSIZE
    bf16, f32 = jnp.bfloat16, jnp.float32

    def remote(src, dst, send, recv, **device):
        return pltpu.make_async_remote_copy(
            src_ref=src, dst_ref=dst, send_sem=send, recv_sem=recv,
            device_id=device, device_id_type=MESH,
        )

    pending = []
    loads = {
        name: pltpu.make_async_copy(src, dst, in_sem.at[index])
        for index, (name, src, dst) in enumerate((
            ("raw2", raw2_hbm, raw2), ("cot", cot_hbm, cot_ref), ("hid", hid_hbm, hid_ref),
            ("raw1", raw1_hbm, raw1), ("lat", lat_hbm, lat_ref), ("gain1", gain1_hbm, gain1),
            ("shift1", shift1_hbm, shift1), ("gain2", gain2_hbm, gain2), ("shift2", shift2_hbm, shift2),
        ))
    }
    loads["raw2"].start()

    barrier = pltpu.get_barrier_semaphore()

    middle = (d > 0) & (d < depth - 1)
    partner = d + 1 - 2 * lax.rem(d, 2)
    lent = jnp.where(2 * d < depth, 1, 0)

    @pl.when(d > 0)
    def _():
        pl.semaphore_signal(barrier, inc=1, device_id={"dp": d - 1}, device_id_type=MESH)

    @pl.when(d < depth - 1)
    def _():
        pl.semaphore_signal(barrier, inc=1, device_id={"dp": d + 1}, device_id_type=MESH)

    for off in range(1, rows):
        pl.semaphore_signal(barrier, inc=1, device_id={"rows": lax.rem(r + off, rows)}, device_id_type=MESH)

    for name, load in loads.items():
        if name != "raw2":
            load.start()

    pad = wide - 3 * half
    own = k == c // 2
    tall = 3 * half
    w2[d, k, :, tall:] = jnp.zeros((tall, pad), bf16)
    s2[:, tall:] = jnp.zeros((tall, pad), bf16)
    for part in range(2):
        w1[d, part, :, tall:] = jnp.zeros((tall, pad), bf16)
        for side_core in range(2):
            s1[part, side_core, :, :, 3 * GSIZE :] = jnp.zeros((3, half, s1.shape[4] - 3 * GSIZE), bf16)
    for xs in (xs1, xs2, xs_far):
        for part in range(2):
            for h in range(rows):
                xs[part, h, 3 * half :] = jnp.zeros((pad, lanes), bf16)
    loads["raw2"].wait()

    def arrange(ready, raw, which):
        start = pl.multiple_of(which * half, 16)
        for tap in range(TAPS):
            down, side = tap // 3, tap % 3
            ready[down * half : (down + 1) * half, side * half : (side + 1) * half] = raw[
                tap, pl.ds(start, half), :
            ]

    def pack(ready):
        for at in range((tall - 128) // pad):
            ready[pad * at : pad * (at + 1), tall:] = ready[tall - pad :, 128 + pad * at : 128 + pad * (at + 1)]

    def unpack(w, origin):
        for part in range(2):
            pieces = [w[origin, part, pad * at : pad * (at + 1), tall:] for at in range((tall - 128) // pad)]
            full = jnp.concatenate(pieces + [jnp.zeros((pad, pad), bf16)], axis=1)
            w[origin, part, tall - pad :, 128:] = full

    arrange(w2.at[d, k], raw2, k)

    pl.semaphore_wait(barrier, rows + jnp.where(middle, 1, 0))

    segments = ((tall, 0, 128), (tall - pad, 128, wide))

    def hop(which, w, origin, part, seg, way):
        deep, low, high = segments[seg]
        piece = w.at[origin, part, 0:deep, low:high]
        return remote(
            piece, piece, z_send.at[which, way, seg], z_recv.at[which, origin - way, part, seg], dp=d + 1 - 2 * way
        )

    near = jnp.minimum(d, depth - 1 - d)

    def nth(step):
        value = step - near if step == 1 else step
        return jnp.where(2 * d < depth, value, depth - 1 - value)

    def start_hops(which, w, part, ways=(0, 1), segs=(0, 1)):
        for way in ways:
            @pl.when((d < depth - 1) if way == 0 else (d > 0))
            def _():
                for seg in segs:
                    hop(which, w, d, part, seg, way).start()

    def start_one(ways):
        for part in (k, 1 - k):
            start_hops(1, w1, part, ways)

    def forward(which, w, step, index):
        origin = nth(step)
        part, seg = (k, 1 - k)[index // 2], index % 2
        for way in range(2):
            @pl.when(middle & ((origin < d) if way == 0 else (origin > d)))
            def _():
                copy = hop(which, w, origin, part, seg, way)
                copy.wait_recv()
                copy.start()

    def take(which, w, step, segs=(0, 1)):
        for part in (k, 1 - k):
            for seg in segs:
                origin = nth(step)
                hop(which, w, origin, part, seg, jnp.where(origin > d, 1, 0)).wait_recv()

    def take_end(which, w, step, segs=(0, 1)):
        @pl.when(jnp.logical_not(middle))
        def _():
            take(which, w, step, segs)

    def wait_hops(which, w, spans):
        for here, way, low, high in spans:
            @pl.when(d == here)
            def _():
                for seg, (deep, left, right) in enumerate(segments):
                    span = w.at[low:high, :, 0:deep, left:right]
                    remote(
                        span, span, z_send.at[which, way, seg], z_recv.at[which, 0, 0, 0], dp=d + 1 - 2 * way
                    ).wait_send()

    start_hops(0, w2, k, segs=(0,))
    pack(w2.at[d, k])
    start_hops(0, w2, k, segs=(1,))
    arrange(s2, raw2, 1 - k)
    pack(s2)
    twin = remote(s2, w2.at[d, k], b_send.at[0], b_recv.at[0], rows=sibling)
    twin.start()
    pending.append(twin)

    loads["cot"].wait()
    cot_t[...] = cot_ref[...].T

    def piece_of(to):
        return cot_t.at[pl.ds(pl.multiple_of((to // 2) * block, block), block), :]

    for off in range(1, chips):
        to = 2 * lax.rem(c + off, chips) + k
        remote(piece_of(to), x_cot.at[k, c], c_send.at[0], c_recv.at[0], rows=to).start()
    x_cot[k, c] = piece_of(r)[...]

    loads["raw1"].wait()
    for part in range(2):
        for side_core in range(2):
            ready = s1.at[part, side_core]
            for tap in range(TAPS):
                down, side = tap // 3, tap % 3
                ready[down, :, side * GSIZE : (side + 1) * GSIZE] = raw1[
                    tap, side_core * half : (side_core + 1) * half, part * GSIZE : (part + 1) * GSIZE
                ]

    for part in range(2):
        for side_core in range(2):
            to = 2 * (2 * k + part) + side_core

            @pl.when(to != r)
            def _():
                remote(s1.at[part, side_core], r1.at[c], f_send.at[0], f_recv.at[0], rows=to).start()

            @pl.when(to == r)
            def _():
                r1[c] = s1[part, side_core]

    loads["hid"].wait()
    hid_full = hid_ref[...].astype(f32).T
    for to in range(rows):
        parts = [
            hid_full[block * b + GSIZE * (to // 2) : block * b + GSIZE * (to // 2 + 1)]
            for b in (to % 2, to % 2 + 2)
        ]
        for slot in range(2):
            hid_two[to, slot] = parts[slot].astype(bf16)
    for off in range(1, rows):
        to = lax.rem(r + off, rows)
        remote(hid_two.at[to], hid_b.at[:, r], h_send.at[0], h_recv.at[0], rows=to).start()
    hid_b[:, r] = hid_two[r]

    remote(s2, w2.at[d, 1 - k], b_send.at[0], b_recv.at[0], rows=sibling).wait_recv()
    start_hops(0, w2, 1 - k)

    forward(0, w2, 1, 0)
    loads["lat"].wait()
    lane = lax.broadcasted_iota(jnp.int32, (1, lanes), 1)
    column = lax.rem(lane, breadth)
    image_of = lax.div(lane, breadth)
    quarter = lax.rem(lane, breadth) // (breadth // 4)

    def image_totals(per_lane):
        total = jnp.zeros_like(per_lane)
        for image in range(images):
            mine = image_of == image
            part = jnp.sum(jnp.where(mine, per_lane, 0.0), axis=1, keepdims=True)
            total = jnp.where(mine, part, total)
        return total

    def pack_sums(one, two):
        one, two = image_totals(one), image_totals(two)
        top, low = slice(0, groups // 2), slice(groups // 2, groups)
        return jnp.where(
            quarter == 0, one[top], jnp.where(quarter == 1, two[top], jnp.where(quarter == 2, one[low], two[low]))
        )

    def send_sums(which, packed):
        st_s[which] = packed
        for off in range(1, rows):
            to = lax.rem(r + off, rows)
            remote(st_s.at[which], st_b.at[which, r], t_send.at[0], t_recv.at[which], rows=to).start()
        st_b[which, r] = packed

    def wait_sums(which):
        span = st_b.at[which, 0 : rows - 1]
        remote(span, span, t_send.at[0], t_recv.at[which], rows=sibling).wait_recv()
        total = st_b[which, 0]
        for h in range(1, rows):
            total = total + st_b[which, h]
        total = total * (1.0 / number)
        full = []
        for at in range(4):
            mine = jnp.where(quarter == at, total, 0.0)
            pair = mine + pltpu.roll(mine, ((1 if at % 2 == 0 else -1) * breadth // 4) % lanes, 1)
            full.append(pair + pltpu.roll(pair, ((1 if at < 2 else -1) * breadth // 2) % lanes, 1))
        return jnp.concatenate([full[0], full[2]], axis=0), jnp.concatenate([full[1], full[3]], axis=0)

    def spread(moment):
        return jnp.broadcast_to(moment[:, None, :], (groups, GSIZE, lanes)).reshape(channels, lanes)

    def by_group(values):
        return jnp.sum(values.reshape(groups, GSIZE, lanes), axis=1)

    nrm1[...] = lat_ref[...].astype(f32).T
    send_sums(0, pack_sums(by_group(nrm1[...]), by_group(nrm1[...] * nrm1[...])))

    for name in ("gain1", "shift1", "gain2", "shift2"):
        loads[name].wait()
    raw_params = [p[...].reshape(1, channels) for p in (gain1, shift1, gain2, shift2)]
    par_ref[...] = jnp.concatenate(raw_params + raw_params, axis=0).T

    def store_shifts(xs, part, h, values):
        left = jnp.where(column == breadth - 1, 0.0, pltpu.roll(values, lanes - 1, 1))
        right = jnp.where(column == 0, 0.0, pltpu.roll(values, 1, 1))
        xs[part, h, 0:half] = left.astype(bf16)
        xs[part, h, half : 2 * half] = values.astype(bf16)
        xs[part, h, 2 * half : 3 * half] = right.astype(bf16)

    def wait_group(src, dst, send, recv):
        remote(src, dst, send, recv, rows=sibling).wait_recv()

    forward(0, w2, 1, 1)
    everyone = x_cot.at[0, 0 : chips - 1]
    wait_group(everyone, everyone, c_send.at[0], c_recv.at[0])

    def share(x, at):
        return remote(x.at[k], x.at[k], d_send.at[at], d_recv.at[at], rows=sibling)

    def shift_rows(x, xs):
        for h in range(rows):
            values = x[h % 2, h // 2].astype(f32)
            for part in range(2):
                store_shifts(xs, part, h, values[part * half : (part + 1) * half])

    share(x_cot, 0).start()
    lend_cot = remote(x_cot.at[k], x_far.at[k], c_send.at[1], c_recv.at[1], dp=partner)
    lend_hid = remote(hid_b.at[lent], hid_far, h_send.at[1], h_recv.at[1], dp=partner)

    @pl.when(jnp.logical_not(middle))
    def _():
        lend_cot.start()

    forward(0, w2, 1, 2)
    share(x_cot, 0).wait_recv()
    shift_rows(x_cot, xs2)

    def conv(w, origin, xs):
        for h in range(0, rows, 2):
            total = None
            for part in range(2):
                pair = jnp.concatenate([xs[part, h], xs[part, h + 1]], axis=1)
                term = jnp.dot(w[origin, part], pair, preferred_element_type=f32)
                total = term if total is None else total + term
            y_ref[h] = total[:, :lanes]
            y_ref[h + 1] = total[:, lanes:]

    def row_of(h):
        total = y_ref[h, half : 2 * half]
        if h + 1 < rows:
            total = total + y_ref[h + 1, 0:half]
        if h > 0:
            total = total + y_ref[h - 1, 2 * half : 3 * half]
        return total

    def conv_two(origin, xs, p, q, send, recv):
        conv(w2, origin, xs)
        for h in range(0, rows, 2):
            low, high = row_of(h), row_of(h + 1)
            for j in range(2):
                both = [low[j * GSIZE : (j + 1) * GSIZE], high[j * GSIZE : (j + 1) * GSIZE]]
                p[j, h // 2] = jnp.concatenate(both, axis=0).astype(bf16)
        for j in range(2):
            to = 2 * (2 * k + j) + lax.rem(origin, 2)

            @pl.when(to != r)
            def _():
                remote(p.at[j], q.at[c], send, recv, rows=to).start()

            @pl.when(to == r)
            def _():
                q[c] = p[j]

    def conv_own(origin):
        slot = origin // 2
        conv_two(origin, xs2, p1.at[origin], q1.at[slot], p_send.at[0], p_recv.at[slot])

    def conv_far(step):
        conv_two(nth(step), xs_far, p_far.at[step - 2], q_far, p_send.at[1], p_recv.at[2])

    def conv_one(origin, last=0):
        conv(w1, origin, xs1)
        for h in range(rows):
            p2[origin, h] = row_of(h).astype(bf16)
        for off in range(1, rows):
            to = lax.rem(r + off, rows)
            remote(p2.at[origin, to], q2.at[origin, r], o_send.at[0], o_recv.at[last], rows=to).start()
        q2[origin, r] = p2[origin, r]

    conv_own(d)
    forward(0, w2, 1, 3)
    for count, here in ((chips - 1, own), (chips, jnp.logical_not(own))):
        @pl.when(here)
        def _():
            span = r1.at[0:count]
            wait_group(span, span, f_send.at[0], f_recv.at[0])

    for part in range(2):
        for j in range(2):
            for side in range(3):
                at = side * half + j * GSIZE
                piece = r1[2 * j + part, :, :, side * GSIZE : (side + 1) * GSIZE]
                w1[d, part, :, at : at + GSIZE] = piece.reshape(tall, GSIZE)
        pack(w1.at[d, part])

    def start_inner(toward):
        for here, way in ((1, toward), (2, 1 - toward)):
            @pl.when(d == here)
            def _():
                start_one((way,))

    start_inner(1)

    take_end(0, w2, 1)
    unpack(w2, nth(1))
    conv_own(nth(1))
    @pl.when(middle)
    def _():
        take(0, w2, 2)
        unpack(w2, nth(2))
        conv_own(nth(2))

    def activation(normed, gain, shift):
        linear = normed * gain + shift
        logistic = 1.0 / (1.0 + jnp.exp(-linear))
        return logistic * (1.0 + linear * (1.0 - logistic)) * gain

    everyone = hid_two.at[0 : rows - 1]
    wait_group(everyone, everyone, h_send.at[0], h_recv.at[0])

    @pl.when(jnp.logical_not(middle))
    def _():
        lend_hid.start()
        start_one((0, 1))

    def field_stats(field, slot, nrm, act, inverse_at):
        plain = jnp.zeros((GSIZE, lanes), f32)
        square = jnp.zeros((GSIZE, lanes), f32)
        for h in range(rows):
            values = field[h].astype(f32)
            plain += values
            square += values * values
        average = image_totals(jnp.sum(plain, axis=0, keepdims=True)) * (1.0 / number)
        meansq = image_totals(jnp.sum(square, axis=0, keepdims=True)) * (1.0 / number)
        inverse = lax.rsqrt(meansq - average * average + 1e-05)
        inv2_ref[inverse_at : inverse_at + 1] = inverse
        at = pl.multiple_of((k + 2 * slot) * block + GSIZE * c, GSIZE)
        gain = par_ref[pl.ds(at, GSIZE), 2:3]
        shift = par_ref[pl.ds(at, GSIZE), 3:4]
        for h in range(rows):
            normed = (field[h].astype(f32) - average) * inverse
            spot = (h % 2) * GSIZE
            nrm[h // 2, spot : spot + GSIZE] = normed
            act[h // 2, spot : spot + GSIZE] = activation(normed, gain, shift)

    for slot in range(2):
        field_stats(hid_b.at[slot], slot, nrm2.at[slot], act2.at[slot], slot)

    @pl.when(middle)
    def _():
        start_inner(0)
        lend_cot.wait_recv()
        share(x_far, 1).start()
        share(x_far, 1).wait_recv()
        shift_rows(x_far, xs_far)
        conv_far(2)
        take(0, w2, 3)
        unpack(w2, nth(3))
        conv_far(3)
        conv_own(nth(3))

    forward(1, w1, 2, 0)
    forward(1, w1, 1, 0)
    @pl.when(middle)
    def _():
        lend_hid.wait_recv()
        field_stats(hid_far, lent, nrm_far, act_far, 2)

    forward(1, w1, 2, 1)
    forward(1, w1, 1, 1)

    average1, meansq1 = wait_sums(0)
    inverse1 = lax.rsqrt(meansq1 - average1 * average1 + 1e-05)
    for g in range(groups):
        rows_g = pl.ds(g * GSIZE, GSIZE)
        normed = (nrm1[rows_g, :] - average1[g : g + 1]) * inverse1[g : g + 1]
        nrm1[rows_g, :] = normed
        act1[rows_g, :] = activation(normed, par_ref[rows_g, 0:1], par_ref[rows_g, 1:2])

    def norm_two(slot, recv, q, nrm, act, inverse, dst):
        for count, here in ((chips - 1, own), (chips, jnp.logical_not(own))):
            @pl.when(here)
            def _():
                span = q.at[0:count]
                wait_group(span, span, p_send.at[0], recv)

        sum_first = jnp.zeros((2 * GSIZE, lanes), f32)
        sum_second = jnp.zeros((2 * GSIZE, lanes), f32)
        scaled = []
        for m in range(rows // 2):
            total = q[0, m].astype(f32)
            for frm in range(1, chips):
                total = total + q[frm, m].astype(f32)
            value = total * act[m]
            scaled.append(value)
            sum_first += value
            sum_second += value * nrm[m]
        first = image_totals(jnp.sum(sum_first, axis=0, keepdims=True)) * (1.0 / number)
        second = image_totals(jnp.sum(sum_second, axis=0, keepdims=True)) * (1.0 / number)
        for m in range(rows // 2):
            dst[m] = (inverse * (scaled[m] - first - nrm[m] * second)).astype(bf16)

    def norm_own(slot):
        norm_two(
            slot, p_recv.at[slot], q1.at[slot], nrm2.at[slot], act2.at[slot],
            inv2_ref[pl.ds(slot, 1), :], hg_two.at[slot],
        )

    lend = remote(hg_far, hg_two.at[lent], e_send.at[0], e_recv.at[0], dp=partner)

    @pl.when(middle)
    def _():
        norm_two(lent, p_recv.at[2], q_far, nrm_far, act_far, inv2_ref[2:3, :], hg_far)
        lend.start()

    forward(1, w1, 2, 2)
    forward(1, w1, 1, 2)
    forward(1, w1, 2, 3)
    forward(1, w1, 1, 3)
    @pl.when(middle)
    def _():
        norm_own(0)
        norm_own(1)

    @pl.when(jnp.logical_not(middle))
    def _():
        norm_own(1 - lent)
        lend.wait_recv()

    for h in range(rows):
        spot = (h % 2) * GSIZE
        both = [hg_two[slot, h // 2].astype(f32)[spot : spot + GSIZE] for slot in range(2)]
        hg_s[h] = jnp.concatenate(both, axis=0).astype(bf16)
    swap = remote(hg_s, hg_r, b_send.at[1], b_recv.at[1], rows=sibling)
    swap.start()
    pending.append(swap)
    for h in range(rows):
        store_shifts(xs1, k, h, hg_s[h].astype(f32))
    forward(1, w1, 3, 0)
    swap.wait_recv()
    for h in range(rows):
        store_shifts(xs1, 1 - k, h, hg_r[h].astype(f32))

    forward(1, w1, 3, 1)
    conv_one(d)
    forward(1, w1, 3, 2)
    take_end(1, w1, 1)
    unpack(w1, nth(1))
    conv_one(nth(1))
    forward(1, w1, 3, 3)
    take_end(1, w1, 2)
    unpack(w1, nth(2))
    conv_one(nth(2))
    take_end(1, w1, 3)
    unpack(w1, nth(3))
    conv_one(nth(3), 1)
    def close_block(origin):
        for part in range(2):
            total = q2[origin, part].astype(f32)
            for frm in range(1, chips):
                total = total + q2[origin, 2 * frm + part].astype(f32)
            at = pl.ds(pl.multiple_of(origin * block + part * half, half), half)
            value = total * act1[at, :]
            act1[at, :] = value
            sums_ref[0, origin, part] = jnp.sum(value.reshape(2, GSIZE, lanes), axis=1)
            sums_ref[1, origin, part] = jnp.sum((value * nrm1[at, :]).reshape(2, GSIZE, lanes), axis=1)

    span = q2.at[0 : depth - 1, 0 : rows - 1]
    wait_group(span, span, o_send.at[0], o_recv.at[0])
    for origin in (d, nth(1), nth(2)):
        close_block(origin)
    span = q2.at[0, 0 : rows - 1]
    wait_group(span, span, o_send.at[0], o_recv.at[1])
    close_block(nth(3))
    one, two = [
        jnp.concatenate([sums_ref[which, origin, part] for origin in range(depth) for part in range(2)], axis=0)
        for which in range(2)
    ]
    send_sums(1, pack_sums(one, two))
    first1, second1 = wait_sums(1)
    value = spread(inverse1) * (act1[...] - spread(first1) - nrm1[...] * spread(second1))
    out_ref[...] = (cot_t[...].astype(f32) + value).astype(bf16).T

    for copy in pending:
        copy.wait_send()
    def sent(span, send, recv):
        remote(span, span, send, recv, rows=sibling).wait_send()

    sent(x_cot.at[0, 0 : chips - 1], c_send.at[0], c_recv.at[0])
    share(x_cot, 0).wait_send()
    sent(hid_two.at[0 : rows - 1], h_send.at[0], h_recv.at[0])
    sent(st_b.at[:, 0 : rows - 1], t_send.at[0], t_recv.at[0])
    sent(p2.at[:, 0 : rows - 1], o_send.at[0], o_recv.at[0])
    for count, here in ((chips - 1, own), (chips, jnp.logical_not(own))):
        @pl.when(here)
        def _():
            sent(r1.at[0:count], f_send.at[0], f_recv.at[0])

            @pl.when(middle)
            def _():
                sent(q1.at[:, 0:count], p_send.at[0], p_recv.at[0])
                sent(q_far.at[0:count], p_send.at[1], p_recv.at[2])

            @pl.when(jnp.logical_not(middle))
            def _():
                sent(q1.at[0, 0:count], p_send.at[0], p_recv.at[0])

    @pl.when(middle)
    def _():
        share(x_far, 1).wait_send()
        lend.wait_send()

    @pl.when(jnp.logical_not(middle))
    def _():
        lend_cot.wait_send()
        lend_hid.wait_send()

    last = depth - 1
    wait_hops(0, w2, [(0, 0, 0, 1), (1, 0, 0, 2), (1, 1, 1, 2), (2, 0, 2, 3), (2, 1, 2, 4), (3, 1, 3, 4)])
    wait_hops(
        1, w1,
        [(here, 0, 0, here + 1) for here in range(last)] + [(here, 1, here, depth) for here in range(1, depth)],
    )


def kernel_body(
    depth, rows,
    latent, hidden, cotangent, filter_one, filter_two, gain_one, shift_one, gain_two, shift_two,
):
    images, _, breadth, channels = latent.shape
    lanes = images * breadth
    block = channels // depth
    half = block // 2
    chips = rows // 2
    wide = -(-3 * half // 128) * 128
    narrow = -(-3 * GSIZE // 128) * 128
    groups = channels // GSIZE
    bf16, f32 = jnp.bfloat16, jnp.float32
    dma = pltpu.SemaphoreType.DMA
    out = pl.pallas_call(
        functools.partial(kernel, depth, rows, breadth),
        out_shape=jax.ShapeDtypeStruct((lanes, channels), bf16),
        in_specs=[pl.BlockSpec(memory_space=pltpu.HBM)] * 9,
        out_specs=pl.BlockSpec(memory_space=pltpu.VMEM),
        scratch_shapes=[
            pltpu.VMEM((lanes, channels), bf16),
            pltpu.VMEM((lanes, channels), bf16),
            pltpu.VMEM((lanes, channels), bf16),
            pltpu.VMEM(filter_one.shape, bf16),
            pltpu.VMEM(filter_two.shape, bf16),
            pltpu.VMEM((channels,), f32),
            pltpu.VMEM((channels,), f32),
            pltpu.VMEM((channels,), f32),
            pltpu.VMEM((channels,), f32),
            dma((9,)),
            pltpu.VMEM((channels, lanes), bf16),
            pltpu.VMEM((2, chips, block, lanes), bf16),
            pltpu.VMEM((2, rows, GSIZE, lanes), bf16),
            pltpu.VMEM((depth, 2, 3 * half, wide), bf16),
            pltpu.VMEM((depth, 2, 3 * half, wide), bf16),
            pltpu.VMEM((2, 2, 3, half, narrow), bf16),
            pltpu.VMEM((3 * half, wide), bf16),
            pltpu.VMEM((chips, 3, half, narrow), bf16),
            pltpu.VMEM((2, rows, wide, lanes), bf16),
            pltpu.VMEM((2, rows, wide, lanes), bf16),
            pltpu.VMEM((rows, 3 * half, lanes), f32),
            pltpu.VMEM((depth, 2, rows // 2, 2 * GSIZE, lanes), bf16),
            pltpu.VMEM((2, chips, rows // 2, 2 * GSIZE, lanes), bf16),
            pltpu.VMEM((depth, rows, half, lanes), bf16),
            pltpu.VMEM((depth, rows, half, lanes), bf16),
            pltpu.VMEM((rows, 2 * GSIZE, lanes), bf16),
            pltpu.VMEM((rows, 2 * GSIZE, lanes), bf16),
            pltpu.VMEM((channels, lanes), f32),
            pltpu.VMEM((channels, lanes), f32),
            pltpu.VMEM((2, rows // 2, 2 * GSIZE, lanes), f32),
            pltpu.VMEM((2, rows // 2, 2 * GSIZE, lanes), f32),
            pltpu.VMEM((4, lanes), f32),
            pltpu.VMEM((2, groups // 2, lanes), f32),
            pltpu.VMEM((2, rows, groups // 2, lanes), f32),
            pltpu.VMEM((channels, 8), f32),
            pltpu.VMEM((2, depth, 2, 2, lanes), f32),
            pltpu.VMEM((2, chips, block, lanes), bf16),
            pltpu.VMEM((rows, 2, GSIZE, lanes), bf16),
            pltpu.VMEM((rows, GSIZE, lanes), bf16),
            pltpu.VMEM((2, rows, wide, lanes), bf16),
            pltpu.VMEM((2, 2, rows // 2, 2 * GSIZE, lanes), bf16),
            pltpu.VMEM((chips, rows // 2, 2 * GSIZE, lanes), bf16),
            pltpu.VMEM((rows // 2, 2 * GSIZE, lanes), f32),
            pltpu.VMEM((rows // 2, 2 * GSIZE, lanes), f32),
            pltpu.VMEM((rows // 2, 2 * GSIZE, lanes), bf16),
            pltpu.VMEM((2, rows // 2, 2 * GSIZE, lanes), bf16),
            dma((2, 2, 2)), dma((2, depth - 1, 2, 2)),
            dma((1,)), dma((1,)),
            dma((2,)), dma((2,)),
            dma((2,)), dma((2,)),
            dma((2,)), dma((2,)),
            dma((2,)), dma((3,)),
            dma((1,)), dma((2,)),
            dma((1,)), dma((2,)),
            dma((2,)), dma((2,)),
            dma((1,)), dma((1,)),
        ],
        compiler_params=pltpu.CompilerParams(
            collective_id=0, has_side_effects=True, vmem_limit_bytes=48 * 1024 * 1024
        ),
    )(
        *[
            pltpu.with_memory_space_constraint(array, pltpu.HBM)
            for array in (
                latent.reshape(lanes, channels), hidden.reshape(lanes, channels),
                cotangent.reshape(lanes, channels), filter_one, filter_two,
                gain_one, shift_one, gain_two, shift_two,
            )
        ]
    )
    return out.reshape(latent.shape)


def solution(mesh):
    depth, rows = mesh.shape["dp"], mesh.shape["rows"]
    in_specs = (
        P("dp", "rows", None, None),
        P("dp", "rows", None, None),
        P("dp", "rows", None, None),
        P(None, "dp", "rows"),
        P(None, "dp", "rows"),
        P(),
        P(),
        P(),
        P(),
    )

    def body(latent, *rest):
        images, rows_here, breadth, channels = latent.shape
        fits = (
            rows_here == 1
            and images * breadth == 128
            and breadth % 4 == 0
            and depth == 4
            and rows == 2 * depth
            and channels == GROUPS * GSIZE
            and channels == depth * (rows // 2) * GSIZE
        )
        if fits:
            return kernel_body(depth, rows, latent, *rest)
        return plain_body(latent, *rest)

    return jax.shard_map(
        body, mesh=mesh, in_specs=in_specs, out_specs=P("dp", "rows", None, None), check_vma=False
    )
```

```python
import functools

import jax
import jax.numpy as jnp
from jax import lax
from jax.experimental import pallas as pl
from jax.experimental.pallas import tpu as pltpu
from jax.sharding import PartitionSpec as P

GROUPS = 16
GSIZE = 40
TAPS = 9
MESH = pl.DeviceIdType.MESH


def extended(block, sides, width):
    for axis, dim in sides:
        count = lax.axis_size(axis)
        forward = [(i, i + 1) for i in range(count - 1)]
        backward = [(target, source) for source, target in forward]
        low = lax.ppermute(
            lax.slice_in_dim(block, block.shape[dim] - width, None, axis=dim), axis, forward
        )
        high = lax.ppermute(lax.slice_in_dim(block, 0, width, axis=dim), axis, backward)
        block = jnp.concatenate([low, block, high], axis=dim)
    return block


def group_sums(values):
    per_channel = jnp.sum(values, axis=(1, 2))
    return jnp.sum(per_channel.reshape(per_channel.shape[0], GROUPS, -1), axis=2)


def expand_groups(moment):
    return jnp.repeat(moment, GSIZE, axis=1)[:, None, None, :]


def finish_stats(sum_plain, sum_square, number):
    average = sum_plain / number
    variance = sum_square / number - average * average
    return (average, lax.rsqrt(variance + 1e-05))


def reduced_stats(field, number):
    values = field.astype(jnp.float32)
    sum_plain, sum_square = lax.psum((group_sums(values), group_sums(values * values)), "rows")
    return finish_stats(sum_plain, sum_square, number)


def norm_backward(field, stats, gain, shift, incoming, number):
    average, inverse = stats
    values = field.astype(jnp.float32)
    normed = (values - expand_groups(average)) * expand_groups(inverse)
    linear = normed * gain + shift
    logistic = jax.nn.sigmoid(linear)
    scaled = incoming * logistic * (1.0 + linear * (1.0 - logistic)) * gain
    sum_first, sum_second = lax.psum((group_sums(scaled), group_sums(scaled * normed)), "rows")
    first = sum_first / number
    second = sum_second / number
    return expand_groups(inverse) * (scaled - expand_groups(first) - normed * expand_groups(second))


def conv_backward(gradient, weights):
    images, rows_here, breadth, channels = gradient.shape
    padded = extended(gradient, (("rows", 1),), 1)
    padded = jnp.pad(padded, ((0, 0), (0, 0), (1, 1), (0, 0)))
    pixels = images * rows_here * breadth
    shifted = []
    for tap_index in range(9):
        down_step = tap_index // 3 - 1
        side_step = tap_index % 3 - 1
        window = padded[
            :, 1 - down_step : 1 - down_step + rows_here, 1 - side_step : 1 - side_step + breadth, :
        ]
        shifted.append(window.reshape(pixels, channels))
    stacked = jnp.stack(shifted, axis=1)
    gathered = lax.all_gather(weights, "dp", axis=1, tiled=True)
    section = lax.all_gather(gathered, "rows", axis=2, tiled=True)
    columns = section.shape[2]
    window = stacked.reshape(pixels, 9 * columns)
    flat = jnp.transpose(section, (0, 2, 1)).reshape(9 * columns, section.shape[1])
    result = jnp.dot(window, flat, preferred_element_type=jnp.float32)
    return result.reshape(images, rows_here, breadth, channels)


def plain_body(
    latent, hidden, cotangent, filter_one, filter_two, gain_one, shift_one, gain_two, shift_two
):
    number = latent.shape[1] * lax.axis_size("rows") * latent.shape[2] * GSIZE
    stats_two = reduced_stats(hidden, number)
    back_two = conv_backward(cotangent, filter_two)
    hidden_grad = norm_backward(hidden, stats_two, gain_two, shift_two, back_two, number).astype(
        jnp.bfloat16
    )
    stats_one = reduced_stats(latent, number)
    back_one = conv_backward(hidden_grad, filter_one)
    latent_part = norm_backward(latent, stats_one, gain_one, shift_one, back_one, number)
    return (cotangent.astype(jnp.float32) + latent_part).astype(jnp.bfloat16)


def kernel(
    depth, rows, breadth,
    lat_hbm, hid_hbm, cot_hbm, raw1_hbm, raw2_hbm, gain1_hbm, shift1_hbm, gain2_hbm, shift2_hbm,
    out_ref,
    lat_ref, hid_ref, cot_ref, raw1, raw2, vectors, in_sem,
    cot_t, x_cot, hid_b, w1, w2, s1, s2, r1,
    xs1, xs2, y_ref, p1, q1, p2, q2, hg_s, hg_r,
    nrm1, act1, nrm2, act2, inv2_ref, st_s, st_b, par_ref,
    sums_ref, x_far, hid_two, hid_far, xs_far, p_far, q_far, nrm_far, act_far, hg_far, hg_two,
    z_send, z_recv, f_send, f_recv, b_send, b_recv, c_send, c_recv, h_send, h_recv,
    p_send, p_recv, o_send, o_recv, t_send, t_recv, d_recv, e_send, e_recv,
):
    d = lax.axis_index("dp")
    r = lax.axis_index("rows")
    chips = rows // 2
    c = r // 2
    k = lax.rem(r, 2)
    sibling = r + 1 - 2 * k
    channels, lanes = cot_t.shape
    block = channels // depth
    half = block // 2
    images = lanes // breadth
    wide = w1.shape[3]
    number = rows * breadth * GSIZE
    groups = channels // GSIZE
    bf16, f32 = jnp.bfloat16, jnp.float32

    def remote(src, dst, send, recv, **device):
        return pltpu.make_async_remote_copy(
            src_ref=src, dst_ref=dst, send_sem=send, recv_sem=recv,
            device_id=device, device_id_type=MESH,
        )

    pending = []
    loads = {
        name: pltpu.make_async_copy(src, dst, in_sem.at[index])
        for index, (name, src, dst) in enumerate((
            ("raw2", raw2_hbm, raw2), ("cot", cot_hbm, cot_ref), ("hid", hid_hbm, hid_ref),
            ("raw1", raw1_hbm, raw1), ("lat", lat_hbm, lat_ref),
        ))
    }
    for index, src in enumerate((gain1_hbm, shift1_hbm, gain2_hbm, shift2_hbm)):
        loads[index] = pltpu.make_async_copy(src, vectors.at[index, 0], in_sem.at[5])
    loads["raw2"].start()

    barrier = pltpu.get_barrier_semaphore()

    middle = (d > 0) & (d < depth - 1)
    partner = d + 1 - 2 * lax.rem(d, 2)
    lent = jnp.where(2 * d < depth, 1, 0)

    @pl.when(d > 0)
    def _():
        pl.semaphore_signal(barrier, inc=1, device_id={"dp": d - 1}, device_id_type=MESH)

    @pl.when(d < depth - 1)
    def _():
        pl.semaphore_signal(barrier, inc=1, device_id={"dp": d + 1}, device_id_type=MESH)

    for off in range(1, rows):
        pl.semaphore_signal(barrier, inc=1, device_id={"rows": lax.rem(r + off, rows)}, device_id_type=MESH)

    for name, load in loads.items():
        if name != "raw2":
            load.start()

    pad = wide - 3 * half
    own = k == c // 2
    tall = 3 * half
    w2[d, k, :, tall:] = jnp.zeros((tall, pad), bf16)
    s2[:, tall:] = jnp.zeros((tall, pad), bf16)
    for part in range(2):
        w1[d, part, :, tall:] = jnp.zeros((tall, pad), bf16)
        for side_core in range(2):
            s1[part, side_core, :, :, 3 * GSIZE :] = jnp.zeros((3, half, s1.shape[4] - 3 * GSIZE), bf16)
    for xs in (xs1, xs2, xs_far):
        for part in range(2):
            for h in range(rows):
                xs[part, h, 3 * half :] = jnp.zeros((pad, lanes), bf16)
    loads["raw2"].wait()

    def arrange(ready, raw, which):
        start = pl.multiple_of(which * half, 16)
        for tap in range(TAPS):
            down, side = tap // 3, tap % 3
            ready[down * half : (down + 1) * half, side * half : (side + 1) * half] = raw[
                tap, pl.ds(start, half), :
            ]

    def pack(ready):
        for at in range((tall - 128) // pad):
            ready[pad * at : pad * (at + 1), tall:] = ready[tall - pad :, 128 + pad * at : 128 + pad * (at + 1)]

    def unpack(w, origin, parts=(0, 1)):
        for part in parts:
            pieces = [w[origin, part, pad * at : pad * (at + 1), tall:] for at in range((tall - 128) // pad)]
            full = jnp.concatenate(pieces + [jnp.zeros((pad, pad), bf16)], axis=1)
            w[origin, part, tall - pad :, 128:] = full

    arrange(w2.at[d, k], raw2, k)

    pl.semaphore_wait(barrier, rows + jnp.where(middle, 1, 0))

    segments = ((tall, 0, 128), (tall - pad, 128, wide))

    def hop(which, w, origin, part, seg, way):
        deep, low, high = segments[seg]
        piece = w.at[origin, part, 0:deep, low:high]
        return remote(
            piece, piece, z_send.at[seg], z_recv.at[which, origin - way, part, seg], dp=d + 1 - 2 * way
        )

    near = jnp.minimum(d, depth - 1 - d)

    def nth(step):
        value = step - near if step == 1 else step
        return jnp.where(2 * d < depth, value, depth - 1 - value)

    def start_hops(which, w, part, ways=(0, 1), segs=(0, 1)):
        for way in ways:
            @pl.when((d < depth - 1) if way == 0 else (d > 0))
            def _():
                for seg in segs:
                    hop(which, w, d, part, seg, way).start()

    def start_one(ways):
        for part in (k, 1 - k):
            start_hops(1, w1, part, ways)

    def forward(which, w, step, index):
        origin = nth(step)
        part, seg = (k, 1 - k)[index // 2], index % 2
        for way in range(2):
            @pl.when(middle & ((origin < d) if way == 0 else (origin > d)))
            def _():
                copy = hop(which, w, origin, part, seg, way)
                copy.wait_recv()
                copy.start()

    def take(which, w, step, parts=(k, 1 - k)):
        for part in parts:
            for seg in range(2):
                origin = nth(step)
                hop(which, w, origin, part, seg, jnp.where(origin > d, 1, 0)).wait_recv()

    def take_end(which, w, step, parts=(k, 1 - k)):
        @pl.when(jnp.logical_not(middle))
        def _():
            take(which, w, step, parts)

    def wait_hops(count):
        for seg, (deep, _, _) in enumerate(segments):
            span = xs1.at[:, 0:count, 0:deep]
            remote(span, span, z_send.at[seg], z_recv.at[0, 0, 0, seg], rows=sibling).wait_send()

    start_hops(0, w2, k, segs=(0,))
    pack(w2.at[d, k])
    start_hops(0, w2, k, segs=(1,))
    arrange(s2, raw2, 1 - k)
    pack(s2)
    twin = remote(s2, w2.at[d, k], b_send.at[0], b_recv.at[0], rows=sibling)
    twin.start()
    pending.append(twin)

    loads["cot"].wait()
    cot_t[...] = cot_ref[...].T

    def piece_of(to):
        return cot_t.at[pl.ds(pl.multiple_of((to // 2) * block, block), block), :]

    for off in range(1, chips):
        to = 2 * lax.rem(c + off, chips) + k
        remote(piece_of(to), x_cot.at[k, c], c_send.at[0], c_recv.at[0], rows=to).start()
    x_cot[k, c] = piece_of(r)[...]

    loads["raw1"].wait()
    for part in range(2):
        for side_core in range(2):
            ready = s1.at[part, side_core]
            for tap in range(TAPS):
                down, side = tap // 3, tap % 3
                ready[down, :, side * GSIZE : (side + 1) * GSIZE] = raw1[
                    tap, side_core * half : (side_core + 1) * half, part * GSIZE : (part + 1) * GSIZE
                ]

    for part in range(2):
        for side_core in range(2):
            to = 2 * (2 * k + part) + side_core

            @pl.when(to != r)
            def _():
                remote(s1.at[part, side_core], r1.at[c], f_send.at[0], f_recv.at[0], rows=to).start()

            @pl.when(to == r)
            def _():
                r1[c] = s1[part, side_core]

    loads["hid"].wait()
    hid_full = hid_ref[...].astype(f32).T
    for to in range(rows):
        parts = [
            hid_full[block * b + GSIZE * (to // 2) : block * b + GSIZE * (to // 2 + 1)]
            for b in (to % 2, to % 2 + 2)
        ]
        for slot in range(2):
            hid_two[to, slot] = parts[slot].astype(bf16)
    for off in range(1, rows):
        to = lax.rem(r + off, rows)
        remote(hid_two.at[to], hid_b.at[:, r], h_send.at[0], h_recv.at[0], rows=to).start()
    hid_b[:, r] = hid_two[r]

    remote(s2, w2.at[d, 1 - k], b_send.at[0], b_recv.at[0], rows=sibling).wait_recv()
    start_hops(0, w2, 1 - k)

    forward(0, w2, 1, 0)
    loads["lat"].wait()
    lane = lax.broadcasted_iota(jnp.int32, (1, lanes), 1)
    column = lax.rem(lane, breadth)
    image_of = lax.div(lane, breadth)
    quarter = lax.rem(lane, breadth) // (breadth // 4)

    def image_totals(per_lane):
        total = jnp.zeros_like(per_lane)
        for image in range(images):
            mine = image_of == image
            part = jnp.sum(jnp.where(mine, per_lane, 0.0), axis=1, keepdims=True)
            total = jnp.where(mine, part, total)
        return total

    def pack_sums(one, two):
        one, two = image_totals(one), image_totals(two)
        top, low = slice(0, groups // 2), slice(groups // 2, groups)
        return jnp.where(
            quarter == 0, one[top], jnp.where(quarter == 1, two[top], jnp.where(quarter == 2, one[low], two[low]))
        )

    def send_sums(which, packed):
        st_s[which] = packed
        for off in range(1, rows):
            to = lax.rem(r + off, rows)
            remote(st_s.at[which], st_b.at[which, r], t_send.at[0], t_recv.at[which], rows=to).start()
        st_b[which, r] = packed

    def wait_sums(which):
        span = st_b.at[which, 0 : rows - 1]
        remote(span, span, t_send.at[0], t_recv.at[which], rows=sibling).wait_recv()
        total = st_b[which, 0]
        for h in range(1, rows):
            total = total + st_b[which, h]
        total = total * (1.0 / number)
        full = []
        for at in range(4):
            mine = jnp.where(quarter == at, total, 0.0)
            pair = mine + pltpu.roll(mine, ((1 if at % 2 == 0 else -1) * breadth // 4) % lanes, 1)
            full.append(pair + pltpu.roll(pair, ((1 if at < 2 else -1) * breadth // 2) % lanes, 1))
        return jnp.concatenate([full[0], full[2]], axis=0), jnp.concatenate([full[1], full[3]], axis=0)

    def spread(moment):
        return jnp.broadcast_to(moment[:, None, :], (groups, GSIZE, lanes)).reshape(channels, lanes)

    def by_group(values):
        return jnp.sum(values.reshape(groups, GSIZE, lanes), axis=1)

    nrm1[...] = lat_ref[...].astype(f32).T
    send_sums(0, pack_sums(by_group(nrm1[...]), by_group(nrm1[...] * nrm1[...])))

    pltpu.make_async_copy(vectors, vectors, in_sem.at[5]).wait()
    raw_params = [vectors[index] for index in range(4)]
    par_ref[...] = jnp.concatenate(raw_params + raw_params, axis=0).T

    def store_shifts(xs, part, h, values):
        left = jnp.where(column == breadth - 1, 0.0, pltpu.roll(values, lanes - 1, 1))
        right = jnp.where(column == 0, 0.0, pltpu.roll(values, 1, 1))
        xs[part, h, 0:half] = left.astype(bf16)
        xs[part, h, half : 2 * half] = values.astype(bf16)
        xs[part, h, 2 * half : 3 * half] = right.astype(bf16)

    def wait_group(src, dst, send, recv):
        remote(src, dst, send, recv, rows=sibling).wait_recv()

    forward(0, w2, 1, 1)
    everyone = x_cot.at[0, 0 : chips - 1]
    wait_group(everyone, everyone, c_send.at[0], c_recv.at[0])

    def share(x, at):
        return remote(x.at[k], x.at[k], c_send.at[1], d_recv.at[at], rows=sibling)

    def shift_rows(x, xs):
        for h in range(rows):
            values = x[h % 2, h // 2].astype(f32)
            for part in range(2):
                store_shifts(xs, part, h, values[part * half : (part + 1) * half])

    share(x_cot, 0).start()
    lend_cot = remote(x_cot.at[k], x_far.at[k], c_send.at[1], c_recv.at[1], dp=partner)
    lend_hid = remote(hid_b.at[lent], hid_far, h_send.at[1], h_recv.at[1], dp=partner)

    @pl.when(jnp.logical_not(middle))
    def _():
        lend_cot.start()

    forward(0, w2, 1, 2)
    share(x_cot, 0).wait_recv()
    shift_rows(x_cot, xs2)

    def conv(w, origin, xs):
        for h in range(0, rows, 2):
            total = None
            for part in range(2):
                pair = jnp.concatenate([xs[part, h], xs[part, h + 1]], axis=1)
                term = jnp.dot(w[origin, part], pair, preferred_element_type=f32)
                total = term if total is None else total + term
            y_ref[h] = total[:, :lanes]
            y_ref[h + 1] = total[:, lanes:]

    def row_of(h):
        total = y_ref[h, half : 2 * half]
        if h + 1 < rows:
            total = total + y_ref[h + 1, 0:half]
        if h > 0:
            total = total + y_ref[h - 1, 2 * half : 3 * half]
        return total

    def conv_two(origin, xs, p, q, send, recv):
        conv(w2, origin, xs)
        for h in range(0, rows, 2):
            low, high = row_of(h), row_of(h + 1)
            for j in range(2):
                both = [low[j * GSIZE : (j + 1) * GSIZE], high[j * GSIZE : (j + 1) * GSIZE]]
                p[j, h // 2] = jnp.concatenate(both, axis=0).astype(bf16)
        for j in range(2):
            to = 2 * (2 * k + j) + lax.rem(origin, 2)

            @pl.when(to != r)
            def _():
                remote(p.at[j], q.at[c], send, recv, rows=to).start()

            @pl.when(to == r)
            def _():
                q[c] = p[j]

    def conv_own(origin):
        slot = origin // 2
        conv_two(origin, xs2, p1.at[origin], q1.at[slot], p_send.at[0], p_recv.at[slot])

    def conv_far(step):
        conv_two(nth(step), xs_far, p_far.at[step - 2], q_far, p_send.at[1], p_recv.at[2])

    def conv_half(origin, part, more):
        for h in range(0, rows, 2):
            pair = jnp.concatenate([xs1[part, h], xs1[part, h + 1]], axis=1)
            term = jnp.dot(w1[origin, part], pair, preferred_element_type=f32)
            for side in range(2):
                value = term[:, side * lanes : (side + 1) * lanes]
                y_ref[h + side] = y_ref[h + side] + value if more else value

    def conv_one(origin, last=0):
        conv(w1, origin, xs1)
        send_rows(origin, last)

    def send_rows(origin, last=0):
        for h in range(rows):
            p2[origin, h] = row_of(h).astype(bf16)
        for off in range(1, rows):
            to = lax.rem(r + off, rows)
            remote(p2.at[origin, to], q2.at[origin, r], o_send.at[0], o_recv.at[last], rows=to).start()
        q2[origin, r] = p2[origin, r]

    conv_own(d)
    forward(0, w2, 1, 3)
    for count, here in ((chips - 1, own), (chips, jnp.logical_not(own))):
        @pl.when(here)
        def _():
            span = r1.at[0:count]
            wait_group(span, span, f_send.at[0], f_recv.at[0])

    for part in range(2):
        for j in range(2):
            for side in range(3):
                at = side * half + j * GSIZE
                piece = r1[2 * j + part, :, :, side * GSIZE : (side + 1) * GSIZE]
                w1[d, part, :, at : at + GSIZE] = piece.reshape(tall, GSIZE)
        pack(w1.at[d, part])

    def start_inner(toward):
        for here, way in ((1, toward), (2, 1 - toward)):
            @pl.when(d == here)
            def _():
                start_one((way,))

    start_inner(1)

    take_end(0, w2, 1)
    unpack(w2, nth(1))
    conv_own(nth(1))
    @pl.when(middle)
    def _():
        take(0, w2, 2)
        unpack(w2, nth(2))
        conv_own(nth(2))

    def activation(normed, gain, shift):
        linear = normed * gain + shift
        logistic = 1.0 / (1.0 + jnp.exp(-linear))
        return logistic * (1.0 + linear * (1.0 - logistic)) * gain

    everyone = hid_two.at[0 : rows - 1]
    wait_group(everyone, everyone, h_send.at[0], h_recv.at[0])

    @pl.when(jnp.logical_not(middle))
    def _():
        lend_hid.start()
        start_one((0, 1))

    def field_stats(field, slot, nrm, act, inverse_at):
        plain = jnp.zeros((GSIZE, lanes), f32)
        square = jnp.zeros((GSIZE, lanes), f32)
        for h in range(rows):
            values = field[h].astype(f32)
            plain += values
            square += values * values
        average = image_totals(jnp.sum(plain, axis=0, keepdims=True)) * (1.0 / number)
        meansq = image_totals(jnp.sum(square, axis=0, keepdims=True)) * (1.0 / number)
        inverse = lax.rsqrt(meansq - average * average + 1e-05)
        inv2_ref[inverse_at : inverse_at + 1] = inverse
        at = pl.multiple_of((k + 2 * slot) * block + GSIZE * c, GSIZE)
        gain = par_ref[pl.ds(at, GSIZE), 2:3]
        shift = par_ref[pl.ds(at, GSIZE), 3:4]
        for h in range(rows):
            normed = (field[h].astype(f32) - average) * inverse
            spot = (h % 2) * GSIZE
            nrm[h // 2, spot : spot + GSIZE] = normed
            act[h // 2, spot : spot + GSIZE] = activation(normed, gain, shift)

    for slot in range(2):
        field_stats(hid_b.at[slot], slot, nrm2.at[slot], act2.at[slot], slot)

    @pl.when(middle)
    def _():
        start_inner(0)
        lend_cot.wait_recv()
        share(x_far, 1).start()
        share(x_far, 1).wait_recv()
        shift_rows(x_far, xs_far)
        conv_far(2)
        take(0, w2, 3)
        unpack(w2, nth(3))
        conv_far(3)
        conv_own(nth(3))

    forward(1, w1, 2, 0)
    forward(1, w1, 1, 0)
    @pl.when(middle)
    def _():
        lend_hid.wait_recv()
        field_stats(hid_far, lent, nrm_far, act_far, 2)

    forward(1, w1, 2, 1)
    forward(1, w1, 1, 1)

    average1, meansq1 = wait_sums(0)
    inverse1 = lax.rsqrt(meansq1 - average1 * average1 + 1e-05)
    for g in range(groups):
        rows_g = pl.ds(g * GSIZE, GSIZE)
        normed = (nrm1[rows_g, :] - average1[g : g + 1]) * inverse1[g : g + 1]
        nrm1[rows_g, :] = normed
        act1[rows_g, :] = activation(normed, par_ref[rows_g, 0:1], par_ref[rows_g, 1:2])

    def norm_two(slot, recv, q, nrm, act, inverse, dst):
        for count, here in ((chips - 1, own), (chips, jnp.logical_not(own))):
            @pl.when(here)
            def _():
                span = q.at[0:count]
                wait_group(span, span, p_send.at[0], recv)

        sum_first = jnp.zeros((2 * GSIZE, lanes), f32)
        sum_second = jnp.zeros((2 * GSIZE, lanes), f32)
        scaled = []
        for m in range(rows // 2):
            total = q[0, m].astype(f32)
            for frm in range(1, chips):
                total = total + q[frm, m].astype(f32)
            value = total * act[m]
            scaled.append(value)
            sum_first += value
            sum_second += value * nrm[m]
        first = image_totals(jnp.sum(sum_first, axis=0, keepdims=True)) * (1.0 / number)
        second = image_totals(jnp.sum(sum_second, axis=0, keepdims=True)) * (1.0 / number)
        for m in range(rows // 2):
            dst[m] = (inverse * (scaled[m] - first - nrm[m] * second)).astype(bf16)

    def norm_own(slot):
        norm_two(
            slot, p_recv.at[slot], q1.at[slot], nrm2.at[slot], act2.at[slot],
            inv2_ref[pl.ds(slot, 1), :], hg_two.at[slot],
        )

    lend = remote(hg_far, hg_two.at[lent], e_send.at[0], e_recv.at[0], dp=partner)

    @pl.when(middle)
    def _():
        norm_two(lent, p_recv.at[2], q_far, nrm_far, act_far, inv2_ref[2:3, :], hg_far)
        lend.start()

    forward(1, w1, 2, 2)
    forward(1, w1, 1, 2)
    forward(1, w1, 2, 3)
    forward(1, w1, 1, 3)
    @pl.when(middle)
    def _():
        norm_own(0)
        norm_own(1)

    @pl.when(jnp.logical_not(middle))
    def _():
        norm_own(1 - lent)
        lend.wait_recv()

    for h in range(rows):
        spot = (h % 2) * GSIZE
        both = [hg_two[slot, h // 2].astype(f32)[spot : spot + GSIZE] for slot in range(2)]
        hg_s[h] = jnp.concatenate(both, axis=0).astype(bf16)
    swap = remote(hg_s, hg_r, b_send.at[1], b_recv.at[1], rows=sibling)
    swap.start()
    pending.append(swap)
    for h in range(rows):
        store_shifts(xs1, k, h, hg_s[h].astype(f32))
    forward(1, w1, 3, 0)
    conv_half(d, k, False)
    swap.wait_recv()
    for h in range(rows):
        store_shifts(xs1, 1 - k, h, hg_r[h].astype(f32))

    forward(1, w1, 3, 1)
    conv_half(d, 1 - k, True)
    send_rows(d)
    forward(1, w1, 3, 2)
    take_end(1, w1, 1)
    unpack(w1, nth(1))
    conv_one(nth(1))
    forward(1, w1, 3, 3)
    take_end(1, w1, 2)
    unpack(w1, nth(2))
    conv_one(nth(2))
    take_end(1, w1, 3, (k,))
    unpack(w1, nth(3), (k,))
    conv_half(nth(3), k, False)
    take_end(1, w1, 3, (1 - k,))
    unpack(w1, nth(3), (1 - k,))
    conv_half(nth(3), 1 - k, True)
    send_rows(nth(3), 1)
    def close_block(origin):
        for part in range(2):
            total = q2[origin, part].astype(f32)
            for frm in range(1, chips):
                total = total + q2[origin, 2 * frm + part].astype(f32)
            at = pl.ds(pl.multiple_of(origin * block + part * half, half), half)
            value = total * act1[at, :]
            act1[at, :] = value
            sums_ref[0, origin, part] = jnp.sum(value.reshape(2, GSIZE, lanes), axis=1)
            sums_ref[1, origin, part] = jnp.sum((value * nrm1[at, :]).reshape(2, GSIZE, lanes), axis=1)

    span = q2.at[0 : depth - 1, 0 : rows - 1]
    wait_group(span, span, o_send.at[0], o_recv.at[0])
    for origin in (d, nth(1), nth(2)):
        close_block(origin)
    span = q2.at[0, 0 : rows - 1]
    wait_group(span, span, o_send.at[0], o_recv.at[1])
    close_block(nth(3))
    one, two = [
        jnp.concatenate([sums_ref[which, origin, part] for origin in range(depth) for part in range(2)], axis=0)
        for which in range(2)
    ]
    send_sums(1, pack_sums(one, two))
    first1, second1 = wait_sums(1)
    value = spread(inverse1) * (act1[...] - spread(first1) - nrm1[...] * spread(second1))
    out_ref[...] = (cot_t[...].astype(f32) + value).astype(bf16).T

    for copy in pending:
        copy.wait_send()
    def sent(span, send, recv):
        remote(span, span, send, recv, rows=sibling).wait_send()

    sent(x_cot.at[0, 0 : chips - 1], c_send.at[0], c_recv.at[0])
    sent(x_far, c_send.at[1], d_recv.at[0])
    sent(hid_two.at[0 : rows - 1], h_send.at[0], h_recv.at[0])
    sent(st_b.at[:, 0 : rows - 1], t_send.at[0], t_recv.at[0])
    sent(p2.at[:, 0 : rows - 1], o_send.at[0], o_recv.at[0])
    for count, here in ((chips - 1, own), (chips, jnp.logical_not(own))):
        @pl.when(here)
        def _():
            sent(r1.at[0:count], f_send.at[0], f_recv.at[0])

            @pl.when(middle)
            def _():
                sent(q1.at[:, 0:count], p_send.at[0], p_recv.at[0])
                sent(q_far.at[0:count], p_send.at[1], p_recv.at[2])

            @pl.when(jnp.logical_not(middle))
            def _():
                sent(q1.at[0, 0:count], p_send.at[0], p_recv.at[0])

    @pl.when(middle)
    def _():
        lend.wait_send()

    @pl.when(jnp.logical_not(middle))
    def _():
        lend_hid.wait_send()

    @pl.when(middle)
    def _():
        wait_hops(2 * depth)

    @pl.when(jnp.logical_not(middle))
    def _():
        wait_hops(2)


def kernel_body(
    depth, rows,
    latent, hidden, cotangent, filter_one, filter_two, gain_one, shift_one, gain_two, shift_two,
):
    images, _, breadth, channels = latent.shape
    lanes = images * breadth
    block = channels // depth
    half = block // 2
    chips = rows // 2
    wide = -(-3 * half // 128) * 128
    narrow = -(-3 * GSIZE // 128) * 128
    groups = channels // GSIZE
    bf16, f32 = jnp.bfloat16, jnp.float32
    dma = pltpu.SemaphoreType.DMA
    out = pl.pallas_call(
        functools.partial(kernel, depth, rows, breadth),
        out_shape=jax.ShapeDtypeStruct((lanes, channels), bf16),
        in_specs=[pl.BlockSpec(memory_space=pltpu.HBM)] * 9,
        out_specs=pl.BlockSpec(memory_space=pltpu.VMEM),
        scratch_shapes=[
            pltpu.VMEM((lanes, channels), bf16),
            pltpu.VMEM((lanes, channels), bf16),
            pltpu.VMEM((lanes, channels), bf16),
            pltpu.VMEM(filter_one.shape, bf16),
            pltpu.VMEM(filter_two.shape, bf16),
            pltpu.VMEM((4, 1, channels), f32),
            dma((6,)),
            pltpu.VMEM((channels, lanes), bf16),
            pltpu.VMEM((2, chips, block, lanes), bf16),
            pltpu.VMEM((2, rows, GSIZE, lanes), bf16),
            pltpu.VMEM((depth, 2, 3 * half, wide), bf16),
            pltpu.VMEM((depth, 2, 3 * half, wide), bf16),
            pltpu.VMEM((2, 2, 3, half, narrow), bf16),
            pltpu.VMEM((3 * half, wide), bf16),
            pltpu.VMEM((chips, 3, half, narrow), bf16),
            pltpu.VMEM((2, rows, wide, lanes), bf16),
            pltpu.VMEM((2, rows, wide, lanes), bf16),
            pltpu.VMEM((rows, 3 * half, lanes), f32),
            pltpu.VMEM((depth, 2, rows // 2, 2 * GSIZE, lanes), bf16),
            pltpu.VMEM((2, chips, rows // 2, 2 * GSIZE, lanes), bf16),
            pltpu.VMEM((depth, rows, half, lanes), bf16),
            pltpu.VMEM((depth, rows, half, lanes), bf16),
            pltpu.VMEM((rows, 2 * GSIZE, lanes), bf16),
            pltpu.VMEM((rows, 2 * GSIZE, lanes), bf16),
            pltpu.VMEM((channels, lanes), f32),
            pltpu.VMEM((channels, lanes), f32),
            pltpu.VMEM((2, rows // 2, 2 * GSIZE, lanes), f32),
            pltpu.VMEM((2, rows // 2, 2 * GSIZE, lanes), f32),
            pltpu.VMEM((4, lanes), f32),
            pltpu.VMEM((2, groups // 2, lanes), f32),
            pltpu.VMEM((2, rows, groups // 2, lanes), f32),
            pltpu.VMEM((channels, 8), f32),
            pltpu.VMEM((2, depth, 2, 2, lanes), f32),
            pltpu.VMEM((2, chips, block, lanes), bf16),
            pltpu.VMEM((rows, 2, GSIZE, lanes), bf16),
            pltpu.VMEM((rows, GSIZE, lanes), bf16),
            pltpu.VMEM((2, rows, wide, lanes), bf16),
            pltpu.VMEM((2, 2, rows // 2, 2 * GSIZE, lanes), bf16),
            pltpu.VMEM((chips, rows // 2, 2 * GSIZE, lanes), bf16),
            pltpu.VMEM((rows // 2, 2 * GSIZE, lanes), f32),
            pltpu.VMEM((rows // 2, 2 * GSIZE, lanes), f32),
            pltpu.VMEM((rows // 2, 2 * GSIZE, lanes), bf16),
            pltpu.VMEM((2, rows // 2, 2 * GSIZE, lanes), bf16),
            dma((2,)), dma((2, depth - 1, 2, 2)),
            dma((1,)), dma((1,)),
            dma((2,)), dma((2,)),
            dma((2,)), dma((2,)),
            dma((2,)), dma((2,)),
            dma((2,)), dma((3,)),
            dma((1,)), dma((2,)),
            dma((1,)), dma((2,)),
            dma((2,)),
            dma((1,)), dma((1,)),
        ],
        compiler_params=pltpu.CompilerParams(
            collective_id=0, has_side_effects=True, vmem_limit_bytes=48 * 1024 * 1024
        ),
    )(
        *[
            pltpu.with_memory_space_constraint(array, pltpu.HBM)
            for array in (
                latent.reshape(lanes, channels), hidden.reshape(lanes, channels),
                cotangent.reshape(lanes, channels), filter_one, filter_two,
                gain_one, shift_one, gain_two, shift_two,
            )
        ]
    )
    return out.reshape(latent.shape)


def solution(mesh):
    depth, rows = mesh.shape["dp"], mesh.shape["rows"]
    in_specs = (
        P("dp", "rows", None, None),
        P("dp", "rows", None, None),
        P("dp", "rows", None, None),
        P(None, "dp", "rows"),
        P(None, "dp", "rows"),
        P(),
        P(),
        P(),
        P(),
    )

    def body(latent, *rest):
        images, rows_here, breadth, channels = latent.shape
        fits = (
            rows_here == 1
            and images * breadth == 128
            and breadth % 4 == 0
            and depth == 4
            and rows == 2 * depth
            and channels == GROUPS * GSIZE
            and channels == depth * (rows // 2) * GSIZE
        )
        if fits:
            return kernel_body(depth, rows, latent, *rest)
        return plain_body(latent, *rest)

    return jax.shard_map(
        body, mesh=mesh, in_specs=in_specs, out_specs=P("dp", "rows", None, None), check_vma=False
    )
```

```python
import functools

import jax
import jax.numpy as jnp
from jax import lax
from jax.experimental import pallas as pl
from jax.experimental.pallas import tpu as pltpu
from jax.sharding import PartitionSpec as P

GROUPS = 16
GSIZE = 40
TAPS = 9
MESH = pl.DeviceIdType.MESH


def extended(block, sides, width):
    for axis, dim in sides:
        count = lax.axis_size(axis)
        forward = [(i, i + 1) for i in range(count - 1)]
        backward = [(target, source) for source, target in forward]
        low = lax.ppermute(
            lax.slice_in_dim(block, block.shape[dim] - width, None, axis=dim), axis, forward
        )
        high = lax.ppermute(lax.slice_in_dim(block, 0, width, axis=dim), axis, backward)
        block = jnp.concatenate([low, block, high], axis=dim)
    return block


def group_sums(values):
    per_channel = jnp.sum(values, axis=(1, 2))
    return jnp.sum(per_channel.reshape(per_channel.shape[0], GROUPS, -1), axis=2)


def expand_groups(moment):
    return jnp.repeat(moment, GSIZE, axis=1)[:, None, None, :]


def finish_stats(sum_plain, sum_square, number):
    average = sum_plain / number
    variance = sum_square / number - average * average
    return (average, lax.rsqrt(variance + 1e-05))


def reduced_stats(field, number):
    values = field.astype(jnp.float32)
    sum_plain, sum_square = lax.psum((group_sums(values), group_sums(values * values)), "rows")
    return finish_stats(sum_plain, sum_square, number)


def norm_backward(field, stats, gain, shift, incoming, number):
    average, inverse = stats
    values = field.astype(jnp.float32)
    normed = (values - expand_groups(average)) * expand_groups(inverse)
    linear = normed * gain + shift
    logistic = jax.nn.sigmoid(linear)
    scaled = incoming * logistic * (1.0 + linear * (1.0 - logistic)) * gain
    sum_first, sum_second = lax.psum((group_sums(scaled), group_sums(scaled * normed)), "rows")
    first = sum_first / number
    second = sum_second / number
    return expand_groups(inverse) * (scaled - expand_groups(first) - normed * expand_groups(second))


def conv_backward(gradient, weights):
    images, rows_here, breadth, channels = gradient.shape
    padded = extended(gradient, (("rows", 1),), 1)
    padded = jnp.pad(padded, ((0, 0), (0, 0), (1, 1), (0, 0)))
    pixels = images * rows_here * breadth
    shifted = []
    for tap_index in range(9):
        down_step = tap_index // 3 - 1
        side_step = tap_index % 3 - 1
        window = padded[
            :, 1 - down_step : 1 - down_step + rows_here, 1 - side_step : 1 - side_step + breadth, :
        ]
        shifted.append(window.reshape(pixels, channels))
    stacked = jnp.stack(shifted, axis=1)
    gathered = lax.all_gather(weights, "dp", axis=1, tiled=True)
    section = lax.all_gather(gathered, "rows", axis=2, tiled=True)
    columns = section.shape[2]
    window = stacked.reshape(pixels, 9 * columns)
    flat = jnp.transpose(section, (0, 2, 1)).reshape(9 * columns, section.shape[1])
    result = jnp.dot(window, flat, preferred_element_type=jnp.float32)
    return result.reshape(images, rows_here, breadth, channels)


def plain_body(
    latent, hidden, cotangent, filter_one, filter_two, gain_one, shift_one, gain_two, shift_two
):
    number = latent.shape[1] * lax.axis_size("rows") * latent.shape[2] * GSIZE
    stats_two = reduced_stats(hidden, number)
    back_two = conv_backward(cotangent, filter_two)
    hidden_grad = norm_backward(hidden, stats_two, gain_two, shift_two, back_two, number).astype(
        jnp.bfloat16
    )
    stats_one = reduced_stats(latent, number)
    back_one = conv_backward(hidden_grad, filter_one)
    latent_part = norm_backward(latent, stats_one, gain_one, shift_one, back_one, number)
    return (cotangent.astype(jnp.float32) + latent_part).astype(jnp.bfloat16)


def kernel(
    depth, rows, breadth,
    lat_hbm, hid_hbm, cot_hbm, raw1_hbm, raw2_hbm, gain1_hbm, shift1_hbm, gain2_hbm, shift2_hbm,
    out_ref,
    lat_ref, hid_ref, cot_ref, raw1, raw2, vectors, in_sem,
    cot_t, x_cot, hid_b, w1, w2, s1, s2, r1,
    xs1, xs2, y_ref, p1, q1, p2, q2, hg_s, hg_r,
    nrm1, act1, nrm2, act2, inv2_ref, st_s, st_b, par_ref,
    sums_ref, x_far, hid_two, hid_far, xs_far, p_far, q_far, nrm_far, act_far, hg_far, hg_two,
    z_send, z_recv, f_send, f_recv, b_send, b_recv, c_send, c_recv, h_send, h_recv,
    p_send, p_recv, o_send, o_recv, t_send, t_recv, d_recv, e_send, e_recv,
):
    d = lax.axis_index("dp")
    r = lax.axis_index("rows")
    chips = rows // 2
    c = r // 2
    k = lax.rem(r, 2)
    sibling = r + 1 - 2 * k
    channels, lanes = cot_t.shape
    block = channels // depth
    half = block // 2
    images = lanes // breadth
    wide = w1.shape[3]
    number = rows * breadth * GSIZE
    groups = channels // GSIZE
    bf16, f32 = jnp.bfloat16, jnp.float32

    def remote(src, dst, send, recv, **device):
        return pltpu.make_async_remote_copy(
            src_ref=src, dst_ref=dst, send_sem=send, recv_sem=recv,
            device_id=device, device_id_type=MESH,
        )

    pending = []
    loads = {
        name: pltpu.make_async_copy(src, dst, in_sem.at[index])
        for index, (name, src, dst) in enumerate((
            ("raw2", raw2_hbm, raw2), ("cot", cot_hbm, cot_ref), ("hid", hid_hbm, hid_ref),
            ("raw1", raw1_hbm, raw1), ("lat", lat_hbm, lat_ref),
        ))
    }
    for index, src in enumerate((gain1_hbm, shift1_hbm, gain2_hbm, shift2_hbm)):
        loads[index] = pltpu.make_async_copy(src, vectors.at[index, 0], in_sem.at[5])
    loads["raw2"].start()

    barrier = pltpu.get_barrier_semaphore()

    middle = (d > 0) & (d < depth - 1)
    partner = d + 1 - 2 * lax.rem(d, 2)
    lent = jnp.where(2 * d < depth, 1, 0)

    @pl.when(d > 0)
    def _():
        pl.semaphore_signal(barrier, inc=1, device_id={"dp": d - 1}, device_id_type=MESH)

    @pl.when(d < depth - 1)
    def _():
        pl.semaphore_signal(barrier, inc=1, device_id={"dp": d + 1}, device_id_type=MESH)

    for off in range(1, rows):
        pl.semaphore_signal(barrier, inc=1, device_id={"rows": lax.rem(r + off, rows)}, device_id_type=MESH)

    for name, load in loads.items():
        if name != "raw2":
            load.start()

    pad = wide - 3 * half
    own = k == c // 2
    tall = 3 * half
    w2[d, k, :, tall:] = jnp.zeros((tall, pad), bf16)
    s2[:, tall:] = jnp.zeros((tall, pad), bf16)
    for part in range(2):
        w1[d, part, :, tall:] = jnp.zeros((tall, pad), bf16)
        for side_core in range(2):
            s1[part, side_core, :, :, 3 * GSIZE :] = jnp.zeros((3, half, s1.shape[4] - 3 * GSIZE), bf16)
    for xs in (xs1, xs2, xs_far):
        for part in range(2):
            for h in range(rows):
                xs[part, h, 3 * half :] = jnp.zeros((pad, lanes), bf16)
    loads["raw2"].wait()

    def arrange(ready, raw, which):
        start = pl.multiple_of(which * half, 16)
        for tap in range(TAPS):
            down, side = tap // 3, tap % 3
            ready[down * half : (down + 1) * half, side * half : (side + 1) * half] = raw[
                tap, pl.ds(start, half), :
            ]

    def pack(ready):
        for at in range((tall - 128) // pad):
            ready[pad * at : pad * (at + 1), tall:] = ready[tall - pad :, 128 + pad * at : 128 + pad * (at + 1)]

    def unpack(w, origin, parts=(0, 1)):
        for part in parts:
            pieces = [w[origin, part, pad * at : pad * (at + 1), tall:] for at in range((tall - 128) // pad)]
            full = jnp.concatenate(pieces + [jnp.zeros((pad, pad), bf16)], axis=1)
            w[origin, part, tall - pad :, 128:] = full

    arrange(w2.at[d, k], raw2, k)

    pl.semaphore_wait(barrier, rows + jnp.where(middle, 1, 0))

    segments = ((tall, 0, 128), (tall - pad, 128, wide))

    def hop(which, w, origin, part, seg, way):
        deep, low, high = segments[seg]
        piece = w.at[origin, part, 0:deep, low:high]
        return remote(
            piece, piece, z_send.at[seg], z_recv.at[which, origin - way, part, seg], dp=d + 1 - 2 * way
        )

    near = jnp.minimum(d, depth - 1 - d)

    def nth(step):
        value = step - near if step == 1 else step
        return jnp.where(2 * d < depth, value, depth - 1 - value)

    def start_hops(which, w, part, ways=(0, 1), segs=(0, 1)):
        for way in ways:
            @pl.when((d < depth - 1) if way == 0 else (d > 0))
            def _():
                for seg in segs:
                    hop(which, w, d, part, seg, way).start()

    def start_one(ways):
        for part in (k, 1 - k):
            start_hops(1, w1, part, ways)

    def forward(which, w, step, index):
        origin = nth(step)
        part, seg = (k, 1 - k)[index // 2], index % 2
        for way in range(2):
            @pl.when(middle & ((origin < d) if way == 0 else (origin > d)))
            def _():
                copy = hop(which, w, origin, part, seg, way)
                copy.wait_recv()
                copy.start()

    def take(which, w, step, parts=(k, 1 - k)):
        for part in parts:
            for seg in range(2):
                origin = nth(step)
                hop(which, w, origin, part, seg, jnp.where(origin > d, 1, 0)).wait_recv()

    def take_end(which, w, step, parts=(k, 1 - k)):
        @pl.when(jnp.logical_not(middle))
        def _():
            take(which, w, step, parts)

    def wait_hops(count):
        for seg, (deep, _, _) in enumerate(segments):
            span = xs1.at[:, 0:count, 0:deep]
            remote(span, span, z_send.at[seg], z_recv.at[0, 0, 0, seg], rows=sibling).wait_send()

    start_hops(0, w2, k, segs=(0,))
    pack(w2.at[d, k])
    start_hops(0, w2, k, segs=(1,))
    arrange(s2, raw2, 1 - k)
    pack(s2)
    twin = remote(s2, w2.at[d, k], b_send.at[0], b_recv.at[0], rows=sibling)
    twin.start()
    pending.append(twin)

    loads["cot"].wait()
    cot_t[...] = cot_ref[...].T

    def piece_of(to):
        return cot_t.at[pl.ds(pl.multiple_of((to // 2) * block, block), block), :]

    for off in range(1, chips):
        to = 2 * lax.rem(c + off, chips) + k
        remote(piece_of(to), x_cot.at[k, c], c_send.at[0], c_recv.at[0], rows=to).start()
    x_cot[k, c] = piece_of(r)[...]

    loads["raw1"].wait()
    for part in range(2):
        for side_core in range(2):
            ready = s1.at[part, side_core]
            for tap in range(TAPS):
                down, side = tap // 3, tap % 3
                ready[down, :, side * GSIZE : (side + 1) * GSIZE] = raw1[
                    tap, side_core * half : (side_core + 1) * half, part * GSIZE : (part + 1) * GSIZE
                ]

    for part in range(2):
        for side_core in range(2):
            to = 2 * (2 * k + part) + side_core

            @pl.when(to != r)
            def _():
                remote(s1.at[part, side_core], r1.at[c], f_send.at[0], f_recv.at[0], rows=to).start()

            @pl.when(to == r)
            def _():
                r1[c] = s1[part, side_core]

    loads["hid"].wait()
    hid_full = hid_ref[...].astype(f32).T
    for to in range(rows):
        parts = [
            hid_full[block * b + GSIZE * (to // 2) : block * b + GSIZE * (to // 2 + 1)]
            for b in (to % 2, to % 2 + 2)
        ]
        for slot in range(2):
            hid_two[to, slot] = parts[slot].astype(bf16)
    for off in range(1, rows):
        to = lax.rem(r + off, rows)
        remote(hid_two.at[to], hid_b.at[:, r], h_send.at[0], h_recv.at[0], rows=to).start()
    hid_b[:, r] = hid_two[r]

    remote(s2, w2.at[d, 1 - k], b_send.at[0], b_recv.at[0], rows=sibling).wait_recv()
    start_hops(0, w2, 1 - k)

    forward(0, w2, 1, 0)
    loads["lat"].wait()
    lane = lax.broadcasted_iota(jnp.int32, (1, lanes), 1)
    column = lax.rem(lane, breadth)
    image_of = lax.div(lane, breadth)
    quarter = lax.rem(lane, breadth) // (breadth // 4)

    def image_totals(per_lane):
        total = jnp.zeros_like(per_lane)
        for image in range(images):
            mine = image_of == image
            part = jnp.sum(jnp.where(mine, per_lane, 0.0), axis=1, keepdims=True)
            total = jnp.where(mine, part, total)
        return total

    def pack_sums(one, two):
        one, two = image_totals(one), image_totals(two)
        top, low = slice(0, groups // 2), slice(groups // 2, groups)
        return jnp.where(
            quarter == 0, one[top], jnp.where(quarter == 1, two[top], jnp.where(quarter == 2, one[low], two[low]))
        )

    def send_sums(which, packed):
        st_s[which] = packed
        for off in range(1, rows):
            to = lax.rem(r + off, rows)
            remote(st_s.at[which], st_b.at[which, r], t_send.at[0], t_recv.at[which], rows=to).start()
        st_b[which, r] = packed

    def wait_sums(which):
        span = st_b.at[which, 0 : rows - 1]
        remote(span, span, t_send.at[0], t_recv.at[which], rows=sibling).wait_recv()
        total = st_b[which, 0]
        for h in range(1, rows):
            total = total + st_b[which, h]
        total = total * (1.0 / number)
        full = []
        for at in range(4):
            mine = jnp.where(quarter == at, total, 0.0)
            pair = mine + pltpu.roll(mine, ((1 if at % 2 == 0 else -1) * breadth // 4) % lanes, 1)
            full.append(pair + pltpu.roll(pair, ((1 if at < 2 else -1) * breadth // 2) % lanes, 1))
        return jnp.concatenate([full[0], full[2]], axis=0), jnp.concatenate([full[1], full[3]], axis=0)

    def spread(moment):
        return jnp.broadcast_to(moment[:, None, :], (groups, GSIZE, lanes)).reshape(channels, lanes)

    def by_group(values):
        return jnp.sum(values.reshape(groups, GSIZE, lanes), axis=1)

    nrm1[...] = lat_ref[...].astype(f32).T
    send_sums(0, pack_sums(by_group(nrm1[...]), by_group(nrm1[...] * nrm1[...])))

    pltpu.make_async_copy(vectors, vectors, in_sem.at[5]).wait()
    raw_params = [vectors[index] for index in range(4)]
    par_ref[...] = jnp.concatenate(raw_params + raw_params, axis=0).T

    def store_shifts(xs, part, h, values):
        left = jnp.where(column == breadth - 1, 0.0, pltpu.roll(values, lanes - 1, 1))
        right = jnp.where(column == 0, 0.0, pltpu.roll(values, 1, 1))
        xs[part, h, 0:half] = left.astype(bf16)
        xs[part, h, half : 2 * half] = values.astype(bf16)
        xs[part, h, 2 * half : 3 * half] = right.astype(bf16)

    def wait_group(src, dst, send, recv):
        remote(src, dst, send, recv, rows=sibling).wait_recv()

    forward(0, w2, 1, 1)
    everyone = x_cot.at[0, 0 : chips - 1]
    wait_group(everyone, everyone, c_send.at[0], c_recv.at[0])

    def share(x, at):
        return remote(x.at[k], x.at[k], c_send.at[1], d_recv.at[at], rows=sibling)

    def shift_rows(x, xs):
        for h in range(rows):
            values = x[h % 2, h // 2].astype(f32)
            for part in range(2):
                store_shifts(xs, part, h, values[part * half : (part + 1) * half])

    share(x_cot, 0).start()
    lend_cot = remote(x_cot.at[k], x_far.at[k], c_send.at[1], c_recv.at[1], dp=partner)
    lend_hid = remote(hid_b.at[lent], hid_far, h_send.at[1], h_recv.at[1], dp=partner)

    @pl.when(jnp.logical_not(middle))
    def _():
        lend_cot.start()

    forward(0, w2, 1, 2)
    share(x_cot, 0).wait_recv()
    shift_rows(x_cot, xs2)

    def conv(w, origin, xs):
        for h in range(0, rows, 2):
            total = None
            for part in range(2):
                pair = jnp.concatenate([xs[part, h], xs[part, h + 1]], axis=1)
                term = jnp.dot(w[origin, part], pair, preferred_element_type=f32)
                total = term if total is None else total + term
            y_ref[h] = total[:, :lanes]
            y_ref[h + 1] = total[:, lanes:]

    def row_of(h):
        total = y_ref[h, half : 2 * half]
        if h + 1 < rows:
            total = total + y_ref[h + 1, 0:half]
        if h > 0:
            total = total + y_ref[h - 1, 2 * half : 3 * half]
        return total

    def conv_two(origin, xs, p, q, send, recv):
        conv(w2, origin, xs)
        for h in range(0, rows, 2):
            low, high = row_of(h), row_of(h + 1)
            for j in range(2):
                both = [low[j * GSIZE : (j + 1) * GSIZE], high[j * GSIZE : (j + 1) * GSIZE]]
                p[j, h // 2] = jnp.concatenate(both, axis=0).astype(bf16)
        for j in range(2):
            to = 2 * (2 * k + j) + lax.rem(origin, 2)

            @pl.when(to != r)
            def _():
                remote(p.at[j], q.at[c], send, recv, rows=to).start()

            @pl.when(to == r)
            def _():
                q[c] = p[j]

    def conv_own(origin):
        slot = origin // 2
        conv_two(origin, xs2, p1.at[origin], q1.at[slot], p_send.at[0], p_recv.at[slot])

    def conv_far(step):
        conv_two(nth(step), xs_far, p_far.at[step - 2], q_far, p_send.at[1], p_recv.at[2])

    def conv_half(origin, part, more):
        for h in range(0, rows, 2):
            pair = jnp.concatenate([xs1[part, h], xs1[part, h + 1]], axis=1)
            term = jnp.dot(w1[origin, part], pair, preferred_element_type=f32)
            for side in range(2):
                value = term[:, side * lanes : (side + 1) * lanes]
                y_ref[h + side] = y_ref[h + side] + value if more else value

    def conv_one(origin, last=0):
        conv(w1, origin, xs1)
        send_rows(origin, last)

    def send_rows(origin, last=0):
        for h in range(rows):
            p2[origin, h] = row_of(h).astype(bf16)
        for off in range(1, rows):
            to = lax.rem(r + off, rows)
            remote(p2.at[origin, to], q2.at[origin, r], o_send.at[0], o_recv.at[last], rows=to).start()
        q2[origin, r] = p2[origin, r]

    conv_own(d)
    forward(0, w2, 1, 3)
    for count, here in ((chips - 1, own), (chips, jnp.logical_not(own))):
        @pl.when(here)
        def _():
            span = r1.at[0:count]
            wait_group(span, span, f_send.at[0], f_recv.at[0])

    for part in range(2):
        for j in range(2):
            for side in range(3):
                at = side * half + j * GSIZE
                piece = r1[2 * j + part, :, :, side * GSIZE : (side + 1) * GSIZE]
                w1[d, part, :, at : at + GSIZE] = piece.reshape(tall, GSIZE)
        pack(w1.at[d, part])

    def start_inner(toward):
        for here, way in ((1, toward), (2, 1 - toward)):
            @pl.when(d == here)
            def _():
                start_one((way,))

    start_inner(1)

    take_end(0, w2, 1)
    unpack(w2, nth(1))
    conv_own(nth(1))
    @pl.when(middle)
    def _():
        take(0, w2, 2)
        unpack(w2, nth(2))
        conv_own(nth(2))

    def activation(normed, gain, shift):
        linear = normed * gain + shift
        logistic = 1.0 / (1.0 + jnp.exp(-linear))
        return logistic * (1.0 + linear * (1.0 - logistic)) * gain

    everyone = hid_two.at[0 : rows - 1]
    wait_group(everyone, everyone, h_send.at[0], h_recv.at[0])

    @pl.when(jnp.logical_not(middle))
    def _():
        lend_hid.start()
        start_one((0, 1))

    def field_stats(field, slot, nrm, act, inverse_at):
        plain = jnp.zeros((GSIZE, lanes), f32)
        square = jnp.zeros((GSIZE, lanes), f32)
        for h in range(rows):
            values = field[h].astype(f32)
            plain += values
            square += values * values
        average = image_totals(jnp.sum(plain, axis=0, keepdims=True)) * (1.0 / number)
        meansq = image_totals(jnp.sum(square, axis=0, keepdims=True)) * (1.0 / number)
        inverse = lax.rsqrt(meansq - average * average + 1e-05)
        inv2_ref[inverse_at : inverse_at + 1] = inverse
        at = pl.multiple_of((k + 2 * slot) * block + GSIZE * c, GSIZE)
        gain = par_ref[pl.ds(at, GSIZE), 2:3]
        shift = par_ref[pl.ds(at, GSIZE), 3:4]
        for h in range(rows):
            normed = (field[h].astype(f32) - average) * inverse
            spot = (h % 2) * GSIZE
            nrm[h // 2, spot : spot + GSIZE] = normed
            act[h // 2, spot : spot + GSIZE] = activation(normed, gain, shift)

    for slot in range(2):
        field_stats(hid_b.at[slot], slot, nrm2.at[slot], act2.at[slot], slot)

    @pl.when(middle)
    def _():
        start_inner(0)
        lend_cot.wait_recv()
        share(x_far, 1).start()
        share(x_far, 1).wait_recv()
        shift_rows(x_far, xs_far)
        conv_far(2)
        take(0, w2, 3)
        unpack(w2, nth(3))
        conv_far(3)
        conv_own(nth(3))

    forward(1, w1, 2, 0)
    forward(1, w1, 1, 0)
    @pl.when(middle)
    def _():
        lend_hid.wait_recv()
        field_stats(hid_far, lent, nrm_far, act_far, 2)

    forward(1, w1, 2, 1)
    forward(1, w1, 1, 1)

    average1, meansq1 = wait_sums(0)
    inverse1 = lax.rsqrt(meansq1 - average1 * average1 + 1e-05)
    for g in range(groups):
        rows_g = pl.ds(g * GSIZE, GSIZE)
        normed = (nrm1[rows_g, :] - average1[g : g + 1]) * inverse1[g : g + 1]
        nrm1[rows_g, :] = normed
        act1[rows_g, :] = activation(normed, par_ref[rows_g, 0:1], par_ref[rows_g, 1:2])

    def norm_two(slot, recv, q, nrm, act, inverse, dst):
        for count, here in ((chips - 1, own), (chips, jnp.logical_not(own))):
            @pl.when(here)
            def _():
                span = q.at[0:count]
                wait_group(span, span, p_send.at[0], recv)

        sum_first = jnp.zeros((2 * GSIZE, lanes), f32)
        sum_second = jnp.zeros((2 * GSIZE, lanes), f32)
        scaled = []
        for m in range(rows // 2):
            total = q[0, m].astype(f32)
            for frm in range(1, chips):
                total = total + q[frm, m].astype(f32)
            value = total * act[m]
            scaled.append(value)
            sum_first += value
            sum_second += value * nrm[m]
        first = image_totals(jnp.sum(sum_first, axis=0, keepdims=True)) * (1.0 / number)
        second = image_totals(jnp.sum(sum_second, axis=0, keepdims=True)) * (1.0 / number)
        for m in range(rows // 2):
            dst[m] = (inverse * (scaled[m] - first - nrm[m] * second)).astype(bf16)

    def norm_own(slot):
        norm_two(
            slot, p_recv.at[slot], q1.at[slot], nrm2.at[slot], act2.at[slot],
            inv2_ref[pl.ds(slot, 1), :], hg_two.at[slot],
        )

    lend = remote(hg_far, hg_two.at[lent], e_send.at[0], e_recv.at[0], dp=partner)

    @pl.when(middle)
    def _():
        norm_two(lent, p_recv.at[2], q_far, nrm_far, act_far, inv2_ref[2:3, :], hg_far)
        lend.start()

    forward(1, w1, 2, 2)
    forward(1, w1, 1, 2)
    forward(1, w1, 2, 3)
    forward(1, w1, 1, 3)
    @pl.when(middle)
    def _():
        norm_own(0)
        norm_own(1)

    @pl.when(jnp.logical_not(middle))
    def _():
        norm_own(1 - lent)
        lend.wait_recv()

    for h in range(rows):
        spot = (h % 2) * GSIZE
        both = [hg_two[slot, h // 2].astype(f32)[spot : spot + GSIZE] for slot in range(2)]
        hg_s[h] = jnp.concatenate(both, axis=0).astype(bf16)
    swap = remote(hg_s, hg_r, b_send.at[1], b_recv.at[1], rows=sibling)
    swap.start()
    pending.append(swap)
    for h in range(rows):
        store_shifts(xs1, k, h, hg_s[h].astype(f32))
    forward(1, w1, 3, 0)
    conv_half(d, k, False)
    forward(1, w1, 3, 1)
    forward(1, w1, 3, 2)
    forward(1, w1, 3, 3)
    swap.wait_recv()
    for h in range(rows):
        store_shifts(xs1, 1 - k, h, hg_r[h].astype(f32))

    conv_half(d, 1 - k, True)
    send_rows(d)
    take_end(1, w1, 1)
    unpack(w1, nth(1))
    conv_one(nth(1))
    take_end(1, w1, 2)
    unpack(w1, nth(2))
    conv_one(nth(2))
    take_end(1, w1, 3, (k,))
    unpack(w1, nth(3), (k,))
    conv_half(nth(3), k, False)
    take_end(1, w1, 3, (1 - k,))
    unpack(w1, nth(3), (1 - k,))
    conv_half(nth(3), 1 - k, True)
    send_rows(nth(3), 1)
    def close_block(origin):
        for part in range(2):
            total = q2[origin, part].astype(f32)
            for frm in range(1, chips):
                total = total + q2[origin, 2 * frm + part].astype(f32)
            at = pl.ds(pl.multiple_of(origin * block + part * half, half), half)
            value = total * act1[at, :]
            act1[at, :] = value
            sums_ref[0, origin, part] = jnp.sum(value.reshape(2, GSIZE, lanes), axis=1)
            sums_ref[1, origin, part] = jnp.sum((value * nrm1[at, :]).reshape(2, GSIZE, lanes), axis=1)

    span = q2.at[0 : depth - 1, 0 : rows - 1]
    wait_group(span, span, o_send.at[0], o_recv.at[0])
    for origin in (d, nth(1), nth(2)):
        close_block(origin)
    span = q2.at[0, 0 : rows - 1]
    wait_group(span, span, o_send.at[0], o_recv.at[1])
    close_block(nth(3))
    one, two = [
        jnp.concatenate([sums_ref[which, origin, part] for origin in range(depth) for part in range(2)], axis=0)
        for which in range(2)
    ]
    send_sums(1, pack_sums(one, two))
    first1, second1 = wait_sums(1)
    value = spread(inverse1) * (act1[...] - spread(first1) - nrm1[...] * spread(second1))
    out_ref[...] = (cot_t[...].astype(f32) + value).astype(bf16).T

    for copy in pending:
        copy.wait_send()
    def sent(span, send, recv):
        remote(span, span, send, recv, rows=sibling).wait_send()

    sent(x_cot.at[0, 0 : chips - 1], c_send.at[0], c_recv.at[0])
    sent(x_far, c_send.at[1], d_recv.at[0])
    sent(hid_two.at[0 : rows - 1], h_send.at[0], h_recv.at[0])
    sent(st_b.at[:, 0 : rows - 1], t_send.at[0], t_recv.at[0])
    sent(p2.at[:, 0 : rows - 1], o_send.at[0], o_recv.at[0])
    for count, here in ((chips - 1, own), (chips, jnp.logical_not(own))):
        @pl.when(here)
        def _():
            sent(r1.at[0:count], f_send.at[0], f_recv.at[0])

            @pl.when(middle)
            def _():
                sent(q1.at[:, 0:count], p_send.at[0], p_recv.at[0])
                sent(q_far.at[0:count], p_send.at[1], p_recv.at[2])

            @pl.when(jnp.logical_not(middle))
            def _():
                sent(q1.at[0, 0:count], p_send.at[0], p_recv.at[0])

    @pl.when(middle)
    def _():
        lend.wait_send()

    @pl.when(jnp.logical_not(middle))
    def _():
        lend_hid.wait_send()

    @pl.when(middle)
    def _():
        wait_hops(2 * depth)

    @pl.when(jnp.logical_not(middle))
    def _():
        wait_hops(2)


def kernel_body(
    depth, rows,
    latent, hidden, cotangent, filter_one, filter_two, gain_one, shift_one, gain_two, shift_two,
):
    images, _, breadth, channels = latent.shape
    lanes = images * breadth
    block = channels // depth
    half = block // 2
    chips = rows // 2
    wide = -(-3 * half // 128) * 128
    narrow = -(-3 * GSIZE // 128) * 128
    groups = channels // GSIZE
    bf16, f32 = jnp.bfloat16, jnp.float32
    dma = pltpu.SemaphoreType.DMA
    out = pl.pallas_call(
        functools.partial(kernel, depth, rows, breadth),
        out_shape=jax.ShapeDtypeStruct((lanes, channels), bf16),
        in_specs=[pl.BlockSpec(memory_space=pltpu.HBM)] * 9,
        out_specs=pl.BlockSpec(memory_space=pltpu.VMEM),
        scratch_shapes=[
            pltpu.VMEM((lanes, channels), bf16),
            pltpu.VMEM((lanes, channels), bf16),
            pltpu.VMEM((lanes, channels), bf16),
            pltpu.VMEM(filter_one.shape, bf16),
            pltpu.VMEM(filter_two.shape, bf16),
            pltpu.VMEM((4, 1, channels), f32),
            dma((6,)),
            pltpu.VMEM((channels, lanes), bf16),
            pltpu.VMEM((2, chips, block, lanes), bf16),
            pltpu.VMEM((2, rows, GSIZE, lanes), bf16),
            pltpu.VMEM((depth, 2, 3 * half, wide), bf16),
            pltpu.VMEM((depth, 2, 3 * half, wide), bf16),
            pltpu.VMEM((2, 2, 3, half, narrow), bf16),
            pltpu.VMEM((3 * half, wide), bf16),
            pltpu.VMEM((chips, 3, half, narrow), bf16),
            pltpu.VMEM((2, rows, wide, lanes), bf16),
            pltpu.VMEM((2, rows, wide, lanes), bf16),
            pltpu.VMEM((rows, 3 * half, lanes), f32),
            pltpu.VMEM((depth, 2, rows // 2, 2 * GSIZE, lanes), bf16),
            pltpu.VMEM((2, chips, rows // 2, 2 * GSIZE, lanes), bf16),
            pltpu.VMEM((depth, rows, half, lanes), bf16),
            pltpu.VMEM((depth, rows, half, lanes), bf16),
            pltpu.VMEM((rows, 2 * GSIZE, lanes), bf16),
            pltpu.VMEM((rows, 2 * GSIZE, lanes), bf16),
            pltpu.VMEM((channels, lanes), f32),
            pltpu.VMEM((channels, lanes), f32),
            pltpu.VMEM((2, rows // 2, 2 * GSIZE, lanes), f32),
            pltpu.VMEM((2, rows // 2, 2 * GSIZE, lanes), f32),
            pltpu.VMEM((4, lanes), f32),
            pltpu.VMEM((2, groups // 2, lanes), f32),
            pltpu.VMEM((2, rows, groups // 2, lanes), f32),
            pltpu.VMEM((channels, 8), f32),
            pltpu.VMEM((2, depth, 2, 2, lanes), f32),
            pltpu.VMEM((2, chips, block, lanes), bf16),
            pltpu.VMEM((rows, 2, GSIZE, lanes), bf16),
            pltpu.VMEM((rows, GSIZE, lanes), bf16),
            pltpu.VMEM((2, rows, wide, lanes), bf16),
            pltpu.VMEM((2, 2, rows // 2, 2 * GSIZE, lanes), bf16),
            pltpu.VMEM((chips, rows // 2, 2 * GSIZE, lanes), bf16),
            pltpu.VMEM((rows // 2, 2 * GSIZE, lanes), f32),
            pltpu.VMEM((rows // 2, 2 * GSIZE, lanes), f32),
            pltpu.VMEM((rows // 2, 2 * GSIZE, lanes), bf16),
            pltpu.VMEM((2, rows // 2, 2 * GSIZE, lanes), bf16),
            dma((2,)), dma((2, depth - 1, 2, 2)),
            dma((1,)), dma((1,)),
            dma((2,)), dma((2,)),
            dma((2,)), dma((2,)),
            dma((2,)), dma((2,)),
            dma((2,)), dma((3,)),
            dma((1,)), dma((2,)),
            dma((1,)), dma((2,)),
            dma((2,)),
            dma((1,)), dma((1,)),
        ],
        compiler_params=pltpu.CompilerParams(
            collective_id=0, has_side_effects=True, vmem_limit_bytes=48 * 1024 * 1024
        ),
    )(
        *[
            pltpu.with_memory_space_constraint(array, pltpu.HBM)
            for array in (
                latent.reshape(lanes, channels), hidden.reshape(lanes, channels),
                cotangent.reshape(lanes, channels), filter_one, filter_two,
                gain_one, shift_one, gain_two, shift_two,
            )
        ]
    )
    return out.reshape(latent.shape)


def solution(mesh):
    depth, rows = mesh.shape["dp"], mesh.shape["rows"]
    in_specs = (
        P("dp", "rows", None, None),
        P("dp", "rows", None, None),
        P("dp", "rows", None, None),
        P(None, "dp", "rows"),
        P(None, "dp", "rows"),
        P(),
        P(),
        P(),
        P(),
    )

    def body(latent, *rest):
        images, rows_here, breadth, channels = latent.shape
        fits = (
            rows_here == 1
            and images * breadth == 128
            and breadth % 4 == 0
            and depth == 4
            and rows == 2 * depth
            and channels == GROUPS * GSIZE
            and channels == depth * (rows // 2) * GSIZE
        )
        if fits:
            return kernel_body(depth, rows, latent, *rest)
        return plain_body(latent, *rest)

    return jax.shard_map(
        body, mesh=mesh, in_specs=in_specs, out_specs=P("dp", "rows", None, None), check_vma=False
    )
```

```python
import functools

import jax
import jax.numpy as jnp
from jax import lax
from jax.experimental import pallas as pl
from jax.experimental.pallas import tpu as pltpu
from jax.sharding import PartitionSpec as P

GROUPS = 16
GSIZE = 40
TAPS = 9
MESH = pl.DeviceIdType.MESH


def extended(block, sides, width):
    for axis, dim in sides:
        count = lax.axis_size(axis)
        forward = [(i, i + 1) for i in range(count - 1)]
        backward = [(target, source) for source, target in forward]
        low = lax.ppermute(
            lax.slice_in_dim(block, block.shape[dim] - width, None, axis=dim), axis, forward
        )
        high = lax.ppermute(lax.slice_in_dim(block, 0, width, axis=dim), axis, backward)
        block = jnp.concatenate([low, block, high], axis=dim)
    return block


def group_sums(values):
    per_channel = jnp.sum(values, axis=(1, 2))
    return jnp.sum(per_channel.reshape(per_channel.shape[0], GROUPS, -1), axis=2)


def expand_groups(moment):
    return jnp.repeat(moment, GSIZE, axis=1)[:, None, None, :]


def finish_stats(sum_plain, sum_square, number):
    average = sum_plain / number
    variance = sum_square / number - average * average
    return (average, lax.rsqrt(variance + 1e-05))


def reduced_stats(field, number):
    values = field.astype(jnp.float32)
    sum_plain, sum_square = lax.psum((group_sums(values), group_sums(values * values)), "rows")
    return finish_stats(sum_plain, sum_square, number)


def norm_backward(field, stats, gain, shift, incoming, number):
    average, inverse = stats
    values = field.astype(jnp.float32)
    normed = (values - expand_groups(average)) * expand_groups(inverse)
    linear = normed * gain + shift
    logistic = jax.nn.sigmoid(linear)
    scaled = incoming * logistic * (1.0 + linear * (1.0 - logistic)) * gain
    sum_first, sum_second = lax.psum((group_sums(scaled), group_sums(scaled * normed)), "rows")
    first = sum_first / number
    second = sum_second / number
    return expand_groups(inverse) * (scaled - expand_groups(first) - normed * expand_groups(second))


def conv_backward(gradient, weights):
    images, rows_here, breadth, channels = gradient.shape
    padded = extended(gradient, (("rows", 1),), 1)
    padded = jnp.pad(padded, ((0, 0), (0, 0), (1, 1), (0, 0)))
    pixels = images * rows_here * breadth
    shifted = []
    for tap_index in range(9):
        down_step = tap_index // 3 - 1
        side_step = tap_index % 3 - 1
        window = padded[
            :, 1 - down_step : 1 - down_step + rows_here, 1 - side_step : 1 - side_step + breadth, :
        ]
        shifted.append(window.reshape(pixels, channels))
    stacked = jnp.stack(shifted, axis=1)
    gathered = lax.all_gather(weights, "dp", axis=1, tiled=True)
    section = lax.all_gather(gathered, "rows", axis=2, tiled=True)
    columns = section.shape[2]
    window = stacked.reshape(pixels, 9 * columns)
    flat = jnp.transpose(section, (0, 2, 1)).reshape(9 * columns, section.shape[1])
    result = jnp.dot(window, flat, preferred_element_type=jnp.float32)
    return result.reshape(images, rows_here, breadth, channels)


def plain_body(
    latent, hidden, cotangent, filter_one, filter_two, gain_one, shift_one, gain_two, shift_two
):
    number = latent.shape[1] * lax.axis_size("rows") * latent.shape[2] * GSIZE
    stats_two = reduced_stats(hidden, number)
    back_two = conv_backward(cotangent, filter_two)
    hidden_grad = norm_backward(hidden, stats_two, gain_two, shift_two, back_two, number).astype(
        jnp.bfloat16
    )
    stats_one = reduced_stats(latent, number)
    back_one = conv_backward(hidden_grad, filter_one)
    latent_part = norm_backward(latent, stats_one, gain_one, shift_one, back_one, number)
    return (cotangent.astype(jnp.float32) + latent_part).astype(jnp.bfloat16)


def kernel(
    depth, rows, breadth,
    lat_hbm, hid_hbm, cot_hbm, raw1_hbm, raw2_hbm, gain1_hbm, shift1_hbm, gain2_hbm, shift2_hbm,
    out_ref,
    lat_ref, hid_ref, cot_ref, raw1, raw2, vectors, in_sem,
    cot_t, x_cot, hid_b, w1, w2, s1, s2, r1,
    xs1, xs2, y_ref, p1, q1, p2, q2, hg_s, hg_r,
    nrm1, act1, nrm2, act2, inv2_ref, st_s, st_b, par_ref,
    sums_ref, x_far, hid_two, hid_far, xs_far, p_far, q_far, nrm_far, act_far, hg_far, hg_two,
    z_send, z_recv, f_send, f_recv, b_send, b_recv, c_send, c_recv, h_send, h_recv,
    p_send, p_recv, o_send, o_recv, t_send, t_recv, d_recv, e_send, e_recv,
):
    d = lax.axis_index("dp")
    r = lax.axis_index("rows")
    chips = rows // 2
    c = r // 2
    k = lax.rem(r, 2)
    sibling = r + 1 - 2 * k
    channels, lanes = cot_t.shape
    block = channels // depth
    half = block // 2
    images = lanes // breadth
    wide = w1.shape[3]
    number = rows * breadth * GSIZE
    groups = channels // GSIZE
    bf16, f32 = jnp.bfloat16, jnp.float32
    across, along, beside = chips - 1 - c, lax.rem(c + 2, chips), c + 1 - 2 * lax.rem(c, 2)
    others = [2 * across + k, 2 * beside + k, 2 * across + 1 - k, 2 * beside + 1 - k, 2 * along + k, 2 * along + 1 - k, sibling]

    def remote(src, dst, send, recv, **device):
        return pltpu.make_async_remote_copy(
            src_ref=src, dst_ref=dst, send_sem=send, recv_sem=recv,
            device_id=device, device_id_type=MESH,
        )

    pending = []
    loads = {
        name: pltpu.make_async_copy(src, dst, in_sem.at[index])
        for index, (name, src, dst) in enumerate((
            ("raw2", raw2_hbm, raw2), ("cot", cot_hbm, cot_ref), ("hid", hid_hbm, hid_ref),
            ("raw1", raw1_hbm, raw1), ("lat", lat_hbm, lat_ref),
        ))
    }
    for index, src in enumerate((gain1_hbm, shift1_hbm, gain2_hbm, shift2_hbm)):
        loads[index] = pltpu.make_async_copy(src, vectors.at[index, 0], in_sem.at[5])
    loads["raw2"].start()

    barrier = pltpu.get_barrier_semaphore()

    middle = (d > 0) & (d < depth - 1)
    partner = d + 1 - 2 * lax.rem(d, 2)
    lent = jnp.where(2 * d < depth, 1, 0)

    @pl.when(d > 0)
    def _():
        pl.semaphore_signal(barrier, inc=1, device_id={"dp": d - 1}, device_id_type=MESH)

    @pl.when(d < depth - 1)
    def _():
        pl.semaphore_signal(barrier, inc=1, device_id={"dp": d + 1}, device_id_type=MESH)

    for off in range(1, rows):
        pl.semaphore_signal(barrier, inc=1, device_id={"rows": lax.rem(r + off, rows)}, device_id_type=MESH)

    for name, load in loads.items():
        if name != "raw2":
            load.start()

    pad = wide - 3 * half
    own = k == c // 2
    tall = 3 * half
    w2[d, k, :, tall:] = jnp.zeros((tall, pad), bf16)
    s2[:, tall:] = jnp.zeros((tall, pad), bf16)
    for part in range(2):
        w1[d, part, :, tall:] = jnp.zeros((tall, pad), bf16)
        for side_core in range(2):
            s1[part, side_core, :, :, 3 * GSIZE :] = jnp.zeros((3, half, s1.shape[4] - 3 * GSIZE), bf16)
    for xs in (xs1, xs2, xs_far):
        for part in range(2):
            for h in range(rows):
                xs[part, h, 3 * half :] = jnp.zeros((pad, lanes), bf16)
    loads["raw2"].wait()

    def arrange(ready, raw, which):
        start = pl.multiple_of(which * half, 16)
        for tap in range(TAPS):
            down, side = tap // 3, tap % 3
            ready[down * half : (down + 1) * half, side * half : (side + 1) * half] = raw[
                tap, pl.ds(start, half), :
            ]

    def pack(ready):
        for at in range((tall - 128) // pad):
            ready[pad * at : pad * (at + 1), tall:] = ready[tall - pad :, 128 + pad * at : 128 + pad * (at + 1)]

    def unpack(w, origin, parts=(0, 1)):
        for part in parts:
            pieces = [w[origin, part, pad * at : pad * (at + 1), tall:] for at in range((tall - 128) // pad)]
            full = jnp.concatenate(pieces + [jnp.zeros((pad, pad), bf16)], axis=1)
            w[origin, part, tall - pad :, 128:] = full

    arrange(w2.at[d, k], raw2, k)

    pl.semaphore_wait(barrier, rows + jnp.where(middle, 1, 0))

    segments = ((tall, 0, 128), (tall - pad, 128, wide))

    def hop(which, w, origin, part, seg, way):
        deep, low, high = segments[seg]
        piece = w.at[origin, part, 0:deep, low:high]
        return remote(
            piece, piece, z_send.at[seg], z_recv.at[which, origin - way, part, seg], dp=d + 1 - 2 * way
        )

    near = jnp.minimum(d, depth - 1 - d)

    def nth(step):
        value = step - near if step == 1 else step
        return jnp.where(2 * d < depth, value, depth - 1 - value)

    def start_hops(which, w, part, ways=(0, 1), segs=(0, 1)):
        for way in ways:
            @pl.when((d < depth - 1) if way == 0 else (d > 0))
            def _():
                for seg in segs:
                    hop(which, w, d, part, seg, way).start()

    def start_one(ways):
        for part in (k, 1 - k):
            start_hops(1, w1, part, ways)

    def forward(which, w, step, index):
        origin = nth(step)
        part, seg = (k, 1 - k)[index // 2], index % 2
        for way in range(2):
            @pl.when(middle & ((origin < d) if way == 0 else (origin > d)))
            def _():
                copy = hop(which, w, origin, part, seg, way)
                copy.wait_recv()
                copy.start()

    def take(which, w, step, parts=(k, 1 - k)):
        for part in parts:
            for seg in range(2):
                origin = nth(step)
                hop(which, w, origin, part, seg, jnp.where(origin > d, 1, 0)).wait_recv()

    def take_end(which, w, step, parts=(k, 1 - k)):
        @pl.when(jnp.logical_not(middle))
        def _():
            take(which, w, step, parts)

    def wait_hops(count):
        for seg, (deep, _, _) in enumerate(segments):
            span = xs1.at[:, 0:count, 0:deep]
            remote(span, span, z_send.at[seg], z_recv.at[0, 0, 0, seg], rows=sibling).wait_send()

    start_hops(0, w2, k, segs=(0,))
    pack(w2.at[d, k])
    start_hops(0, w2, k, segs=(1,))
    arrange(s2, raw2, 1 - k)
    pack(s2)
    twin = remote(s2, w2.at[d, k], b_send.at[0], b_recv.at[0], rows=sibling)
    twin.start()
    pending.append(twin)

    loads["cot"].wait()
    cot_t[...] = cot_ref[...].T

    def piece_of(to):
        return cot_t.at[pl.ds(pl.multiple_of((to // 2) * block, block), block), :]

    for off in range(1, chips):
        to = 2 * lax.rem(c + off, chips) + k
        remote(piece_of(to), x_cot.at[k, c], c_send.at[0], c_recv.at[0], rows=to).start()
    x_cot[k, c] = piece_of(r)[...]

    loads["raw1"].wait()
    for part in range(2):
        for side_core in range(2):
            ready = s1.at[part, side_core]
            for tap in range(TAPS):
                down, side = tap // 3, tap % 3
                ready[down, :, side * GSIZE : (side + 1) * GSIZE] = raw1[
                    tap, side_core * half : (side_core + 1) * half, part * GSIZE : (part + 1) * GSIZE
                ]

    for part in range(2):
        for side_core in range(2):
            to = 2 * (2 * k + part) + side_core

            @pl.when(to != r)
            def _():
                remote(s1.at[part, side_core], r1.at[c], f_send.at[0], f_recv.at[0], rows=to).start()

            @pl.when(to == r)
            def _():
                r1[c] = s1[part, side_core]

    loads["hid"].wait()
    hid_full = hid_ref[...].astype(f32).T
    for to in range(rows):
        parts = [
            hid_full[block * b + GSIZE * (to // 2) : block * b + GSIZE * (to // 2 + 1)]
            for b in (to % 2, to % 2 + 2)
        ]
        for slot in range(2):
            hid_two[to, slot] = parts[slot].astype(bf16)
    for off in range(1, rows):
        to = lax.rem(r + off, rows)
        remote(hid_two.at[to], hid_b.at[:, r], h_send.at[0], h_recv.at[0], rows=to).start()
    hid_b[:, r] = hid_two[r]

    remote(s2, w2.at[d, 1 - k], b_send.at[0], b_recv.at[0], rows=sibling).wait_recv()
    start_hops(0, w2, 1 - k)

    forward(0, w2, 1, 0)
    loads["lat"].wait()
    lane = lax.broadcasted_iota(jnp.int32, (1, lanes), 1)
    column = lax.rem(lane, breadth)
    image_of = lax.div(lane, breadth)
    quarter = lax.rem(lane, breadth) // (breadth // 4)

    def image_totals(per_lane):
        total = jnp.zeros_like(per_lane)
        for image in range(images):
            mine = image_of == image
            part = jnp.sum(jnp.where(mine, per_lane, 0.0), axis=1, keepdims=True)
            total = jnp.where(mine, part, total)
        return total

    def pack_sums(one, two):
        one, two = image_totals(one), image_totals(two)
        top, low = slice(0, groups // 2), slice(groups // 2, groups)
        return jnp.where(
            quarter == 0, one[top], jnp.where(quarter == 1, two[top], jnp.where(quarter == 2, one[low], two[low]))
        )

    def send_sums(which, packed):
        st_s[which] = packed
        for to in others:
            remote(st_s.at[which], st_b.at[which, r], t_send.at[0], t_recv.at[which], rows=to).start()
        st_b[which, r] = packed

    def wait_sums(which):
        span = st_b.at[which, 0 : rows - 1]
        remote(span, span, t_send.at[0], t_recv.at[which], rows=sibling).wait_recv()
        total = st_b[which, 0]
        for h in range(1, rows):
            total = total + st_b[which, h]
        total = total * (1.0 / number)
        full = []
        for at in range(4):
            mine = jnp.where(quarter == at, total, 0.0)
            pair = mine + pltpu.roll(mine, ((1 if at % 2 == 0 else -1) * breadth // 4) % lanes, 1)
            full.append(pair + pltpu.roll(pair, ((1 if at < 2 else -1) * breadth // 2) % lanes, 1))
        return jnp.concatenate([full[0], full[2]], axis=0), jnp.concatenate([full[1], full[3]], axis=0)

    def spread(moment):
        return jnp.broadcast_to(moment[:, None, :], (groups, GSIZE, lanes)).reshape(channels, lanes)

    def by_group(values):
        return jnp.sum(values.reshape(groups, GSIZE, lanes), axis=1)

    nrm1[...] = lat_ref[...].astype(f32).T
    send_sums(0, pack_sums(by_group(nrm1[...]), by_group(nrm1[...] * nrm1[...])))

    pltpu.make_async_copy(vectors, vectors, in_sem.at[5]).wait()
    raw_params = [vectors[index] for index in range(4)]
    par_ref[...] = jnp.concatenate(raw_params + raw_params, axis=0).T

    def store_shifts(xs, part, h, values):
        left = jnp.where(column == breadth - 1, 0.0, pltpu.roll(values, lanes - 1, 1))
        right = jnp.where(column == 0, 0.0, pltpu.roll(values, 1, 1))
        xs[part, h, 0:half] = left.astype(bf16)
        xs[part, h, half : 2 * half] = values.astype(bf16)
        xs[part, h, 2 * half : 3 * half] = right.astype(bf16)

    def wait_group(src, dst, send, recv):
        remote(src, dst, send, recv, rows=sibling).wait_recv()

    forward(0, w2, 1, 1)
    everyone = x_cot.at[0, 0 : chips - 1]
    wait_group(everyone, everyone, c_send.at[0], c_recv.at[0])

    def share(x, at):
        return remote(x.at[k], x.at[k], c_send.at[1], d_recv.at[at], rows=sibling)

    def shift_rows(x, xs):
        for h in range(rows):
            values = x[h % 2, h // 2].astype(f32)
            for part in range(2):
                store_shifts(xs, part, h, values[part * half : (part + 1) * half])

    share(x_cot, 0).start()
    lend_cot = remote(x_cot.at[k], x_far.at[k], c_send.at[1], c_recv.at[1], dp=partner)
    lend_hid = remote(hid_b.at[lent], hid_far, h_send.at[1], h_recv.at[1], dp=partner)

    @pl.when(jnp.logical_not(middle))
    def _():
        lend_cot.start()

    forward(0, w2, 1, 2)
    share(x_cot, 0).wait_recv()
    shift_rows(x_cot, xs2)

    def conv(w, origin, xs):
        for h in range(0, rows, 2):
            total = None
            for part in range(2):
                pair = jnp.concatenate([xs[part, h], xs[part, h + 1]], axis=1)
                term = jnp.dot(w[origin, part], pair, preferred_element_type=f32)
                total = term if total is None else total + term
            y_ref[h] = total[:, :lanes]
            y_ref[h + 1] = total[:, lanes:]

    def row_of(h):
        total = y_ref[h, half : 2 * half]
        if h + 1 < rows:
            total = total + y_ref[h + 1, 0:half]
        if h > 0:
            total = total + y_ref[h - 1, 2 * half : 3 * half]
        return total

    def conv_two(origin, xs, p, q, send, recv):
        conv(w2, origin, xs)
        for h in range(0, rows, 2):
            low, high = row_of(h), row_of(h + 1)
            for j in range(2):
                both = [low[j * GSIZE : (j + 1) * GSIZE], high[j * GSIZE : (j + 1) * GSIZE]]
                p[j, h // 2] = jnp.concatenate(both, axis=0).astype(bf16)
        for j in range(2):
            to = 2 * (2 * k + j) + lax.rem(origin, 2)

            @pl.when(to != r)
            def _():
                remote(p.at[j], q.at[c], send, recv, rows=to).start()

            @pl.when(to == r)
            def _():
                q[c] = p[j]

    def conv_own(origin):
        slot = origin // 2
        conv_two(origin, xs2, p1.at[origin], q1.at[slot], p_send.at[0], p_recv.at[slot])

    def conv_far(step):
        conv_two(nth(step), xs_far, p_far.at[step - 2], q_far, p_send.at[1], p_recv.at[2])

    def conv_half(origin, part, more):
        for h in range(0, rows, 2):
            pair = jnp.concatenate([xs1[part, h], xs1[part, h + 1]], axis=1)
            term = jnp.dot(w1[origin, part], pair, preferred_element_type=f32)
            for side in range(2):
                value = term[:, side * lanes : (side + 1) * lanes]
                y_ref[h + side] = y_ref[h + side] + value if more else value

    def conv_one(origin, last=0):
        conv(w1, origin, xs1)
        send_rows(origin, last)

    def send_rows(origin, last=0):
        for h in range(rows):
            p2[origin, h] = row_of(h).astype(bf16)
        for to in others:
            remote(p2.at[origin, to], q2.at[origin, r], o_send.at[0], o_recv.at[last], rows=to).start()
        q2[origin, r] = p2[origin, r]

    conv_own(d)
    forward(0, w2, 1, 3)
    for count, here in ((chips - 1, own), (chips, jnp.logical_not(own))):
        @pl.when(here)
        def _():
            span = r1.at[0:count]
            wait_group(span, span, f_send.at[0], f_recv.at[0])

    for part in range(2):
        for j in range(2):
            for side in range(3):
                at = side * half + j * GSIZE
                piece = r1[2 * j + part, :, :, side * GSIZE : (side + 1) * GSIZE]
                w1[d, part, :, at : at + GSIZE] = piece.reshape(tall, GSIZE)
        pack(w1.at[d, part])

    def start_inner(toward):
        for here, way in ((1, toward), (2, 1 - toward)):
            @pl.when(d == here)
            def _():
                start_one((way,))

    start_inner(1)

    take_end(0, w2, 1)
    unpack(w2, nth(1))
    conv_own(nth(1))
    @pl.when(middle)
    def _():
        take(0, w2, 2)
        unpack(w2, nth(2))
        conv_own(nth(2))

    def activation(normed, gain, shift):
        linear = normed * gain + shift
        logistic = 1.0 / (1.0 + jnp.exp(-linear))
        return logistic * (1.0 + linear * (1.0 - logistic)) * gain

    everyone = hid_two.at[0 : rows - 1]
    wait_group(everyone, everyone, h_send.at[0], h_recv.at[0])

    @pl.when(jnp.logical_not(middle))
    def _():
        lend_hid.start()
        start_one((0, 1))

    def field_stats(field, slot, nrm, act, inverse_at):
        plain = jnp.zeros((GSIZE, lanes), f32)
        square = jnp.zeros((GSIZE, lanes), f32)
        for h in range(rows):
            values = field[h].astype(f32)
            plain += values
            square += values * values
        average = image_totals(jnp.sum(plain, axis=0, keepdims=True)) * (1.0 / number)
        meansq = image_totals(jnp.sum(square, axis=0, keepdims=True)) * (1.0 / number)
        inverse = lax.rsqrt(meansq - average * average + 1e-05)
        inv2_ref[inverse_at : inverse_at + 1] = inverse
        at = pl.multiple_of((k + 2 * slot) * block + GSIZE * c, GSIZE)
        gain = par_ref[pl.ds(at, GSIZE), 2:3]
        shift = par_ref[pl.ds(at, GSIZE), 3:4]
        for h in range(rows):
            normed = (field[h].astype(f32) - average) * inverse
            spot = (h % 2) * GSIZE
            nrm[h // 2, spot : spot + GSIZE] = normed
            act[h // 2, spot : spot + GSIZE] = activation(normed, gain, shift)

    for slot in range(2):
        field_stats(hid_b.at[slot], slot, nrm2.at[slot], act2.at[slot], slot)

    @pl.when(middle)
    def _():
        start_inner(0)
        lend_cot.wait_recv()
        share(x_far, 1).start()
        share(x_far, 1).wait_recv()
        shift_rows(x_far, xs_far)
        conv_far(2)
        take(0, w2, 3)
        unpack(w2, nth(3))
        conv_far(3)
        conv_own(nth(3))

    forward(1, w1, 2, 0)
    forward(1, w1, 1, 0)
    @pl.when(middle)
    def _():
        lend_hid.wait_recv()
        field_stats(hid_far, lent, nrm_far, act_far, 2)

    forward(1, w1, 2, 1)
    forward(1, w1, 1, 1)

    average1, meansq1 = wait_sums(0)
    inverse1 = lax.rsqrt(meansq1 - average1 * average1 + 1e-05)
    for g in range(groups):
        rows_g = pl.ds(g * GSIZE, GSIZE)
        normed = (nrm1[rows_g, :] - average1[g : g + 1]) * inverse1[g : g + 1]
        nrm1[rows_g, :] = normed
        act1[rows_g, :] = activation(normed, par_ref[rows_g, 0:1], par_ref[rows_g, 1:2])

    def norm_two(slot, recv, q, nrm, act, inverse, dst):
        for count, here in ((chips - 1, own), (chips, jnp.logical_not(own))):
            @pl.when(here)
            def _():
                span = q.at[0:count]
                wait_group(span, span, p_send.at[0], recv)

        sum_first = jnp.zeros((2 * GSIZE, lanes), f32)
        sum_second = jnp.zeros((2 * GSIZE, lanes), f32)
        scaled = []
        for m in range(rows // 2):
            total = q[0, m].astype(f32)
            for frm in range(1, chips):
                total = total + q[frm, m].astype(f32)
            value = total * act[m]
            scaled.append(value)
            sum_first += value
            sum_second += value * nrm[m]
        first = image_totals(jnp.sum(sum_first, axis=0, keepdims=True)) * (1.0 / number)
        second = image_totals(jnp.sum(sum_second, axis=0, keepdims=True)) * (1.0 / number)
        for m in range(rows // 2):
            dst[m] = (inverse * (scaled[m] - first - nrm[m] * second)).astype(bf16)

    def norm_own(slot):
        norm_two(
            slot, p_recv.at[slot], q1.at[slot], nrm2.at[slot], act2.at[slot],
            inv2_ref[pl.ds(slot, 1), :], hg_two.at[slot],
        )

    lend = remote(hg_far, hg_two.at[lent], e_send.at[0], e_recv.at[0], dp=partner)

    @pl.when(middle)
    def _():
        norm_two(lent, p_recv.at[2], q_far, nrm_far, act_far, inv2_ref[2:3, :], hg_far)
        lend.start()

    forward(1, w1, 2, 2)
    forward(1, w1, 1, 2)
    forward(1, w1, 2, 3)
    forward(1, w1, 1, 3)
    @pl.when(middle)
    def _():
        norm_own(0)
        norm_own(1)

    @pl.when(jnp.logical_not(middle))
    def _():
        norm_own(1 - lent)
        lend.wait_recv()

    for h in range(rows):
        spot = (h % 2) * GSIZE
        both = [hg_two[slot, h // 2].astype(f32)[spot : spot + GSIZE] for slot in range(2)]
        hg_s[h] = jnp.concatenate(both, axis=0).astype(bf16)
    swap = remote(hg_s, hg_r, b_send.at[1], b_recv.at[1], rows=sibling)
    swap.start()
    pending.append(swap)
    for h in range(rows):
        store_shifts(xs1, k, h, hg_s[h].astype(f32))
    forward(1, w1, 3, 0)
    conv_half(d, k, False)
    forward(1, w1, 3, 1)
    forward(1, w1, 3, 2)
    forward(1, w1, 3, 3)
    swap.wait_recv()
    for h in range(rows):
        store_shifts(xs1, 1 - k, h, hg_r[h].astype(f32))

    conv_half(d, 1 - k, True)
    send_rows(d)
    take_end(1, w1, 1)
    unpack(w1, nth(1))
    conv_one(nth(1))
    take_end(1, w1, 2)
    unpack(w1, nth(2))
    conv_one(nth(2))
    take_end(1, w1, 3, (k,))
    unpack(w1, nth(3), (k,))
    conv_half(nth(3), k, False)
    take_end(1, w1, 3, (1 - k,))
    unpack(w1, nth(3), (1 - k,))
    conv_half(nth(3), 1 - k, True)
    send_rows(nth(3), 1)
    def close_block(origin):
        for part in range(2):
            total = q2[origin, part].astype(f32)
            for frm in range(1, chips):
                total = total + q2[origin, 2 * frm + part].astype(f32)
            at = pl.ds(pl.multiple_of(origin * block + part * half, half), half)
            value = total * act1[at, :]
            act1[at, :] = value
            sums_ref[0, origin, part] = jnp.sum(value.reshape(2, GSIZE, lanes), axis=1)
            sums_ref[1, origin, part] = jnp.sum((value * nrm1[at, :]).reshape(2, GSIZE, lanes), axis=1)

    span = q2.at[0 : depth - 1, 0 : rows - 1]
    wait_group(span, span, o_send.at[0], o_recv.at[0])
    for origin in (d, nth(1), nth(2)):
        close_block(origin)
    span = q2.at[0, 0 : rows - 1]
    wait_group(span, span, o_send.at[0], o_recv.at[1])
    close_block(nth(3))
    one, two = [
        jnp.concatenate([sums_ref[which, origin, part] for origin in range(depth) for part in range(2)], axis=0)
        for which in range(2)
    ]
    send_sums(1, pack_sums(one, two))
    first1, second1 = wait_sums(1)
    value = spread(inverse1) * (act1[...] - spread(first1) - nrm1[...] * spread(second1))
    out_ref[...] = (cot_t[...].astype(f32) + value).astype(bf16).T

    for copy in pending:
        copy.wait_send()
    def sent(span, send, recv):
        remote(span, span, send, recv, rows=sibling).wait_send()

    sent(x_cot.at[0, 0 : chips - 1], c_send.at[0], c_recv.at[0])
    sent(x_far, c_send.at[1], d_recv.at[0])
    sent(hid_two.at[0 : rows - 1], h_send.at[0], h_recv.at[0])
    sent(st_b.at[:, 0 : rows - 1], t_send.at[0], t_recv.at[0])
    sent(p2.at[:, 0 : rows - 1], o_send.at[0], o_recv.at[0])
    for count, here in ((chips - 1, own), (chips, jnp.logical_not(own))):
        @pl.when(here)
        def _():
            sent(r1.at[0:count], f_send.at[0], f_recv.at[0])

            @pl.when(middle)
            def _():
                sent(q1.at[:, 0:count], p_send.at[0], p_recv.at[0])
                sent(q_far.at[0:count], p_send.at[1], p_recv.at[2])

            @pl.when(jnp.logical_not(middle))
            def _():
                sent(q1.at[0, 0:count], p_send.at[0], p_recv.at[0])

    @pl.when(middle)
    def _():
        lend.wait_send()

    @pl.when(jnp.logical_not(middle))
    def _():
        lend_hid.wait_send()

    @pl.when(middle)
    def _():
        wait_hops(2 * depth)

    @pl.when(jnp.logical_not(middle))
    def _():
        wait_hops(2)


def kernel_body(
    depth, rows,
    latent, hidden, cotangent, filter_one, filter_two, gain_one, shift_one, gain_two, shift_two,
):
    images, _, breadth, channels = latent.shape
    lanes = images * breadth
    block = channels // depth
    half = block // 2
    chips = rows // 2
    wide = -(-3 * half // 128) * 128
    narrow = -(-3 * GSIZE // 128) * 128
    groups = channels // GSIZE
    bf16, f32 = jnp.bfloat16, jnp.float32
    dma = pltpu.SemaphoreType.DMA
    out = pl.pallas_call(
        functools.partial(kernel, depth, rows, breadth),
        out_shape=jax.ShapeDtypeStruct((lanes, channels), bf16),
        in_specs=[pl.BlockSpec(memory_space=pltpu.HBM)] * 9,
        out_specs=pl.BlockSpec(memory_space=pltpu.VMEM),
        scratch_shapes=[
            pltpu.VMEM((lanes, channels), bf16),
            pltpu.VMEM((lanes, channels), bf16),
            pltpu.VMEM((lanes, channels), bf16),
            pltpu.VMEM(filter_one.shape, bf16),
            pltpu.VMEM(filter_two.shape, bf16),
            pltpu.VMEM((4, 1, channels), f32),
            dma((6,)),
            pltpu.VMEM((channels, lanes), bf16),
            pltpu.VMEM((2, chips, block, lanes), bf16),
            pltpu.VMEM((2, rows, GSIZE, lanes), bf16),
            pltpu.VMEM((depth, 2, 3 * half, wide), bf16),
            pltpu.VMEM((depth, 2, 3 * half, wide), bf16),
            pltpu.VMEM((2, 2, 3, half, narrow), bf16),
            pltpu.VMEM((3 * half, wide), bf16),
            pltpu.VMEM((chips, 3, half, narrow), bf16),
            pltpu.VMEM((2, rows, wide, lanes), bf16),
            pltpu.VMEM((2, rows, wide, lanes), bf16),
            pltpu.VMEM((rows, 3 * half, lanes), f32),
            pltpu.VMEM((depth, 2, rows // 2, 2 * GSIZE, lanes), bf16),
            pltpu.VMEM((2, chips, rows // 2, 2 * GSIZE, lanes), bf16),
            pltpu.VMEM((depth, rows, half, lanes), bf16),
            pltpu.VMEM((depth, rows, half, lanes), bf16),
            pltpu.VMEM((rows, 2 * GSIZE, lanes), bf16),
            pltpu.VMEM((rows, 2 * GSIZE, lanes), bf16),
            pltpu.VMEM((channels, lanes), f32),
            pltpu.VMEM((channels, lanes), f32),
            pltpu.VMEM((2, rows // 2, 2 * GSIZE, lanes), f32),
            pltpu.VMEM((2, rows // 2, 2 * GSIZE, lanes), f32),
            pltpu.VMEM((4, lanes), f32),
            pltpu.VMEM((2, groups // 2, lanes), f32),
            pltpu.VMEM((2, rows, groups // 2, lanes), f32),
            pltpu.VMEM((channels, 8), f32),
            pltpu.VMEM((2, depth, 2, 2, lanes), f32),
            pltpu.VMEM((2, chips, block, lanes), bf16),
            pltpu.VMEM((rows, 2, GSIZE, lanes), bf16),
            pltpu.VMEM((rows, GSIZE, lanes), bf16),
            pltpu.VMEM((2, rows, wide, lanes), bf16),
            pltpu.VMEM((2, 2, rows // 2, 2 * GSIZE, lanes), bf16),
            pltpu.VMEM((chips, rows // 2, 2 * GSIZE, lanes), bf16),
            pltpu.VMEM((rows // 2, 2 * GSIZE, lanes), f32),
            pltpu.VMEM((rows // 2, 2 * GSIZE, lanes), f32),
            pltpu.VMEM((rows // 2, 2 * GSIZE, lanes), bf16),
            pltpu.VMEM((2, rows // 2, 2 * GSIZE, lanes), bf16),
            dma((2,)), dma((2, depth - 1, 2, 2)),
            dma((1,)), dma((1,)),
            dma((2,)), dma((2,)),
            dma((2,)), dma((2,)),
            dma((2,)), dma((2,)),
            dma((2,)), dma((3,)),
            dma((1,)), dma((2,)),
            dma((1,)), dma((2,)),
            dma((2,)),
            dma((1,)), dma((1,)),
        ],
        compiler_params=pltpu.CompilerParams(
            collective_id=0, has_side_effects=True, vmem_limit_bytes=48 * 1024 * 1024
        ),
    )(
        *[
            pltpu.with_memory_space_constraint(array, pltpu.HBM)
            for array in (
                latent.reshape(lanes, channels), hidden.reshape(lanes, channels),
                cotangent.reshape(lanes, channels), filter_one, filter_two,
                gain_one, shift_one, gain_two, shift_two,
            )
        ]
    )
    return out.reshape(latent.shape)


def solution(mesh):
    depth, rows = mesh.shape["dp"], mesh.shape["rows"]
    in_specs = (
        P("dp", "rows", None, None),
        P("dp", "rows", None, None),
        P("dp", "rows", None, None),
        P(None, "dp", "rows"),
        P(None, "dp", "rows"),
        P(),
        P(),
        P(),
        P(),
    )

    def body(latent, *rest):
        images, rows_here, breadth, channels = latent.shape
        fits = (
            rows_here == 1
            and images * breadth == 128
            and breadth % 4 == 0
            and depth == 4
            and rows == 2 * depth
            and channels == GROUPS * GSIZE
            and channels == depth * (rows // 2) * GSIZE
        )
        if fits:
            return kernel_body(depth, rows, latent, *rest)
        return plain_body(latent, *rest)

    return jax.shard_map(
        body, mesh=mesh, in_specs=in_specs, out_specs=P("dp", "rows", None, None), check_vma=False
    )
```
